128 devices in a mesh: data: 1, ctx: 128 (over z, y, x, core).
Axes of the slice: x: 4, y: 4, z: 4, core: 2. Of those that a mesh axis runs over, the one named last changes fastest.
Arguments:
- queries: bfloat16 [1, 32768, 5, 128], P('data', 'ctx')
- keys_in: bfloat16 [1, 32768, 1, 128], P('data', 'ctx')
- values_in: bfloat16 [1, 32768, 1, 128], P('data', 'ctx')
- grad_out: bfloat16 [1, 32768, 5, 128], P('data', 'ctx')
Outputs:
- output 1: bfloat16 [1, 32768, 5, 128], P('data', 'ctx')
- output 2: bfloat16 [1, 32768, 5, 128], P('data', 'ctx')
- output 3: bfloat16 [1, 32768, 1, 128], P('data', 'ctx')
- output 4: bfloat16 [1, 32768, 1, 128], P('data', 'ctx')
All inputs are finite; a program needn't handle non-finite values.
Results may differ from the reference program's by a relative error of at most 0.00975.
Values are sent between devices in bfloat16 or wider.
A program may use at most 1 GiB of HBM per device.

```python
import jax
import jax.numpy as jnp
from jax import lax

BATCH = 1
TOKENS_DEV = 256
CTX_DEVICES = 128
Q_LOCAL = 5
KV_LOCAL = 1
HEAD_DIM = 128

SEQ_LEN = CTX_DEVICES * TOKENS_DEV
HALF_LEN = TOKENS_DEV // 2
NUM_PIECES = 2 * CTX_DEVICES
GROUP_SIZE = Q_LOCAL // KV_LOCAL
SPREAD = 1.6


def true_positions():
    token_index = jnp.arange(SEQ_LEN, dtype=jnp.int32)
    shard_id = token_index // TOKENS_DEV
    offset = token_index % TOKENS_DEV
    low_pos = shard_id * HALF_LEN + offset
    high_pos = (NUM_PIECES - 1 - shard_id) * HALF_LEN + offset - HALF_LEN
    return jnp.where(offset < HALF_LEN, low_pos, high_pos)


def setup_inputs(seed: int = 0, part: int = 0) -> dict:
    base_key = jax.random.fold_in(jax.random.key(seed), part)
    key_q, key_k, key_v, key_g = jax.random.split(base_key, 4)
    q_shape = (BATCH, SEQ_LEN, Q_LOCAL, HEAD_DIM)
    kv_shape = (BATCH, SEQ_LEN, KV_LOCAL, HEAD_DIM)
    queries = SPREAD * jax.random.normal(key_q, q_shape, jnp.float32)
    keys_in = SPREAD * jax.random.normal(key_k, kv_shape, jnp.float32)
    values_in = jax.random.normal(key_v, kv_shape, jnp.float32)
    grad_out = jax.random.normal(key_g, q_shape, jnp.float32)
    return {"queries": queries.astype(jnp.bfloat16), "keys_in": keys_in.astype(jnp.bfloat16), "values_in": values_in.astype(jnp.bfloat16), "grad_out": grad_out.astype(jnp.bfloat16)}


def reference(queries, keys_in, values_in, grad_out):
    score_scale = HEAD_DIM ** -0.5
    positions = true_positions()
    block_pos = positions.reshape(NUM_PIECES, HALF_LEN)
    keys_wide = keys_in.astype(jnp.float32)
    values_wide = values_in.astype(jnp.float32)

    def to_blocks(tensor):
        return tensor.reshape(BATCH, NUM_PIECES, HALF_LEN, KV_LOCAL, GROUP_SIZE, HEAD_DIM).transpose(1, 0, 2, 3, 4, 5)

    def from_blocks(tensor):
        return tensor.transpose(1, 0, 2, 3, 4, 5).reshape(BATCH, SEQ_LEN, Q_LOCAL, HEAD_DIM)

    def masked_scores(q_blk, pos_blk):
        raw_scores = jnp.einsum("bqhgd,bkhd->bhgqk", q_blk.astype(jnp.float32), keys_wide) * score_scale
        visible = pos_blk[:, None] >= positions[None, :]
        return jnp.where(visible, raw_scores, -jnp.inf)

    def forward_block(blk_args):
        q_blk, pos_blk = blk_args
        masked = masked_scores(q_blk, pos_blk)
        row_max = jnp.max(masked, axis=-1)
        row_sum = jnp.sum(jnp.exp(masked - row_max[..., None]), axis=-1)
        log_sum = row_max + jnp.log(row_sum)
        prob_tile = jnp.exp(masked - log_sum[..., None]).astype(jnp.bfloat16).astype(jnp.float32)
        out_blk = jnp.einsum("bhgqk,bkhd->bqhgd", prob_tile, values_wide)
        return out_blk.astype(jnp.bfloat16), log_sum

    q_blocks = to_blocks(queries)
    g_blocks = to_blocks(grad_out)
    out_blocks, lse_blocks = lax.map(forward_block, (q_blocks, block_pos))
    d_rows = jnp.einsum("nbqhgd,nbqhgd->nbhgq", g_blocks.astype(jnp.float32), out_blocks.astype(jnp.float32))

    def backward_step(loop_carry, blk_args):
        dk_acc, dv_acc = loop_carry
        q_blk, g_blk, lse_blk, drow_blk, pos_blk = blk_args
        q_wide = q_blk.astype(jnp.float32)
        g_wide = g_blk.astype(jnp.float32)
        prob_tile = jnp.exp(masked_scores(q_blk, pos_blk) - lse_blk[..., None])
        prob_low = prob_tile.astype(jnp.bfloat16).astype(jnp.float32)
        dv_acc = dv_acc + jnp.einsum("bhgqk,bqhgd->bkhd", prob_low, g_wide)
        dprob_tile = jnp.einsum("bqhgd,bkhd->bhgqk", g_wide, values_wide)
        dscore_tile = (prob_tile * (dprob_tile - drow_blk[..., None])).astype(jnp.bfloat16).astype(jnp.float32)
        dq_blk = jnp.einsum("bhgqk,bkhd->bqhgd", dscore_tile, keys_wide) * score_scale
        dk_acc = dk_acc + jnp.einsum("bhgqk,bqhgd->bkhd", dscore_tile, q_wide) * score_scale
        return (dk_acc, dv_acc), dq_blk.astype(jnp.bfloat16)

    zeros_kv = jnp.zeros((BATCH, SEQ_LEN, KV_LOCAL, HEAD_DIM), jnp.float32)
    grads_kv, dq_blocks = lax.scan(backward_step, (zeros_kv, zeros_kv), (q_blocks, g_blocks, lse_blocks, d_rows, block_pos))
    return (from_blocks(out_blocks), from_blocks(dq_blocks), grads_kv[0].astype(jnp.bfloat16), grads_kv[1].astype(jnp.bfloat16))
```

```python
import functools
import math

import jax
import jax.numpy as jnp
from jax import lax
from jax.experimental import pallas as pl
from jax.experimental.pallas import tpu as pltpu
from jax.sharding import PartitionSpec as P

MESH = pl.DeviceIdType.MESH
NEG = -1e30
HD = 128
HEADS = 5
PIECE = 128
SCALE = HD ** -0.5
LOG2E = 1.4426950408889634

TREE6 = [None, 0, 1, 1, 2, 0, 2, 0, 3, 3, 1, 3, 2, 3, 2, 2, 4, 4, 4, 1, 4, 4, 2, 4, 3, 0, 1, 0, 3, 4, 3, 2, 5, 0, 5, 5, 2, 5, 1, 1, 5,
         3, 1, 0, 3, 5, 5, 1, 4, 0, 4, 5, 2, 0, 4, 2, 3, 0, 5, 5, 5, 4, 2, 3]


def popcount(value):
    return bin(value).count("1")


class Plan:
    def __init__(self, dims):
        self.dims = dims
        self.blocks = 1 << dims
        self.pairs = self.blocks // 2
        if dims == 6:
            self.link = list(TREE6)
        else:
            self.link = [None] * self.blocks
            count = [0] * dims
            for r in sorted(range(1, self.blocks), key=popcount):
                self.link[r] = min((d for d in range(dims) if (r >> d) & 1), key=lambda d: count[d])
                count[self.link[r]] += 1
        self.kids = {r: [r | (1 << d) for d in range(dims) if not (r >> d) & 1 and self.link[r | (1 << d)] == d]
                     for r in range(self.blocks)}
        self.height = {}
        for r in sorted(range(self.blocks), key=popcount, reverse=True):
            self.height[r] = max([1 + self.height[k] for k in self.kids[r]], default=0)
        for r in self.kids:
            self.kids[r].sort(key=lambda k: -self.height[k])
        self.forward()
        self.backward()

    def forward(self, block_us=2.8, hop_us=1.9, group_us=0.36):
        free = [0.0] * self.dims
        due = {}
        done = {0}

        def send(r, now):
            for k in self.kids[r]:
                d = self.link[k]
                free[d] = max(free[d], now) + block_us
                due[k] = free[d] + hop_us

        send(0, 0.0)
        now = 1.5
        steps, waits, ready = [], [], []
        while len(done) < self.blocks or ready:
            for r in sorted((r for r in due if r not in done and due[r] <= now), key=lambda r: due[r]):
                done.add(r)
                now += 0.03
                send(r, now)
                waits.append(r)
                if r ^ 1 in done:
                    ready += [r >> 1] * (3 if r == 1 else 2)
            if ready and (0 in ready or steps):
                pair = 0 if 0 in ready else ready[0]
                ready.remove(pair)
                steps.append((waits, pair))
                waits = []
                now += group_us
            else:
                now = max(now, min(due[r] for r in due if r not in done))
        self.fwd_steps = steps

    def backward(self, block_us=5.6, hop_us=2.0, group_us=0.95):
        order = [pair for _, pair in reversed(self.fwd_steps)]
        free = [0.0] * self.dims
        due = {}
        computed, sent = set(), set()
        now = 0.0
        steps, left = [], {pair: order.count(pair) for pair in order}
        sends = []
        position = 0
        while True:
            again = True
            while again:
                again = False
                able = [r for r in computed - sent if r and all(due.get(k, 1e9) <= now for k in self.kids[r])]
                for r in sorted(able, key=lambda r: (-popcount(r), r)):
                    sent.add(r)
                    now += 0.12 * len(self.kids[r]) + 0.03
                    d = self.link[r]
                    free[d] = max(free[d], now) + block_us
                    due[r] = free[d] + hop_us
                    sends.append(r)
                    again = True
            if position < len(order):
                pair = order[position]
                position += 1
                now += group_us
                left[pair] -= 1
                if not left[pair]:
                    computed |= {2 * pair, 2 * pair + 1}
                steps.append((sends, pair))
                sends = []
            elif len(sent) < self.blocks - 1:
                now = max(now, min(max(due.get(k, 1e9) for k in self.kids[r]) for r in range(1, self.blocks) if r not in sent))
            else:
                break
        self.bwd_steps = steps
        self.bwd_tail = sends


def xor(a, b):
    return a + b - 2 * a * b


def lookup(index, table):
    level = [jnp.int32(v) for v in table]
    bit = 1
    while len(level) > 1:
        odd = (index // bit) % 2 == 1
        nxt = []
        for i in range(0, len(level) - 1, 2):
            nxt.append(jnp.where(odd, level[i + 1], level[i]))
        if len(level) % 2:
            nxt.append(level[-1])
        level = nxt
        bit *= 2
    return level[0]


def branch(index, low, high, leaf):
    if high - low == 1:
        leaf(low)
        return
    mid = (low + high) // 2

    @pl.when(index < mid)
    def _():
        branch(index, low, mid, leaf)

    @pl.when(index >= mid)
    def _():
        branch(index, mid, high, leaf)


def kernel(plan, q_ref, k_ref, v_ref, g_ref, o_ref, dq_out, dk_out, dv_out,
           kv, stg, land, q_s, g_s, q_t, g_t, acc, mst, lst, xacc, xm, xl, lrow, drow, lcol, dcol, dq_s, xdq,
           ag_send, ag_recv, rs_send, rs_recv, x_send, x_recv):
    dims = plan.dims
    pieces = 4 * plan.blocks
    me = lax.axis_index("ctx")
    core = me % 2
    chip = me // 2
    bits = [(chip // (1 << d)) % 2 for d in range(dims)]
    gray = [xor(bits[d], bits[d + 1]) if d % 2 == 0 and d + 1 < dims else bits[d] for d in range(dims)]
    nbr = []
    for d in range(dims):
        other = chip + (1 - 2 * bits[d]) * (1 << d)
        if d % 2:
            other = other + (1 - 2 * bits[d - 1]) * (1 << (d - 1))
        nbr.append(2 * other + core)
    mate = me + 1 - 2 * core
    my_pair = chip // 2

    barrier = pltpu.get_barrier_semaphore()
    for dev in nbr + [mate]:
        pl.semaphore_signal(barrier, inc=1, device_id={"ctx": dev}, device_id_type=MESH)

    for h in range(2):
        rows = pl.ds(h * PIECE, PIECE)
        kv[0, 0, 0, h] = k_ref[rows, :]
        kv[0, 0, 1, h] = v_ref[rows, :].T
        for head in range(HEADS):
            c = h * 10 + head
            q_s[c] = q_ref[head, rows, :]
            g_s[c] = g_ref[head, rows, :]
    mst[...] = jnp.full(mst.shape, NEG, jnp.float32)
    lst[...] = jnp.zeros(lst.shape, jnp.float32)
    acc[...] = jnp.zeros(acc.shape, jnp.float32)
    dq_s[...] = jnp.zeros(dq_s.shape, jnp.float32)

    pl.semaphore_wait(barrier, dims + 1)

    def ag_copy(k):
        d = plan.link[k]
        r = k ^ (1 << d)
        return pltpu.make_async_remote_copy(
            src_ref=kv.at[r >> 1, r & 1], dst_ref=kv.at[k >> 1, k & 1], send_sem=ag_send.at[k], recv_sem=ag_recv.at[k],
            device_id={"ctx": nbr[d]}, device_id_type=MESH)

    def rs_copy(r):
        return pltpu.make_async_remote_copy(
            src_ref=stg.at[r >> 1, r & 1], dst_ref=land.at[r], send_sem=rs_send.at[r], recv_sem=rs_recv.at[r],
            device_id={"ctx": nbr[plan.link[r]]}, device_id_type=MESH)

    def mate_copy(src, dst, sem):
        return pltpu.make_async_remote_copy(src_ref=src, dst_ref=dst, send_sem=x_send.at[sem], recv_sem=x_recv.at[sem],
                                            device_id={"ctx": mate}, device_id_type=MESH)

    def own(ref, h):
        return ref.at[pl.ds(h * 10, 5)]

    def theirs(ref, h):
        return ref.at[pl.ds(h * 10 + 5, 5)]

    x_q = [mate_copy(own(ref, h), theirs(ref, h), 2 * j + h) for j, ref in enumerate((q_s, g_s)) for h in range(2)]
    for copy in x_q:
        copy.start()
    for k in plan.kids[0]:
        ag_copy(k).start()

    def ag_events(waits):
        for r in waits:
            ag_copy(r).wait_recv()
            for k in plan.kids[r]:
                ag_copy(k).start()

    def transposes(c):
        q_t[c] = q_s[c].T
        g_t[c] = g_s[c].T

    for h in range(2):
        pl.loop(h * 10, h * 10 + 5)(transposes)
    for copy in x_q:
        copy.wait_recv()
    for h in range(2):
        pl.loop(h * 10 + 5, h * 10 + 10)(transposes)

    def is_future(pair):
        rel = [(pair // (1 << (d - 1))) % 2 for d in range(1, dims)]
        gp = [None] + [xor(gray[d], rel[d - 1]) for d in range(1, dims)]
        other = gp[1] if dims > 1 else 0
        for d in range(2, dims):
            bit = xor(gp[d], gp[d + 1]) if d % 2 == 0 and d + 1 < dims else gp[d]
            other = other + bit * (1 << (d - 1))
        return (other - my_pair + plan.blocks) // plan.blocks

    def key_base(par, h):
        low = me if par == 0 else 2 * (chip + 1 - 2 * (chip % 2)) + core
        return (pieces - 1 - low if h else low) * PIECE

    def query_base(c):
        h, par = c // 10, (c // 5) % 2
        low = me if par == 0 else mate
        return (pieces - 1 - low if h else low) * PIECE

    def two(base0, base1, shape, axis):
        i = lax.broadcasted_iota(jnp.int32, shape, axis)
        return i + jnp.where(i < PIECE, base0, base1 - PIECE)

    coef = SCALE * LOG2E

    def key_tile(pair, h):
        return jnp.concatenate([kv[pair, 0, 0, h], kv[pair, 1, 0, h]], axis=0)

    def value_tile_t(pair, h):
        return jnp.concatenate([kv[pair, 0, 1, h], kv[pair, 1, 1, h]], axis=1)

    def wide(ref, c):
        return jnp.concatenate([ref[c], ref[c + 1]], axis=1)

    def tall(ref, c):
        return jnp.concatenate([ref[c], ref[c + 1]], axis=0)

    def fwd_group(pair, h, qg, masked):
        kt = key_tile(pair, h)
        vt = value_tile_t(pair, h)
        for t in range(HEADS):
            c = qg * 10 + 2 * t
            s = jnp.dot(kt, wide(q_t, c), preferred_element_type=jnp.float32) * coef
            if masked:
                kpos = two(key_base(0, h), key_base(1, h), s.shape, 0)
                qpos = two(query_base(c), query_base(c + 1), s.shape, 1)
                s = jnp.where(qpos >= kpos, s, NEG)
            m_old = wide(mst, c)
            m_new = jnp.maximum(m_old, jnp.max(s, axis=0, keepdims=True))
            p = jnp.exp2(s - m_new[0:1])
            decay = jnp.exp2(m_old - m_new)
            l_new = wide(lst, c) * decay + jnp.sum(p.reshape(s.shape[0] // 8, 8, s.shape[1]), axis=0)
            a_new = wide(acc, c) * decay[0:1] + jnp.dot(vt, p.astype(jnp.bfloat16), preferred_element_type=jnp.float32)
            for j in range(2):
                cols = slice(j * 128, j * 128 + 128)
                mst[c + j] = m_new[:, cols]
                lst[c + j] = l_new[:, cols]
                acc[c + j] = a_new[:, cols]

    own_groups = ((0, 0, True), (0, 1, False), (1, 1, True))
    for step, (h, qg, masked) in enumerate(own_groups):
        ag_events(plan.fwd_steps[step][0])
        fwd_group(0, h, qg, masked)

    steps = plan.fwd_steps[3:]

    if steps:
        @pl.loop(0, len(steps))
        def _(step):
            branch(step, 0, len(steps), lambda i: ag_events(steps[i][0]))
            pair = lookup(step // 2, [pair for _, pair in steps[::2]])
            fut = is_future(pair)
            g = step % 2
            fwd_group(pair, fut * g, 1 - (1 - fut) * (1 - g), False)

    x_m = []
    for h in range(2):
        inbox = pl.ds(h * 5, 5)
        x_m += [mate_copy(theirs(acc, h), xacc.at[inbox], 4 + 3 * h), mate_copy(theirs(mst, h), xm.at[inbox], 5 + 3 * h),
                mate_copy(theirs(lst, h), xl.at[inbox], 6 + 3 * h)]
    for copy in x_m:
        copy.start()
    x_r = [mate_copy(own(ref, h), theirs(ref, h), 10 + 2 * j + h) for j, ref in enumerate((lrow, drow)) for h in range(2)]

    for h in range(2):
        for copy in x_m[3 * h:3 * h + 3]:
            copy.wait_recv()
        for head in range(HEADS):
            c, x = h * 10 + head, h * 5 + head
            m1, m2 = mst[c], xm[x]
            m = jnp.maximum(m1, m2)
            w1, w2 = jnp.exp2(m1 - m), jnp.exp2(m2 - m)
            total = jnp.sum(lst[c] * w1 + xl[x] * w2, axis=0, keepdims=True)
            out = (acc[c] * w1[0:1] + xacc[x] * w2[0:1]) / total
            low = out.astype(jnp.bfloat16)
            o_ref[head, pl.ds(h * PIECE, PIECE), :] = out.T.astype(jnp.bfloat16)
            lrow[c] = m + jnp.log2(total)
            d = jnp.sum(low.astype(jnp.float32) * g_t[c].astype(jnp.float32), axis=0, keepdims=True)
            drow[c] = jnp.broadcast_to(d, (8, 128))
    for copy in x_r:
        copy.start()

    def columns(c):
        lcol[c] = jnp.broadcast_to(lrow[c, 0:1], (128, 128)).T
        dcol[c] = jnp.broadcast_to(drow[c, 0:1], (128, 128)).T

    for h in range(2):
        pl.loop(h * 10, h * 10 + 5)(columns)
    for copy in x_r:
        copy.wait_recv()
    for h in range(2):
        pl.loop(h * 10 + 5, h * 10 + 10)(columns)

    def bwd_group(pair, h, qg, masked):
        kt = key_tile(pair, h)
        vt = value_tile_t(pair, h)
        dk_sum = dv_sum = None
        for t in range(HEADS):
            c = qg * 10 + 2 * t
            s = lax.dot_general(tall(q_s, c), kt, (((1,), (1,)), ((), ())), preferred_element_type=jnp.float32) * coef
            if masked:
                qpos = two(query_base(c), query_base(c + 1), s.shape, 0)
                kpos = two(key_base(0, h), key_base(1, h), s.shape, 1)
                s = jnp.where(qpos >= kpos, s, NEG)
            lse = tall(lcol, c)
            p = jnp.exp2(s - jnp.concatenate([lse, lse], axis=1))
            dp = jnp.dot(tall(g_s, c), vt, preferred_element_type=jnp.float32)
            dr = tall(dcol, c)
            ds = (p * (dp - jnp.concatenate([dr, dr], axis=1))).astype(jnp.bfloat16)
            dv = jnp.dot(wide(g_t, c), p.astype(jnp.bfloat16), preferred_element_type=jnp.float32)
            dk = jnp.dot(wide(q_t, c), ds, preferred_element_type=jnp.float32)
            dk_sum, dv_sum = (dk, dv) if dk_sum is None else (dk_sum + dk, dv_sum + dv)
            dq = jnp.dot(ds, kt, preferred_element_type=jnp.float32)
            for j in range(2):
                dq_s[c + j] += dq[j * 128:j * 128 + 128]
        for par in range(2):
            cols = slice(par * 128, par * 128 + 128)
            stg[pair, par, 0, h] += dk_sum[:, cols]
            stg[pair, par, 1, h] += dv_sum[:, cols]

    def rs_events(sends):
        for r in sends:
            for k in plan.kids[r]:
                rs_copy(k).wait_recv()

                @pl.loop(0, 4)
                def _(j):
                    stg[r >> 1, r & 1, j // 2, j % 2] += land[k, j // 2, j % 2]
            rs_copy(r).start()

    def clear(pair):
        for par in range(2):
            for j in range(4):
                stg[pair, par, j // 2, j % 2] = jnp.zeros((128, 128), jnp.float32)

    count = len(plan.bwd_steps) - 3
    if count:
        @pl.loop(0, count)
        def _(step):
            branch(step, 0, count, lambda i: rs_events(plan.bwd_steps[i][0]))
            pair = lookup(step // 2, [pair for _, pair in plan.bwd_steps[:count:2]])
            fut = is_future(pair)
            g = step % 2

            @pl.when(g == 0)
            def _():
                clear(pair)

            bwd_group(pair, fut * g, 1 - (1 - fut) * (1 - g), False)

    clear(0)
    for step, (h, qg, masked) in enumerate(own_groups):
        rs_events(plan.bwd_steps[count + step][0])
        bwd_group(0, h, qg, masked)

    x_d = [mate_copy(theirs(dq_s, h), xdq.at[pl.ds(h * 5, 5)], 14 + h) for h in range(2)]
    for copy in x_d:
        copy.start()
    rs_events(plan.bwd_tail)
    for h in range(2):
        x_d[h].wait_recv()
        for head in range(HEADS):
            total = (dq_s[h * 10 + head] + xdq[h * 5 + head]) * SCALE
            dq_out[head, pl.ds(h * PIECE, PIECE), :] = total.astype(jnp.bfloat16)
    for k in plan.kids[0]:
        rs_copy(k).wait_recv()
    for h in range(2):
        for j, ref in enumerate((dk_out, dv_out)):
            total = stg[0, 0, j, h]
            for k in plan.kids[0]:
                total = total + land[k, j, h]
            if j == 0:
                total = total * SCALE
            ref[pl.ds(h * PIECE, PIECE), :] = total.T.astype(jnp.bfloat16)

    for k in range(1, plan.blocks):
        ag_copy(k).wait_send()
        rs_copy(k).wait_send()
    for copy in x_q + x_m + x_r + x_d:
        copy.wait_send()


def solution(mesh):
    size = mesh.shape["ctx"]
    plan = Plan(int(math.log2(size)) - 1)
    spec = P("data", "ctx", None, None)
    n = plan.blocks
    f32, bf16 = jnp.float32, jnp.bfloat16
    vm = pltpu.VMEM

    def local(queries, keys, values, grad_out):
        tokens = queries.shape[1]
        q = queries[0].transpose(1, 0, 2)
        g = grad_out[0].transpose(1, 0, 2)
        tile = (128, 128)
        big = jax.ShapeDtypeStruct((HEADS, tokens, HD), bf16)
        small = jax.ShapeDtypeStruct((tokens, HD), bf16)
        flops = 14 * 640 * PIECE * n * 2 * HD
        o, dq, dk, dv = pl.pallas_call(
            functools.partial(kernel, plan),
            out_shape=(big, big, small, small),
            in_specs=[pl.BlockSpec(memory_space=vm)] * 4,
            out_specs=(pl.BlockSpec(memory_space=vm),) * 4,
            scratch_shapes=[
                vm((n // 2, 2, 2, 2) + tile, bf16),
                vm((n // 2, 2, 2, 2) + tile, f32),
                vm((n, 2, 2) + tile, f32),
                vm((20,) + tile, bf16), vm((20,) + tile, bf16), vm((20,) + tile, bf16), vm((20,) + tile, bf16),
                vm((20,) + tile, f32), vm((20, 8, 128), f32), vm((20, 8, 128), f32),
                vm((10,) + tile, f32), vm((10, 8, 128), f32), vm((10, 8, 128), f32),
                vm((20, 8, 128), f32), vm((20, 8, 128), f32),
                vm((20,) + tile, f32), vm((20,) + tile, f32),
                vm((20,) + tile, f32), vm((10,) + tile, f32),
                pltpu.SemaphoreType.DMA((n,)), pltpu.SemaphoreType.DMA((n,)),
                pltpu.SemaphoreType.DMA((n,)), pltpu.SemaphoreType.DMA((n,)),
                pltpu.SemaphoreType.DMA((16,)), pltpu.SemaphoreType.DMA((16,)),
            ],
            compiler_params=pltpu.CompilerParams(collective_id=0, has_side_effects=True, vmem_limit_bytes=67043328),
            cost_estimate=pl.CostEstimate(flops=flops, bytes_accessed=4 << 20, transcendentals=0),
        )(q, keys[0, :, 0], values[0, :, 0], g)
        return (o.transpose(1, 0, 2)[None], dq.transpose(1, 0, 2)[None], dk[None, :, None], dv[None, :, None])

    return jax.shard_map(local, mesh=mesh, in_specs=(spec,) * 4, out_specs=(spec,) * 4, check_vma=False)
```

```python
import functools
import math

import jax
import jax.numpy as jnp
from jax import lax
from jax.experimental import pallas as pl
from jax.experimental.pallas import tpu as pltpu
from jax.sharding import PartitionSpec as P

MESH = pl.DeviceIdType.MESH
NEG = -1e30
HD = 128
HEADS = 5
PIECE = 128
SCALE = HD ** -0.5
LOG2E = 1.4426950408889634

TREE6 = "011202033132322444144243010343250552511531035514045204230555423"


def popcount(value):
    return bin(value).count("1")


class Plan:
    def __init__(self, dims):
        self.dims = dims
        self.blocks = 1 << dims
        self.pairs = self.blocks // 2
        if dims == 6:
            self.link = [None] + [int(d) for d in TREE6]
        else:
            self.link = [None] * self.blocks
            count = [0] * dims
            for r in sorted(range(1, self.blocks), key=popcount):
                self.link[r] = min((d for d in range(dims) if (r >> d) & 1), key=lambda d: count[d])
                count[self.link[r]] += 1
        self.kids = {r: [r | (1 << d) for d in range(dims) if not (r >> d) & 1 and self.link[r | (1 << d)] == d]
                     for r in range(self.blocks)}
        self.height = {}
        for r in sorted(range(self.blocks), key=popcount, reverse=True):
            self.height[r] = max([1 + self.height[k] for k in self.kids[r]], default=0)
        for r in self.kids:
            self.kids[r].sort(key=lambda k: -self.height[k])
        self.forward()
        self.backward()

    def forward(self, block_us=2.8, hop_us=1.9, group_us=0.36):
        free = [0.0] * self.dims
        due = {}
        done = {0}

        def send(r, now):
            for k in self.kids[r]:
                d = self.link[k]
                free[d] = max(free[d], now) + block_us
                due[k] = free[d] + hop_us

        send(0, 0.0)
        now = 1.5
        steps, waits, ready = [], [], []
        while len(done) < self.blocks or ready:
            for r in sorted((r for r in due if r not in done and due[r] <= now), key=lambda r: due[r]):
                done.add(r)
                now += 0.03
                send(r, now)
                waits.append(r)
                if r ^ 1 in done:
                    ready += [r >> 1] * (3 if r == 1 else 2)
            if ready and (0 in ready or steps):
                pair = 0 if 0 in ready else ready[0]
                ready.remove(pair)
                steps.append((waits, pair))
                waits = []
                now += group_us
            else:
                now = max(now, min(due[r] for r in due if r not in done))
        self.fwd_steps = steps

    def backward(self, block_us=5.6, hop_us=2.0, group_us=0.95):
        order = [pair for _, pair in reversed(self.fwd_steps)]
        free = [0.0] * self.dims
        due = {}
        computed, sent = set(), set()
        now = 0.0
        steps, left = [], {pair: order.count(pair) for pair in order}
        sends = []
        position = 0
        while True:
            again = True
            while again:
                again = False
                able = [r for r in computed - sent if r and all(due.get(k, 1e9) <= now for k in self.kids[r])]
                for r in sorted(able, key=lambda r: (-popcount(r), r)):
                    sent.add(r)
                    now += 0.12 * len(self.kids[r]) + 0.03
                    d = self.link[r]
                    free[d] = max(free[d], now) + block_us
                    due[r] = free[d] + hop_us
                    sends.append(r)
                    again = True
            if position < len(order):
                pair = order[position]
                position += 1
                now += group_us
                left[pair] -= 1
                if not left[pair]:
                    computed |= {2 * pair, 2 * pair + 1}
                steps.append((sends, pair))
                sends = []
            elif len(sent) < self.blocks - 1:
                now = max(now, min(max(due.get(k, 1e9) for k in self.kids[r]) for r in range(1, self.blocks) if r not in sent))
            else:
                break
        self.bwd_steps = steps
        self.bwd_tail = sends


def xor(a, b):
    return a + b - 2 * a * b


def lookup(index, table):
    level = [jnp.int32(v) for v in table]
    bit = 1
    while len(level) > 1:
        odd = (index // bit) % 2 == 1
        nxt = []
        for i in range(0, len(level) - 1, 2):
            nxt.append(jnp.where(odd, level[i + 1], level[i]))
        if len(level) % 2:
            nxt.append(level[-1])
        level = nxt
        bit *= 2
    return level[0]


def branch(index, low, high, leaf):
    if high - low == 1:
        leaf(low)
        return
    mid = (low + high) // 2
    lax.cond(index < mid, lambda: branch(index, low, mid, leaf), lambda: branch(index, mid, high, leaf))


def kernel(plan, q_ref, k_ref, v_ref, g_ref, o_ref, dq_out, dk_out, dv_out,
           kv, stg, land, s_buf, t_buf, p_buf, d_buf, q_s, g_s, q_t, g_t, acc, mst, lst, dec, xacc, xm, xl, lrow, drow, lcol, dcol, dq_s, xdq,
           ag_send, ag_recv, rs_send, rs_recv, x_send, x_recv):
    dims = plan.dims
    pieces = 4 * plan.blocks
    me = lax.axis_index("ctx")
    core = me % 2
    chip = me // 2
    bits = [(chip // (1 << d)) % 2 for d in range(dims)]
    gray = [xor(bits[d], bits[d + 1]) if d % 2 == 0 and d + 1 < dims else bits[d] for d in range(dims)]
    nbr = []
    for d in range(dims):
        other = chip + (1 - 2 * bits[d]) * (1 << d)
        if d % 2:
            other = other + (1 - 2 * bits[d - 1]) * (1 << (d - 1))
        nbr.append(2 * other + core)
    mate = me + 1 - 2 * core
    my_pair = chip // 2

    barrier = pltpu.get_barrier_semaphore()
    for dev in nbr + [mate]:
        pl.semaphore_signal(barrier, inc=1, device_id={"ctx": dev}, device_id_type=MESH)

    for h in range(2):
        rows = pl.ds(h * PIECE, PIECE)
        kv[0, 0, 0, h] = k_ref[rows, :]
        kv[0, 0, 1, h] = v_ref[rows, :].T
        for head in range(HEADS):
            c = h * 10 + head
            q_s[c] = q_ref[head, rows, :]
            g_s[c] = g_ref[head, rows, :]
    mst[...] = jnp.full(mst.shape, NEG, jnp.float32)
    lst[...] = jnp.zeros(lst.shape, jnp.float32)
    acc[...] = jnp.zeros(acc.shape, jnp.float32)
    dec[...] = jnp.ones(dec.shape, jnp.float32)
    p_buf[...] = jnp.zeros(p_buf.shape, jnp.bfloat16)
    d_buf[...] = jnp.zeros(d_buf.shape, jnp.bfloat16)
    dq_s[...] = jnp.zeros(dq_s.shape, jnp.float32)

    pl.semaphore_wait(barrier, dims + 1)

    def ag_copy(k):
        d = plan.link[k]
        r = k ^ (1 << d)
        return pltpu.make_async_remote_copy(
            src_ref=kv.at[r >> 1, r & 1], dst_ref=kv.at[k >> 1, k & 1], send_sem=ag_send.at[k], recv_sem=ag_recv.at[k],
            device_id={"ctx": nbr[d]}, device_id_type=MESH)

    def rs_copy(r):
        return pltpu.make_async_remote_copy(
            src_ref=stg.at[r >> 1, r & 1], dst_ref=land.at[r], send_sem=rs_send.at[r], recv_sem=rs_recv.at[r],
            device_id={"ctx": nbr[plan.link[r]]}, device_id_type=MESH)

    def mate_copy(src, dst, sem):
        return pltpu.make_async_remote_copy(src_ref=src, dst_ref=dst, send_sem=x_send.at[sem], recv_sem=x_recv.at[sem],
                                            device_id={"ctx": mate}, device_id_type=MESH)

    def own(ref, h):
        return ref.at[pl.ds(h * 10, 5)]

    def theirs(ref, h):
        return ref.at[pl.ds(h * 10 + 5, 5)]

    x_q = [mate_copy(own(ref, h), theirs(ref, h), 2 * j + h) for j, ref in enumerate((q_s, g_s)) for h in range(2)]
    for copy in x_q:
        copy.start()
    for k in plan.kids[0]:
        ag_copy(k).start()

    def ag_events(waits):
        for r in waits:
            ag_copy(r).wait_recv()
            for k in plan.kids[r]:
                ag_copy(k).start()

    def transposes(c):
        q_t[c] = q_s[c].T
        g_t[c] = g_s[c].T

    for h in range(2):
        pl.loop(h * 10, h * 10 + 5)(transposes)
    for copy in x_q:
        copy.wait_recv()
    for h in range(2):
        pl.loop(h * 10 + 5, h * 10 + 10)(transposes)

    def is_future(pair):
        rel = [(pair // (1 << (d - 1))) % 2 for d in range(1, dims)]
        gp = [None] + [xor(gray[d], rel[d - 1]) for d in range(1, dims)]
        other = gp[1] if dims > 1 else 0
        for d in range(2, dims):
            bit = xor(gp[d], gp[d + 1]) if d % 2 == 0 and d + 1 < dims else gp[d]
            other = other + bit * (1 << (d - 1))
        return (other - my_pair + plan.blocks) // plan.blocks

    def key_base(par, h):
        low = me if par == 0 else 2 * (chip + 1 - 2 * (chip % 2)) + core
        return (low + h * (pieces - 1 - 2 * low)) * PIECE

    def query_base(c):
        h, par = c // 10, (c // 5) % 2
        low = me + par * (mate - me)
        return (low + h * (pieces - 1 - 2 * low)) * PIECE

    def two(base0, base1, shape, axis):
        i = lax.broadcasted_iota(jnp.int32, shape, axis)
        return i + jnp.where(i < PIECE, base0, base1 - PIECE)

    coef = SCALE * LOG2E

    def key_tile(pair, h):
        return jnp.concatenate([kv[pair, 0, 0, h], kv[pair, 1, 0, h]], axis=0)

    def value_tile_t(pair, h):
        return jnp.concatenate([kv[pair, 0, 1, h], kv[pair, 1, 1, h]], axis=1)

    def wide(ref, c):
        return jnp.concatenate([ref[c], ref[c + 1]], axis=1)

    def tall(ref, c):
        return jnp.concatenate([ref[c], ref[c + 1]], axis=0)

    tiles = [slice(t * 256, t * 256 + 256) for t in range(HEADS)]

    def mask_scores(h, qg, keys_axis):
        @pl.loop(0, HEADS)
        def _(t):
            c = qg * 10 + 2 * t
            shape = (256, 256)
            kpos = two(key_base(0, h), key_base(1, h), shape, keys_axis)
            qpos = two(query_base(c), query_base(c + 1), shape, 1 - keys_axis)
            s_buf[t] = jnp.where(qpos >= kpos, s_buf[t], NEG)

    def fwd_scores(pair, h, qg):
        kt = key_tile(pair, h)
        for t in range(HEADS):
            s_buf[t] = jnp.dot(kt, wide(q_t, qg * 10 + 2 * t), preferred_element_type=jnp.float32)

    def fwd_softmax(qg):
        for t in range(HEADS):
            c = qg * 10 + 2 * t
            m_old = wide(mst, c)
            m_new = jnp.maximum(m_old, jnp.max(s_buf[t], axis=0, keepdims=True) * coef)
            p = jnp.exp2(s_buf[t] * coef - m_new[0:1])
            decay = jnp.exp2(m_old - m_new)
            l_new = wide(lst, c) * decay + jnp.sum(p.reshape(32, 8, 256), axis=0)
            p_buf[tiles[t], :] = p.astype(jnp.bfloat16)
            dec[t] = decay
            for j in range(2):
                cols = slice(j * 128, j * 128 + 128)
                mst[c + j] = m_new[:, cols]
                lst[c + j] = l_new[:, cols]

    def fwd_out(pair, h, qg):
        vt = value_tile_t(pair, h)
        for t in range(HEADS):
            c = qg * 10 + 2 * t
            pv = jnp.dot(vt, p_buf[tiles[t], :], preferred_element_type=jnp.float32)
            for j in range(2):
                cols = slice(j * 128, j * 128 + 128)
                acc[c + j] = acc[c + j] * dec[t, 0:1, cols] + pv[:, cols]

    steps = plan.fwd_steps
    nsteps = len(steps)
    fwd_pairs = [pair for _, pair in steps]

    def fwd_place(j):
        j = jnp.minimum(j, nsteps - 1)
        pair = lookup(j, fwd_pairs)
        fut = is_future(pair)
        mine = 1 - jnp.minimum(j // 3, 1)
        g = (j - 3) % 2
        h = mine * (j // 2) + (1 - mine) * fut * g
        qg = mine * ((j + 1) // 2) + (1 - mine) * (1 - (1 - fut) * (1 - g))
        return pair, h, qg

    ag_events(steps[0][0])
    fwd_scores(0, 0, 0)
    first = (me * 0,) * 3

    def fwd_turn(j, carry):
        old, cur = carry
        branch(j, 0, nsteps, lambda i: ag_events(steps[i + 1][0]) if i + 1 < nsteps else None)
        new = fwd_place(j + 1)

        @pl.when((j == 0) | (j == 2))
        def _():
            mask_scores(cur[1], cur[2], 0)

        fwd_out(*old)
        fwd_softmax(cur[2])
        fwd_scores(*new)
        return cur, new

    last = lax.fori_loop(0, nsteps, fwd_turn, (first, first))[0]
    fwd_out(*last)

    x_m = []
    for h in range(2):
        inbox = pl.ds(h * 5, 5)
        x_m += [mate_copy(theirs(acc, h), xacc.at[inbox], 4 + 3 * h), mate_copy(theirs(mst, h), xm.at[inbox], 5 + 3 * h),
                mate_copy(theirs(lst, h), xl.at[inbox], 6 + 3 * h)]
    for copy in x_m:
        copy.start()
    x_r = [mate_copy(own(ref, h), theirs(ref, h), 10 + 2 * j + h) for j, ref in enumerate((lrow, drow)) for h in range(2)]

    for h in range(2):
        for copy in x_m[3 * h:3 * h + 3]:
            copy.wait_recv()
        for head in range(HEADS):
            c, x = h * 10 + head, h * 5 + head
            m1, m2 = mst[c], xm[x]
            m = jnp.maximum(m1, m2)
            w1, w2 = jnp.exp2(m1 - m), jnp.exp2(m2 - m)
            total = jnp.sum(lst[c] * w1 + xl[x] * w2, axis=0, keepdims=True)
            out = (acc[c] * w1[0:1] + xacc[x] * w2[0:1]) / total
            low = out.astype(jnp.bfloat16)
            o_ref[head, pl.ds(h * PIECE, PIECE), :] = out.T.astype(jnp.bfloat16)
            lrow[c] = m + jnp.log2(total)
            d = jnp.sum(low.astype(jnp.float32) * g_t[c].astype(jnp.float32), axis=0, keepdims=True)
            drow[c] = jnp.broadcast_to(d, (8, 128))
    for copy in x_r:
        copy.start()

    def columns(c):
        lcol[c] = jnp.broadcast_to(lrow[c, 0:1], (128, 128)).T
        dcol[c] = jnp.broadcast_to(drow[c, 0:1], (128, 128)).T

    for h in range(2):
        pl.loop(h * 10, h * 10 + 5)(columns)
    for copy in x_r:
        copy.wait_recv()
    for h in range(2):
        pl.loop(h * 10 + 5, h * 10 + 10)(columns)

    def bwd_scores(pair, h, qg):
        kt = key_tile(pair, h)
        vt = value_tile_t(pair, h)
        for t in range(HEADS):
            c = qg * 10 + 2 * t
            s_buf[t] = lax.dot_general(tall(q_s, c), kt, (((1,), (1,)), ((), ())), preferred_element_type=jnp.float32)
            t_buf[t] = jnp.dot(tall(g_s, c), vt, preferred_element_type=jnp.float32)

    def bwd_softmax(qg):
        for t in range(HEADS):
            c = qg * 10 + 2 * t
            lse, dr = tall(lcol, c), tall(dcol, c)
            p = jnp.exp2(s_buf[t] * coef - jnp.concatenate([lse, lse], axis=1))
            p_buf[tiles[t], :] = p.astype(jnp.bfloat16)
            d_buf[tiles[t], :] = (p * (t_buf[t] - jnp.concatenate([dr, dr], axis=1))).astype(jnp.bfloat16)

    def bwd_out(pair, h, qg):
        kt = key_tile(pair, h)
        for ref, buf, j in ((q_t, d_buf, 0), (g_t, p_buf, 1)):
            rows = jnp.concatenate([ref[qg * 10 + i] for i in range(10)], axis=1)
            grad = jnp.dot(rows, buf[...], preferred_element_type=jnp.float32)
            for par in range(2):
                stg[pair, par, j, h] += grad[:, par * 128:par * 128 + 128]
        for t in range(HEADS):
            c = qg * 10 + 2 * t
            dq = jnp.dot(d_buf[tiles[t], :], kt, preferred_element_type=jnp.float32)
            for j in range(2):
                dq_s[c + j] += dq[j * 128:j * 128 + 128]

    def rs_adds(sends):
        for r in sends:
            for k in plan.kids[r]:
                rs_copy(k).wait_recv()

                @pl.loop(0, 4)
                def _(j):
                    stg[r >> 1, r & 1, j // 2, j % 2] += land[k, j // 2, j % 2]

    def rs_starts(sends):
        for r in sends:
            rs_copy(r).start()

    def clear(pair):
        for par in range(2):
            for j in range(4):
                stg[pair, par, j // 2, j % 2] = jnp.zeros((128, 128), jnp.float32)

    bwd_pairs = [pair for _, pair in plan.bwd_steps]
    sends_at = [sends for sends, _ in plan.bwd_steps]

    def bwd_place(j):
        j = jnp.minimum(j, nsteps - 1)
        pair = lookup(j, bwd_pairs)
        fut = is_future(pair)
        i = j - (nsteps - 3)
        mine = (j + 3) // nsteps
        g = j % 2
        h = mine * (i // 2) + (1 - mine) * fut * g
        qg = mine * ((i + 1) // 2) + (1 - mine) * (1 - (1 - fut) * (1 - g))
        return pair, h, qg

    first = bwd_place(me * 0)
    bwd_scores(*first)

    def bwd_turn(j, carry):
        old, cur = carry
        branch(j, 0, nsteps, lambda i: rs_adds(sends_at[i - 1] if i else ()))
        new = bwd_place(j + 1)

        @pl.when((j % 2 == 1) & (j < nsteps - 1))
        def _():
            clear(old[0])

        @pl.when((j == nsteps - 3) | (j == nsteps - 1))
        def _():
            mask_scores(cur[1], cur[2], 1)

        branch(j, 0, nsteps, lambda i: rs_starts(sends_at[i - 1] if i else ()))
        bwd_out(*old)
        bwd_softmax(cur[2])
        bwd_scores(*new)
        return cur, new

    last = lax.fori_loop(0, nsteps, bwd_turn, (first, first))[0]
    rs_adds(sends_at[nsteps - 1])
    rs_starts(sends_at[nsteps - 1])
    bwd_out(*last)

    x_d = [mate_copy(theirs(dq_s, h), xdq.at[pl.ds(h * 5, 5)], 14 + h) for h in range(2)]
    for copy in x_d:
        copy.start()
    for r in plan.bwd_tail:
        rs_adds([r])
        rs_starts([r])
    for h in range(2):
        x_d[h].wait_recv()
        for head in range(HEADS):
            total = (dq_s[h * 10 + head] + xdq[h * 5 + head]) * SCALE
            dq_out[head, pl.ds(h * PIECE, PIECE), :] = total.astype(jnp.bfloat16)
    for k in plan.kids[0]:
        rs_copy(k).wait_recv()
    for h in range(2):
        for j, ref in enumerate((dk_out, dv_out)):
            total = stg[0, 0, j, h]
            for k in plan.kids[0]:
                total = total + land[k, j, h]
            if j == 0:
                total = total * SCALE
            ref[pl.ds(h * PIECE, PIECE), :] = total.T.astype(jnp.bfloat16)

    for k in range(1, plan.blocks):
        ag_copy(k).wait_send()
        rs_copy(k).wait_send()
    for copy in x_q + x_m + x_r + x_d:
        copy.wait_send()


def solution(mesh):
    size = mesh.shape["ctx"]
    plan = Plan(int(math.log2(size)) - 1)
    spec = P("data", "ctx", None, None)
    n = plan.blocks
    f32, bf16 = jnp.float32, jnp.bfloat16
    vm = pltpu.VMEM

    def local(queries, keys, values, grad_out):
        tokens = queries.shape[1]
        q = queries[0].transpose(1, 0, 2)
        g = grad_out[0].transpose(1, 0, 2)
        tile = (128, 128)
        big = jax.ShapeDtypeStruct((HEADS, tokens, HD), bf16)
        small = jax.ShapeDtypeStruct((tokens, HD), bf16)
        flops = 14 * 640 * PIECE * n * 2 * HD
        o, dq, dk, dv = pl.pallas_call(
            functools.partial(kernel, plan),
            out_shape=(big, big, small, small),
            in_specs=[pl.BlockSpec(memory_space=vm)] * 4,
            out_specs=(pl.BlockSpec(memory_space=vm),) * 4,
            scratch_shapes=[
                vm((n // 2, 2, 2, 2) + tile, bf16),
                vm((n // 2, 2, 2, 2) + tile, f32),
                vm((n, 2, 2) + tile, f32),
                vm((HEADS, 256, 256), f32), vm((HEADS, 256, 256), f32), vm((HEADS * 256, 256), bf16), vm((HEADS * 256, 256), bf16),
                vm((20,) + tile, bf16), vm((20,) + tile, bf16), vm((20,) + tile, bf16), vm((20,) + tile, bf16),
                vm((20,) + tile, f32), vm((20, 8, 128), f32), vm((20, 8, 128), f32), vm((HEADS, 8, 256), f32),
                vm((10,) + tile, f32), vm((10, 8, 128), f32), vm((10, 8, 128), f32),
                vm((20, 8, 128), f32), vm((20, 8, 128), f32),
                vm((20,) + tile, f32), vm((20,) + tile, f32),
                vm((20,) + tile, f32), vm((10,) + tile, f32),
                pltpu.SemaphoreType.DMA((n,)), pltpu.SemaphoreType.DMA((n,)),
                pltpu.SemaphoreType.DMA((n,)), pltpu.SemaphoreType.DMA((n,)),
                pltpu.SemaphoreType.DMA((16,)), pltpu.SemaphoreType.DMA((16,)),
            ],
            compiler_params=pltpu.CompilerParams(collective_id=0, has_side_effects=True, vmem_limit_bytes=67043328),
            cost_estimate=pl.CostEstimate(flops=flops, bytes_accessed=4 << 20, transcendentals=0),
        )(q, keys[0, :, 0], values[0, :, 0], g)
        return (o.transpose(1, 0, 2)[None], dq.transpose(1, 0, 2)[None], dk[None, :, None], dv[None, :, None])

    return jax.shard_map(local, mesh=mesh, in_specs=(spec,) * 4, out_specs=(spec,) * 4, check_vma=False)
```

```python
import functools
import math

import jax
import jax.numpy as jnp
from jax import lax
from jax.experimental import pallas as pl
from jax.experimental.pallas import tpu as pltpu
from jax.sharding import PartitionSpec as P

MESH = pl.DeviceIdType.MESH
NEG = -1e30
HD = 128
HEADS = 5
PIECE = 128
SCALE = HD ** -0.5
LOG2E = 1.4426950408889634

FWD_TREE = "010202133103210444120443011432155552012335020504415455253342323"
BWD_TREE = "011222230313310441022204331404450555021505035314544242153135354"
BWD_ORDER = "tvlurfanb7spjm9dqehkcoi635g1428"


def popcount(value):
    return bin(value).count("1")


class Tree:
    def __init__(self, dims, links):
        blocks = 1 << dims
        if dims == 6:
            self.link = [None] + [int(d) for d in links]
        else:
            self.link = [None] * blocks
            count = [0] * dims
            for r in sorted(range(1, blocks), key=popcount):
                self.link[r] = min((d for d in range(dims) if (r >> d) & 1), key=lambda d: count[d])
                count[self.link[r]] += 1
        self.kids = {r: [k for k in range(1, blocks) if k & ~(1 << self.link[k]) == r] for r in range(blocks)}
        height = {}
        for r in sorted(range(blocks), key=popcount, reverse=True):
            height[r] = max([1 + height[k] for k in self.kids[r]], default=0)
        for r in self.kids:
            self.kids[r].sort(key=lambda k: -height[k])


class Plan:
    def __init__(self, dims):
        self.dims = dims
        self.blocks = 1 << dims
        self.fwd = Tree(dims, FWD_TREE)
        self.bwd = Tree(dims, BWD_TREE)
        self.forward()
        self.backward()

    def forward(self, block_us=2.82, hop_us=1.9, turn_us=1.0):
        free = [0.0] * self.dims
        due = {}
        done = {0}

        def send(r, now):
            for k in self.fwd.kids[r]:
                d = self.fwd.link[k]
                free[d] = max(free[d], now) + block_us
                due[k] = free[d] + hop_us

        send(0, 0.0)
        now = 1.5
        steps, waits, ready = [], [], []
        while len(done) < self.blocks or ready:
            for r in sorted((r for r in due if r not in done and due[r] <= now), key=lambda r: due[r]):
                done.add(r)
                now += 0.03
                send(r, now)
                waits.append(r)
                if r ^ 1 in done:
                    ready += [r >> 1] * (2 if r == 1 else 1)
            if ready and (0 in ready or steps):
                pair = 0 if 0 in ready else ready[0]
                ready.remove(pair)
                steps.append((waits, pair))
                waits = []
                now += turn_us
            else:
                now = max(now, min(due[r] for r in due if r not in done))
        self.fwd_steps = steps

    def backward(self, block_us=5.64, hop_us=2.0, turn_us=1.6, add_us=0.06):
        if self.dims == 6:
            order = [int(c, 32) for c in BWD_ORDER]
        else:
            order = sorted(range(1, self.blocks // 2), key=lambda pair: -popcount(pair))
        order += [0, 0]
        tree = self.bwd
        free = [0.0] * self.dims
        due = {}
        waiting = set()
        now = turn_us
        steps, sends = [], []
        position = 0
        while True:
            able = True
            while able:
                able = [r for r in waiting if all(due.get(k, 1e9) <= now for k in tree.kids[r])]
                for r in sorted(able, key=lambda r: (-popcount(r), r)):
                    waiting.discard(r)
                    now += add_us * len(tree.kids[r]) + 0.02
                    d = tree.link[r]
                    free[d] = max(free[d], now) + block_us
                    due[r] = free[d] + hop_us
                    sends.append(r)
            if position < len(order):
                pair = order[position]
                position += 1
                now += turn_us
                if pair or position == len(order):
                    waiting |= {2 * pair, 2 * pair + 1} - {0}
                steps.append((sends, pair))
                sends = []
            elif waiting:
                now = max(now, min(max(due.get(k, 1e9) for k in tree.kids[r]) for r in waiting))
            else:
                break
        self.bwd_steps = steps
        self.bwd_tail = sends


def xor(a, b):
    return a + b - 2 * a * b


def lookup(index, table):
    level = [jnp.int32(v) for v in table]
    bit = 1
    while len(level) > 1:
        odd = (index // bit) % 2 == 1
        nxt = []
        for i in range(0, len(level) - 1, 2):
            nxt.append(jnp.where(odd, level[i + 1], level[i]))
        if len(level) % 2:
            nxt.append(level[-1])
        level = nxt
        bit *= 2
    return level[0]


def branch(index, count, leaf):
    once = index // count + 1

    def pick(low, high):
        if high - low == 1:
            acts = leaf(low)
            if acts:
                pl.loop(0, once)(lambda _: [act() for act in acts] and None)
            return
        mid = (low + high) // 2
        lax.cond(index < mid, lambda: pick(low, mid), lambda: pick(mid, high))

    pick(0, count)


def kernel(plan, q_ref, k_ref, v_ref, g_ref, o_ref, dq_out, dk_out, dv_out,
           kv, stg, land, s_buf, t_buf, p_buf, d_buf, top, q_s, g_s, q_t, g_t, acc, mst, lst, dec, xacc, xm, xl, lrow, drow, lcol, dcol, dq_s, xdq,
           ag_send, ag_recv, rs_send, rs_recv, x_send, x_recv):
    dims = plan.dims
    pieces = 4 * plan.blocks
    me = lax.axis_index("ctx")
    core = me % 2
    chip = me // 2
    bits = [(chip // (1 << d)) % 2 for d in range(dims)]
    gray = [xor(bits[d], bits[d + 1]) if d % 2 == 0 and d + 1 < dims else bits[d] for d in range(dims)]
    nbr = []
    for d in range(dims):
        other = chip + (1 - 2 * bits[d]) * (1 << d)
        if d % 2:
            other = other + (1 - 2 * bits[d - 1]) * (1 << (d - 1))
        nbr.append(2 * other + core)
    mate = me + 1 - 2 * core
    my_pair = chip // 2

    barrier = pltpu.get_barrier_semaphore()
    for dev in nbr + [mate]:
        pl.semaphore_signal(barrier, inc=1, device_id={"ctx": dev}, device_id_type=MESH)

    for h in range(2):
        rows = pl.ds(h * PIECE, PIECE)
        kv[0, 0, 0, h] = k_ref[rows, :]
        kv[0, 0, 1, h] = v_ref[rows, :].T
        for head in range(HEADS):
            c = h * 10 + head
            q_s[c] = q_ref[head, rows, :]
            g_s[c] = g_ref[head, rows, :]
    mst[...] = jnp.full(mst.shape, NEG, jnp.float32)
    lst[...] = jnp.zeros(lst.shape, jnp.float32)
    acc[...] = jnp.zeros(acc.shape, jnp.float32)
    dec[...] = jnp.ones(dec.shape, jnp.float32)
    p_buf[...] = jnp.zeros(p_buf.shape, jnp.bfloat16)
    d_buf[...] = jnp.zeros(d_buf.shape, jnp.bfloat16)

    pl.semaphore_wait(barrier, dims + 1)

    def ag_copy(k):
        d = plan.fwd.link[k]
        r = k ^ (1 << d)
        return pltpu.make_async_remote_copy(
            src_ref=kv.at[r >> 1, r & 1], dst_ref=kv.at[k >> 1, k & 1], send_sem=ag_send.at[k], recv_sem=ag_recv.at[k],
            device_id={"ctx": nbr[d]}, device_id_type=MESH)

    def rs_copy(r):
        return pltpu.make_async_remote_copy(
            src_ref=stg.at[r >> 1, r & 1], dst_ref=land.at[r], send_sem=rs_send.at[r], recv_sem=rs_recv.at[r],
            device_id={"ctx": nbr[plan.bwd.link[r]]}, device_id_type=MESH)

    def mate_copy(src, dst, sem):
        return pltpu.make_async_remote_copy(src_ref=src, dst_ref=dst, send_sem=x_send.at[sem], recv_sem=x_recv.at[sem],
                                            device_id={"ctx": mate}, device_id_type=MESH)

    def own(ref, h):
        return ref.at[pl.ds(h * 10, 5)]

    def theirs(ref, h):
        return ref.at[pl.ds(h * 10 + 5, 5)]

    x_q = [mate_copy(own(ref, h), theirs(ref, h), 2 * j + h) for j, ref in enumerate((q_s, g_s)) for h in range(2)]
    for copy in x_q:
        copy.start()
    for k in plan.fwd.kids[0]:
        ag_copy(k).start()

    def ag_events(waits):
        return [act for r in waits for act in [ag_copy(r).wait_recv] + [ag_copy(k).start for k in plan.fwd.kids[r]]]

    def transposes(c):
        q_t[c] = q_s[c].T
        g_t[c] = g_s[c].T

    for h in range(2):
        pl.loop(h * 10, h * 10 + 5)(transposes)
    for copy in x_q:
        copy.wait_recv()
    for h in range(2):
        pl.loop(h * 10 + 5, h * 10 + 10)(transposes)

    def is_future(pair):
        rel = [(pair // (1 << (d - 1))) % 2 for d in range(1, dims)]
        gp = [None] + [xor(gray[d], rel[d - 1]) for d in range(1, dims)]
        other = gp[1] if dims > 1 else 0
        for d in range(2, dims):
            bit = xor(gp[d], gp[d + 1]) if d % 2 == 0 and d + 1 < dims else gp[d]
            other = other + bit * (1 << (d - 1))
        return (other - my_pair + plan.blocks) // plan.blocks

    def key_base(par, h):
        low = me if par == 0 else 2 * (chip + 1 - 2 * (chip % 2)) + core
        return (low + h * (pieces - 1 - 2 * low)) * PIECE

    def query_base(c):
        h, par = c // 10, (c // 5) % 2
        low = me + par * (mate - me)
        return (low + h * (pieces - 1 - 2 * low)) * PIECE

    def two(base0, base1, shape, axis):
        i = lax.broadcasted_iota(jnp.int32, shape, axis)
        return i + jnp.where(i < PIECE, base0, base1 - PIECE)

    coef = SCALE * LOG2E

    def key_tile(pair, h):
        return jnp.concatenate([kv[pair, 0, 0, h], kv[pair, 1, 0, h]], axis=0)

    def value_tile_t(pair, h):
        return jnp.concatenate([kv[pair, 0, 1, h], kv[pair, 1, 1, h]], axis=1)

    def wide(ref, c):
        return jnp.concatenate([ref[c], ref[c + 1]], axis=1)

    def tall(ref, c):
        return jnp.concatenate([ref[c], ref[c + 1]], axis=0)

    def rows(slot, t):
        return pl.ds((slot * HEADS + t) * 256, 256)

    def place(pair, own_turn):
        mine = (half_pairs - pair) // half_pairs
        fut = is_future(pair)
        return (pair,) + tuple(
            part for slot in range(2)
            for part in (mine * own_turn + (1 - mine) * fut * slot, mine * slot + (1 - mine) * (fut + (1 - fut) * slot)))

    half_pairs = plan.blocks // 2

    def groups(turn):
        return tuple((slot, turn[0], turn[1 + 2 * slot], turn[2 + 2 * slot]) for slot in range(2))

    def mask_scores(turn, keys_axis):
        h = turn[1]

        @pl.loop(0, HEADS * (1 + h))
        def _(t):
            c = 2 * t
            shape = (256, 256)
            kpos = two(key_base(0, h), key_base(1, h), shape, keys_axis)
            qpos = two(query_base(c), query_base(c + 1), shape, 1 - keys_axis)
            s = jnp.where(qpos >= kpos, s_buf[t], NEG)
            s_buf[t] = s
            if keys_axis == 0:
                top[t] = jnp.max(s.reshape(32, 8, 256), axis=0)

    def fwd_scores(turn, some=range(10)):
        for slot, pair, h, qg in groups(turn):
            kt = key_tile(pair, h)
            for t in range(HEADS):
                if slot * HEADS + t not in some:
                    continue
                s = jnp.dot(kt, wide(q_t, qg * 10 + 2 * t), preferred_element_type=jnp.float32)
                s_buf[slot * HEADS + t] = s
                top[slot * HEADS + t] = jnp.max(s.reshape(32, 8, 256), axis=0)

    def fwd_softmax(turn, some):
        for slot, _, _, qg in groups(turn):
            for t in range(HEADS):
                b = slot * HEADS + t
                if b not in some:
                    continue
                c = qg * 10 + 2 * t
                m_old = wide(mst, c)
                m_new = jnp.maximum(m_old, jnp.max(top[b], axis=0, keepdims=True) * coef)
                p = jnp.exp2(s_buf[b] * coef - m_new[0:1])
                decay = jnp.exp2(m_old - m_new)
                l_new = wide(lst, c) * decay + jnp.sum(p.reshape(32, 8, 256), axis=0)
                p_buf[rows(slot, t), :] = p.astype(jnp.bfloat16)
                dec[b] = decay
                for j in range(2):
                    cols = slice(j * 128, j * 128 + 128)
                    mst[c + j] = m_new[:, cols]
                    lst[c + j] = l_new[:, cols]

    def fwd_out(turn, some=range(10)):
        for slot, pair, h, qg in groups(turn):
            vt = value_tile_t(pair, h)
            for t in range(HEADS):
                if slot * HEADS + t not in some:
                    continue
                c = qg * 10 + 2 * t
                pv = jnp.dot(vt, p_buf[rows(slot, t), :], preferred_element_type=jnp.float32)
                for j in range(2):
                    cols = slice(j * 128, j * 128 + 128)
                    acc[c + j] = acc[c + j] * dec[slot * HEADS + t, 0:1, cols] + pv[:, cols]

    turns = len(plan.fwd_steps)
    fwd_waits = [waits for waits, _ in plan.fwd_steps]
    fwd_pairs = [pair for _, pair in plan.fwd_steps]

    def fwd_place(j):
        return place(lookup(jnp.minimum(j, turns - 1), fwd_pairs), jnp.minimum(j, 1))

    for act in ag_events(fwd_waits[0]):
        act()
    first = fwd_place(me * 0)
    fwd_scores(first)

    def fwd_turn(j, carry):
        old, cur = carry
        branch(j, turns, lambda i: ag_events(fwd_waits[i + 1]) if i + 1 < turns else [])
        new = fwd_place(j + 1)

        @pl.when(j < 2)
        def _():
            mask_scores(cur, 0)

        for b in range(12):
            fwd_out(old, (b,))
            fwd_softmax(cur, (b - 1,))
            fwd_scores(new, (b - 2,))
        return cur, new

    last = lax.fori_loop(0, turns, fwd_turn, (first, first))[0]
    fwd_out(last)

    def bwd_scores(turn, some=range(10)):
        for slot, pair, h, qg in groups(turn):
            kt = key_tile(pair, h)
            vt = value_tile_t(pair, h)
            for t in range(HEADS):
                if slot * HEADS + t not in some:
                    continue
                c = qg * 10 + 2 * t
                s_buf[slot * HEADS + t] = lax.dot_general(tall(q_s, c), kt, (((1,), (1,)), ((), ())),
                                                          preferred_element_type=jnp.float32)
                t_buf[slot * HEADS + t] = jnp.dot(tall(g_s, c), vt, preferred_element_type=jnp.float32)

    def bwd_softmax(turn, some):
        for slot, _, _, qg in groups(turn):
            for t in range(HEADS):
                b = slot * HEADS + t
                if b not in some:
                    continue
                c = qg * 10 + 2 * t
                lse, dr = tall(lcol, c), tall(dcol, c)
                p = jnp.exp2(s_buf[b] * coef - jnp.concatenate([lse, lse], axis=1))
                p_buf[rows(slot, t), :] = p.astype(jnp.bfloat16)
                d_buf[rows(slot, t), :] = (p * (t_buf[b] - jnp.concatenate([dr, dr], axis=1))).astype(jnp.bfloat16)

    def bwd_out(turn, some=range(10), sums=None):
        sums = {} if sums is None else sums
        for slot, pair, h, qg in groups(turn):
            kt = key_tile(pair, h)
            for t in range(HEADS):
                if slot * HEADS + t not in some:
                    continue
                c = qg * 10 + 2 * t
                ds = d_buf[rows(slot, t), :]
                for j, (ref, buf) in enumerate(((q_t, ds), (g_t, p_buf[rows(slot, t), :]))):
                    grad = jnp.dot(wide(ref, c), buf, preferred_element_type=jnp.float32)
                    sums[j] = sums[j] + grad if t else grad
                    for par in range(2 if t == HEADS - 1 else 0):
                        stg[pair, par, j, h] += sums[j][:, par * 128:par * 128 + 128]
                dq = lax.dot_general(kt, ds, (((0,), (1,)), ((), ())), preferred_element_type=jnp.float32)
                for j in range(2):
                    dq_s[c + j] += dq[:, j * 128:j * 128 + 128]
        return sums

    bwd_pairs = [pair for _, pair in plan.bwd_steps]
    sends_at = [sends for sends, _ in plan.bwd_steps]

    def bwd_place(j):
        return place(lookup(jnp.minimum(j, turns - 1), bwd_pairs), jnp.maximum(j - (turns - 2), 0) - jnp.maximum(j - (turns - 1), 0))

    x_m = []
    for h in range(2):
        inbox = pl.ds(h * 5, 5)
        x_m += [mate_copy(theirs(acc, h), xacc.at[inbox], 4 + 3 * h), mate_copy(theirs(mst, h), xm.at[inbox], 5 + 3 * h),
                mate_copy(theirs(lst, h), xl.at[inbox], 6 + 3 * h)]
    for copy in x_m:
        copy.start()
    p_buf[...] = jnp.zeros(p_buf.shape, jnp.bfloat16)
    dq_s[...] = jnp.zeros(dq_s.shape, jnp.float32)
    first = bwd_place(me * 0)
    bwd_scores(first)
    x_r = [mate_copy(own(ref, h), theirs(ref, h), 10 + 2 * j + h) for j, ref in enumerate((lrow, drow)) for h in range(2)]

    for h in range(2):
        for copy in x_m[3 * h:3 * h + 3]:
            copy.wait_recv()
        for head in range(HEADS):
            c, x = h * 10 + head, h * 5 + head
            m1, m2 = mst[c], xm[x]
            m = jnp.maximum(m1, m2)
            w1, w2 = jnp.exp2(m1 - m), jnp.exp2(m2 - m)
            total = jnp.sum(lst[c] * w1 + xl[x] * w2, axis=0, keepdims=True)
            out = (acc[c] * w1[0:1] + xacc[x] * w2[0:1]) / total
            low = out.astype(jnp.bfloat16)
            o_ref[head, pl.ds(h * PIECE, PIECE), :] = out.T.astype(jnp.bfloat16)
            lrow[c] = m + jnp.log2(total)
            d = jnp.sum(low.astype(jnp.float32) * g_t[c].astype(jnp.float32), axis=0, keepdims=True)
            drow[c] = jnp.broadcast_to(d, (8, 128))
    for copy in x_r:
        copy.start()

    def columns(c):
        lcol[c] = jnp.broadcast_to(lrow[c, 0:1], (128, 128)).T
        dcol[c] = jnp.broadcast_to(drow[c, 0:1], (128, 128)).T

    for h in range(2):
        pl.loop(h * 10, h * 10 + 5)(columns)
    for copy in x_r:
        copy.wait_recv()
    for h in range(2):
        pl.loop(h * 10 + 5, h * 10 + 10)(columns)

    def rs_add(r, k):
        rs_copy(k).wait_recv()
        for j in range(4):
            stg[r >> 1, r & 1, j // 2, j % 2] += land[k, j // 2, j % 2]

    def rs_events(sends):
        return [functools.partial(rs_add, r, k) for r in sends for k in plan.bwd.kids[r]] + [rs_copy(r).start for r in sends]

    def clear(pair):
        for par in range(2):
            for j in range(4):
                stg[pair, par, j // 2, j % 2] = jnp.zeros((128, 128), jnp.float32)

    def bwd_turn(j, carry):
        old, cur = carry
        branch(j, turns, lambda i: rs_events(sends_at[i - 1]) if i else [])
        new = bwd_place(j + 1)

        @pl.when((j > 0) & (j < turns))
        def _():
            clear(old[0])

        @pl.when(j >= turns - 2)
        def _():
            mask_scores(cur, 1)

        sums = {}
        for b in range(12):
            sums = bwd_out(old, (b,), sums)
            bwd_softmax(cur, (b - 1,))
            bwd_scores(new, (b - 2,))
        return cur, new

    last = lax.fori_loop(0, turns, bwd_turn, (first, first))[0]
    for act in rs_events(sends_at[turns - 1]):
        act()
    bwd_out(last)

    x_d = [mate_copy(theirs(dq_s, h), xdq.at[pl.ds(h * 5, 5)], 14 + h) for h in range(2)]
    for copy in x_d:
        copy.start()
    for r in plan.bwd_tail:
        for act in rs_events([r]):
            act()
    for h in range(2):
        x_d[h].wait_recv()
        for head in range(HEADS):
            total = (dq_s[h * 10 + head] + xdq[h * 5 + head]) * SCALE
            dq_out[head, pl.ds(h * PIECE, PIECE), :] = total.T.astype(jnp.bfloat16)
    for k in plan.bwd.kids[0]:
        rs_copy(k).wait_recv()
    for h in range(2):
        for j, ref in enumerate((dk_out, dv_out)):
            total = stg[0, 0, j, h]
            for k in plan.bwd.kids[0]:
                total = total + land[k, j, h]
            if j == 0:
                total = total * SCALE
            ref[pl.ds(h * PIECE, PIECE), :] = total.T.astype(jnp.bfloat16)

    for k in range(1, plan.blocks):
        ag_copy(k).wait_send()
        rs_copy(k).wait_send()
    for copy in x_q + x_m + x_r + x_d:
        copy.wait_send()


def solution(mesh):
    size = mesh.shape["ctx"]
    plan = Plan(int(math.log2(size)) - 1)
    spec = P("data", "ctx", None, None)
    n = plan.blocks
    f32, bf16 = jnp.float32, jnp.bfloat16
    vm = pltpu.VMEM

    def local(queries, keys, values, grad_out):
        tokens = queries.shape[1]
        q = queries[0].transpose(1, 0, 2)
        g = grad_out[0].transpose(1, 0, 2)
        tile = (128, 128)
        big = jax.ShapeDtypeStruct((HEADS, tokens, HD), bf16)
        small = jax.ShapeDtypeStruct((tokens, HD), bf16)
        flops = 14 * 640 * PIECE * n * 2 * HD
        o, dq, dk, dv = pl.pallas_call(
            functools.partial(kernel, plan),
            out_shape=(big, big, small, small),
            in_specs=[pl.BlockSpec(memory_space=vm)] * 4,
            out_specs=(pl.BlockSpec(memory_space=vm),) * 4,
            scratch_shapes=[
                vm((n // 2, 2, 2, 2) + tile, bf16),
                vm((n // 2, 2, 2, 2) + tile, f32),
                vm((n, 2, 2) + tile, f32),
                vm((10, 256, 256), f32), vm((10, 256, 256), f32), vm((2560, 256), bf16), vm((2560, 256), bf16), vm((10, 8, 256), f32),
                vm((20,) + tile, bf16), vm((20,) + tile, bf16), vm((20,) + tile, bf16), vm((20,) + tile, bf16),
                vm((20,) + tile, f32), vm((20, 8, 128), f32), vm((20, 8, 128), f32), vm((10, 8, 256), f32),
                vm((10,) + tile, f32), vm((10, 8, 128), f32), vm((10, 8, 128), f32),
                vm((20, 8, 128), f32), vm((20, 8, 128), f32),
                vm((20,) + tile, f32), vm((20,) + tile, f32),
                vm((20,) + tile, f32), vm((10,) + tile, f32),
                pltpu.SemaphoreType.DMA((n,)), pltpu.SemaphoreType.DMA((n,)),
                pltpu.SemaphoreType.DMA((n,)), pltpu.SemaphoreType.DMA((n,)),
                pltpu.SemaphoreType.DMA((16,)), pltpu.SemaphoreType.DMA((16,)),
            ],
            compiler_params=pltpu.CompilerParams(collective_id=0, has_side_effects=True, vmem_limit_bytes=67043328),
            cost_estimate=pl.CostEstimate(flops=flops, bytes_accessed=4 << 20, transcendentals=0),
        )(q, keys[0, :, 0], values[0, :, 0], g)
        return (o.transpose(1, 0, 2)[None], dq.transpose(1, 0, 2)[None], dk[None, :, None], dv[None, :, None])

    return jax.shard_map(local, mesh=mesh, in_specs=(spec,) * 4, out_specs=(spec,) * 4, check_vma=False)
```

```python
import functools
import math

import jax
import jax.numpy as jnp
from jax import lax
from jax.experimental import pallas as pl
from jax.experimental.pallas import tpu as pltpu
from jax.sharding import PartitionSpec as P

MESH = pl.DeviceIdType.MESH
NEG = -1e30
HD = 128
HEADS = 5
PIECE = 128
SCALE = HD ** -0.5
LOG2E = 1.4426950408889634
TILES = 2 * HEADS

KEY_TREE = "011221033303230444022204041233350552225555023554414241430104552"
VALUE_TREE = "010201133132030404124203411303055112015353553124445242153504414"
DK_TREE = "011201030113022404042143013424255155512503350504044245135103424"
DV_TREE = "011222133313022444124423431243055505220331030555415254133515214"
BWD_ORDER = "vlruetqkfpndmjbs7h9c56i34o8ag21"


def popcount(value):
    return bin(value).count("1")


class Tree:
    def __init__(self, dims, links):
        blocks = 1 << dims
        if dims == 6:
            self.link = [None] + [int(d) for d in links]
        else:
            self.link = [None] * blocks
            count = [0] * dims
            for r in sorted(range(1, blocks), key=popcount):
                self.link[r] = min((d for d in range(dims) if (r >> d) & 1), key=lambda d: count[d])
                count[self.link[r]] += 1
        self.kids = {r: [k for k in range(1, blocks) if k & ~(1 << self.link[k]) == r] for r in range(blocks)}
        height = {}
        for r in sorted(range(blocks), key=popcount, reverse=True):
            height[r] = max([1 + height[k] for k in self.kids[r]], default=0)
        for r in self.kids:
            self.kids[r].sort(key=lambda k: -height[k])


class Plan:
    def __init__(self, dims):
        self.dims = dims
        self.blocks = 1 << dims
        self.turns = self.blocks // 2 + 1
        self.fwd = [Tree(dims, KEY_TREE), Tree(dims, VALUE_TREE)]
        self.bwd = [Tree(dims, DK_TREE), Tree(dims, DV_TREE)]
        self.forward()
        self.backward()

    def forward(self, unit_us=1.41, hop_us=1.9, turn_us=0.85):
        free = [0.0] * self.dims
        due = {}
        done = {(0, 0), (0, 1)}
        now = 1.0
        steps, waits, ready, order = [], [], [0], []

        def send(r, x):
            for k in self.fwd[x].kids[r]:
                d = self.fwd[x].link[k]
                free[d] = max(free[d], now) + unit_us
                due[k, x] = free[d] + hop_us

        now = 0.0
        send(0, 0)
        send(0, 1)
        now = 1.0
        while True:
            for unit in sorted((u for u in due if u not in done and due[u] <= now), key=lambda u: (due[u], u)):
                done.add(unit)
                now += 0.02
                send(*unit)
                waits.append(unit)
                if unit[1] == 0 and (unit[0] ^ 1, 0) in done:
                    ready.append(unit[0] >> 1)
            turn = len(steps)
            late = order[max(turn - 2, 0):turn - 1] if turn < self.turns else order[turn - 2:]
            lacking = [r for pair in late for r in (2 * pair, 2 * pair + 1) if (r, 1) not in done]
            if turn == 2 < self.turns:
                lacking = []
            if lacking or not (ready or turn == self.turns):
                now = max(now, min(due[u] for u in due if u not in done))
                continue
            if turn == self.turns:
                break
            order.append(ready.pop(0))
            steps.append(waits)
            waits = []
            now += turn_us if turn else 0.0
        self.fwd_waits = steps + [waits]
        self.fwd_pairs = order
        self.fwd_mate = max(i for i, pair in enumerate(order) if pair == 0)

    def backward(self, unit_us=2.82, hop_us=2.0, turn_us=1.6, add_us=0.03):
        if self.dims == 6:
            order = [int(c, 32) for c in BWD_ORDER]
        else:
            order = sorted(range(1, self.blocks // 2), key=lambda pair: -popcount(pair))
        order += [0, 0]
        free = [0.0] * self.dims
        due = {}
        waiting = set()
        now = turn_us
        steps, sends = [], []
        position = 0

        def kids(unit):
            return [(k, unit[1]) for k in self.bwd[unit[1]].kids[unit[0]]]

        while True:
            able = True
            while able:
                able = [u for u in waiting if all(due.get(k, 1e9) <= now for k in kids(u))]
                for unit in sorted(able, key=lambda u: (-popcount(u[0]), u)):
                    waiting.discard(unit)
                    now += add_us * len(kids(unit)) + 0.01
                    d = self.bwd[unit[1]].link[unit[0]]
                    free[d] = max(free[d], now) + unit_us
                    due[unit] = free[d] + hop_us
                    sends.append(unit)
            if position < len(order):
                pair = order[position]
                position += 1
                now += turn_us
                if pair:
                    waiting |= {(2 * pair + i, x) for i in range(2) for x in range(2)}
                elif position < len(order):
                    waiting |= {(1, 0), (1, 1)}
                steps.append(sends)
                sends = []
            elif waiting:
                now = max(now, min(max(due.get(k, 1e9) for k in kids(u)) for u in waiting))
            else:
                break
        self.bwd_sends = steps + [sends]
        self.bwd_pairs = order
        self.bwd_last = sorted((u for x in range(2) for u in kids((0, x))), key=lambda u: due[u])


def xor(a, b):
    return a + b - 2 * a * b


def lookup(index, table):
    level = [jnp.int32(v) for v in table]
    bit = 1
    while len(level) > 1:
        odd = (index // bit) % 2 == 1
        nxt = [jnp.where(odd, level[i + 1], level[i]) for i in range(0, len(level) - 1, 2)]
        level = nxt + level[2 * len(nxt):]
        bit *= 2
    return level[0]


def branch(index, count, leaf):
    once = index // count + 1

    def pick(low, high):
        if high - low == 1:
            acts = leaf(low)
            if acts:
                pl.loop(0, once)(lambda _: [act() for act in acts] and None)
            return
        mid = (low + high) // 2
        lax.cond(index < mid, lambda: pick(low, mid), lambda: pick(mid, high))

    pick(0, count)


def kernel(plan, q_ref, k_ref, v_ref, g_ref, o_ref, dq_ref, dk_ref, dv_ref,
           kv, stg, land, s_buf, t_buf, p_buf, d_buf, top, q_s, g_s, v_s, q_t, g_t, c_t, acc, mst, lst, dec,
           xacc, xm, xl, lrow, drow, lcol, dcol, dq_s, xdq, o_s, dq_o, dk_o, dv_o,
           ag_send, ag_recv, rs_send, rs_recv, x_send, x_recv, io):
    dims, turns = plan.dims, plan.turns
    pieces = 4 * plan.blocks
    f32, bf16 = jnp.float32, jnp.bfloat16
    me = lax.axis_index("ctx")
    core = me % 2
    chip = me // 2
    bits = [(chip // (1 << d)) % 2 for d in range(dims)]
    gray = [xor(bits[d], bits[d + 1]) if d % 2 == 0 and d + 1 < dims else bits[d] for d in range(dims)]
    nbr = []
    for d in range(dims):
        other = chip + (1 - 2 * bits[d]) * (1 << d)
        if d % 2:
            other = other + (1 - 2 * bits[d - 1]) * (1 << (d - 1))
        nbr.append(2 * other + core)
    mate = me + 1 - 2 * core
    my_pair = chip // 2

    barrier = pltpu.get_barrier_semaphore()
    for dev in nbr + [mate]:
        pl.semaphore_signal(barrier, inc=1, device_id={"ctx": dev}, device_id_type=MESH)

    def half(h):
        return pl.ds(h * PIECE, PIECE)

    loads = []
    for h in range(2):
        loads += [pltpu.make_async_copy(v_ref.at[half(h)], v_s.at[h], io.at[h]),
                  pltpu.make_async_copy(k_ref.at[half(h)], kv.at[0, 0, 0, h], io.at[2 + h])]
    for h in range(2):
        for j, (src, dst) in enumerate(((q_ref, q_s), (g_ref, g_s))):
            loads.append(pltpu.make_async_copy(src.at[:, half(h)], dst.at[pl.ds(h * TILES, HEADS)], io.at[4 + 2 * j + h]))
    for copy in loads:
        copy.start()
    mst[...] = jnp.full(mst.shape, NEG, f32)
    lst[...] = jnp.zeros(lst.shape, f32)
    acc[...] = jnp.zeros(acc.shape, f32)
    dec[...] = jnp.ones(dec.shape, f32)
    p_buf[...] = jnp.zeros(p_buf.shape, bf16)
    for copy in loads[:4]:
        copy.wait()
    for h in range(2):
        kv[0, 0, 1, h] = v_s[h].T

    pl.semaphore_wait(barrier, dims + 1)

    def ag_copy(k, x):
        d = plan.fwd[x].link[k]
        r = k ^ (1 << d)
        return pltpu.make_async_remote_copy(
            src_ref=kv.at[r >> 1, r & 1, x], dst_ref=kv.at[k >> 1, k & 1, x], send_sem=ag_send.at[k, x],
            recv_sem=ag_recv.at[k, x], device_id={"ctx": nbr[d]}, device_id_type=MESH)

    def rs_copy(r, x):
        return pltpu.make_async_remote_copy(
            src_ref=stg.at[r >> 1, r & 1, x], dst_ref=land.at[r, x], send_sem=rs_send.at[r, x], recv_sem=rs_recv.at[r, x],
            device_id={"ctx": nbr[plan.bwd[x].link[r]]}, device_id_type=MESH)

    def mate_copy(src, dst, sem):
        return pltpu.make_async_remote_copy(src_ref=src, dst_ref=dst, send_sem=x_send.at[sem], recv_sem=x_recv.at[sem],
                                            device_id={"ctx": mate}, device_id_type=MESH)

    def own(ref, h):
        return ref.at[pl.ds(h * TILES, HEADS)]

    def theirs(ref, h):
        return ref.at[pl.ds(h * TILES + HEADS, HEADS)]

    for x in range(2):
        for k in plan.fwd[x].kids[0]:
            ag_copy(k, x).start()
    for copy in loads[4:]:
        copy.wait()
    x_q = [mate_copy(own(ref, h), theirs(ref, h), 2 * j + h) for j, ref in enumerate((q_s, g_s)) for h in range(2)]
    for copy in x_q:
        copy.start()

    def ag_events(waits):
        return [act for r, x in waits for act in [ag_copy(r, x).wait_recv] + [ag_copy(k, x).start for k in plan.fwd[x].kids[r]]]

    coef = SCALE * LOG2E

    def transposes(c):
        turned = q_s[c].T
        q_t[c] = turned
        g_t[c] = g_s[c].T
        scaled = turned.astype(f32) * coef
        high = scaled.astype(bf16)
        c_t[c, 0] = high
        c_t[c, 1] = (scaled - high.astype(f32)).astype(bf16)

    for h in range(2):
        pl.loop(h * TILES, h * TILES + HEADS)(transposes)
    for copy in x_q:
        copy.wait_recv()
    for h in range(2):
        pl.loop(h * TILES + HEADS, h * TILES + TILES)(transposes)

    def is_future(pair):
        rel = [(pair // (1 << (d - 1))) % 2 for d in range(1, dims)]
        gp = [None] + [xor(gray[d], rel[d - 1]) for d in range(1, dims)]
        other = gp[1] if dims > 1 else 0
        for d in range(2, dims):
            bit = xor(gp[d], gp[d + 1]) if d % 2 == 0 and d + 1 < dims else gp[d]
            other = other + bit * (1 << (d - 1))
        return (other - my_pair + plan.blocks) // plan.blocks

    def place(pair, a):
        mine = (plan.blocks // 2 - pair) // (plan.blocks // 2)
        fut = is_future(pair)
        turn = (pair,)
        for slot in range(2):
            h = (1 - mine) * fut * slot
            turn += (mine * a, h, mine * a + 1 - mine, mine + h, mine * slot + (1 - mine) * (fut + (1 - fut) * slot))
        return turn

    def groups(turn):
        for slot in range(2):
            p0, h0, p1, h1, qg = turn[1 + 5 * slot:6 + 5 * slot]
            yield slot, ((turn[0], p0, h0), (turn[0], p1, h1)), qg * TILES

    def key_tile(where):
        return jnp.concatenate([kv[pair, par, 0, h] for pair, par, h in where], axis=0)

    def value_tile_t(where):
        return jnp.concatenate([kv[pair, par, 1, h] for pair, par, h in where], axis=1)

    def wide(ref, c):
        return jnp.concatenate([ref[c], ref[c + 1]], axis=1)

    def tall(ref, c):
        return jnp.concatenate([ref[c], ref[c + 1]], axis=0)

    def rows(b):
        return pl.ds(b * 256, 256)

    def mask_scores(a, keys_axis):
        key_low = me + a * (2 * (1 - 2 * (chip % 2)))

        def two(base0, base1, axis):
            i = lax.broadcasted_iota(jnp.int32, (256, 256), axis)
            return i + jnp.where(i < PIECE, base0, base1 - PIECE)

        def query_base(c):
            h, par = c // TILES, (c // HEADS) % 2
            low = me + par * (mate - me)
            return (low + h * (pieces - 1 - 2 * low)) * PIECE

        @pl.loop(0, TILES)
        def _(b):
            kpos = two(key_low * PIECE, (pieces - 1 - key_low) * PIECE, keys_axis)
            qpos = two(query_base(2 * b), query_base(2 * b + 1), 1 - keys_axis)
            s = jnp.where(qpos >= kpos, s_buf[b], NEG)
            s_buf[b] = s
            if keys_axis == 0:
                top[b] = jnp.max(s.reshape(32, 8, 256), axis=0)

    def fwd_scores(turn, some=range(TILES)):
        for slot, where, base in groups(turn):
            kt = key_tile(where)
            twice = jnp.concatenate([kt, kt], axis=1)
            for t in range(HEADS):
                b, c = slot * HEADS + t, base + 2 * t
                if b in some:
                    scaled = jnp.concatenate([wide(c_t.at[:, i], c) for i in range(2)], axis=0)
                    s = jnp.dot(twice, scaled, preferred_element_type=f32)
                    s_buf[b] = s
                    top[b] = jnp.max(s.reshape(32, 8, 256), axis=0)

    def fwd_softmax(turn, some):
        for slot, _, base in groups(turn):
            for t in range(HEADS):
                b, c = slot * HEADS + t, base + 2 * t
                if b not in some:
                    continue
                m_old = wide(mst, c)
                m_new = jnp.maximum(m_old, jnp.max(top[b], axis=0, keepdims=True))
                p = jnp.exp2(s_buf[b] - m_new[0:1])
                decay = jnp.exp2(m_old - m_new)
                l_new = wide(lst, c) * decay + jnp.sum(p.reshape(32, 8, 256), axis=0)
                p_buf[rows(b), :] = p.astype(bf16)
                dec[b] = decay
                for j in range(2):
                    cols = slice(j * 128, j * 128 + 128)
                    mst[c + j] = m_new[:, cols]
                    lst[c + j] = l_new[:, cols]

    def fwd_out(turn, some=range(TILES)):
        for slot, where, base in groups(turn):
            vt = value_tile_t(where)
            for t in range(HEADS):
                b, c = slot * HEADS + t, base + 2 * t
                if b in some:
                    pv = jnp.dot(vt, p_buf[rows(b), :], preferred_element_type=f32)
                    for j in range(2):
                        cols = slice(j * 128, j * 128 + 128)
                        acc[c + j] = acc[c + j] * dec[b, 0:1, cols] + pv[:, cols]

    def fwd_place(j):
        return place(lookup(jnp.minimum(j, turns - 1), plan.fwd_pairs), jnp.minimum(j, 1))

    for act in ag_events(plan.fwd_waits[0]):
        act()
    first = fwd_place(me * 0)
    fwd_scores(first)

    def fwd_turn(j, carry):
        old, cur = carry
        branch(j, turns, lambda i: ag_events(plan.fwd_waits[i + 1]))
        new = fwd_place(j + 1)

        @pl.when((j == 0) | (j == plan.fwd_mate))
        def _():
            mask_scores(jnp.minimum(j, 1), 0)

        for b in range(TILES + 2):
            fwd_scores(new, (b - 2,))
            fwd_softmax(cur, (b - 1,))
            fwd_out(old, (b,))
        return cur, new

    last = lax.fori_loop(0, turns, fwd_turn, (first, first))[0]
    fwd_out(last)

    def bwd_scores(turn, some=range(TILES)):
        for slot, where, base in groups(turn):
            kt, vt = key_tile(where), value_tile_t(where)
            for t in range(HEADS):
                b, c = slot * HEADS + t, base + 2 * t
                if b in some:
                    s_buf[b] = lax.dot_general(tall(q_s, c), kt, (((1,), (1,)), ((), ())), preferred_element_type=f32)
                    t_buf[b] = jnp.dot(tall(g_s, c), vt, preferred_element_type=f32)

    def bwd_softmax(turn, some):
        for slot, _, base in groups(turn):
            for t in range(HEADS):
                b, c = slot * HEADS + t, base + 2 * t
                if b in some:
                    lse, dr = tall(lcol, c), tall(dcol, c)
                    p = jnp.exp2(s_buf[b] * coef - jnp.concatenate([lse, lse], axis=1))
                    p_buf[rows(b), :] = p.astype(bf16)
                    d_buf[rows(b), :] = (p * (t_buf[b] - jnp.concatenate([dr, dr], axis=1))).astype(bf16)

    def bwd_out(turn, sums, some=range(TILES)):
        for slot, where, base in groups(turn):
            kt = key_tile(where)
            for t in range(HEADS):
                b, c = slot * HEADS + t, base + 2 * t
                if b not in some:
                    continue
                ds = d_buf[rows(b), :]
                for x, (ref, buf) in enumerate(((q_t, ds), (g_t, p_buf[rows(b), :]))):
                    grad = jnp.dot(wide(ref, c), buf, preferred_element_type=f32)
                    sums[x] = sums[x] + grad if t else grad
                    for j, (pair, par, h) in enumerate(where if t == HEADS - 1 else ()):
                        stg[pair, par, x, h] += sums[x][:, j * 128:j * 128 + 128]
                dq = lax.dot_general(kt, ds, (((0,), (1,)), ((), ())), preferred_element_type=f32)
                for j in range(2):
                    dq_s[c + j] += dq[:, j * 128:j * 128 + 128]

    def bwd_place(j):
        at = jnp.minimum(j, turns - 1)
        return place(lookup(at, plan.bwd_pairs), 1 - (at + 1) // turns)

    x_m = []
    for h in range(2):
        inbox = pl.ds(h * HEADS, HEADS)
        x_m += [mate_copy(theirs(ref, h), box.at[inbox], 4 + 3 * h + i)
                for i, (ref, box) in enumerate(((acc, xacc), (mst, xm), (lst, xl)))]
    for copy in x_m:
        copy.start()
    first = bwd_place(me * 0)
    bwd_scores(first)
    p_buf[...] = jnp.zeros(p_buf.shape, bf16)
    d_buf[...] = jnp.zeros(d_buf.shape, bf16)
    dq_s[...] = jnp.zeros(dq_s.shape, f32)
    x_r = [mate_copy(own(ref, h), theirs(ref, h), 10 + 2 * j + h) for j, ref in enumerate((lrow, drow)) for h in range(2)]

    for h in range(2):
        for copy in x_m[3 * h:3 * h + 3]:
            copy.wait_recv()
        for head in range(HEADS):
            c, i = h * TILES + head, h * HEADS + head
            m1, m2 = mst[c], xm[i]
            m = jnp.maximum(m1, m2)
            w1, w2 = jnp.exp2(m1 - m), jnp.exp2(m2 - m)
            total = jnp.sum(lst[c] * w1 + xl[i] * w2, axis=0, keepdims=True)
            out = (acc[c] * w1[0:1] + xacc[i] * w2[0:1]) / total
            o_s[head, half(h), :] = out.T.astype(bf16)
            lrow[c] = m + jnp.log2(total)
            rounded = out.astype(bf16).astype(f32)
            drow[c] = jnp.broadcast_to(jnp.sum(rounded * g_t[c].astype(f32), axis=0, keepdims=True), (8, 128))
    for copy in x_r:
        copy.start()
    stores = [pltpu.make_async_copy(o_s, o_ref, io.at[8])]
    stores[0].start()

    def columns(c):
        lcol[c] = jnp.broadcast_to(lrow[c, 0:1], (128, 128)).T
        dcol[c] = jnp.broadcast_to(drow[c, 0:1], (128, 128)).T

    for h in range(2):
        pl.loop(h * TILES, h * TILES + HEADS)(columns)
    for copy in x_r:
        copy.wait_recv()
    for h in range(2):
        pl.loop(h * TILES + HEADS, h * TILES + TILES)(columns)

    def rs_add(r, k, x):
        rs_copy(k, x).wait_recv()
        for h in range(2):
            stg[r >> 1, r & 1, x, h] += land[k, x, h]

    def rs_events(sends):
        return ([functools.partial(rs_add, r, k, x) for r, x in sends for k in plan.bwd[x].kids[r]]
                + [rs_copy(r, x).start for r, x in sends])

    def clear(pair):
        for i in range(8):
            stg[pair, i // 4, i // 2 % 2, i % 2] = jnp.zeros((128, 128), f32)

    def bwd_turn(j, carry):
        old, cur = carry
        branch(j, turns, lambda i: rs_events(plan.bwd_sends[i - 1]) if i else [])
        new = bwd_place(j + 1)

        @pl.when((j > 0) & (j < turns))
        def _():
            clear(old[0])

        @pl.when(j >= turns - 2)
        def _():
            mask_scores(turns - 1 - j, 1)

        sums = {}
        for b in range(TILES + 2):
            bwd_out(old, sums, (b,))
            bwd_softmax(cur, (b - 1,))
            bwd_scores(new, (b - 2,))
        return cur, new

    last = lax.fori_loop(0, turns, bwd_turn, (first, first))[0]
    for act in rs_events(plan.bwd_sends[turns - 1]):
        act()
    bwd_out(last, {})

    x_d = [mate_copy(theirs(dq_s, h), xdq.at[pl.ds(h * HEADS, HEADS)], 14 + h) for h in range(2)]
    for copy in x_d:
        copy.start()
    for unit in plan.bwd_sends[turns]:
        for act in rs_events([unit]):
            act()
    for h in range(2):
        x_d[h].wait_recv()
        for head in range(HEADS):
            total = (dq_s[h * TILES + head] + xdq[h * HEADS + head]) * SCALE
            dq_o[head, half(h), :] = total.T.astype(bf16)
    stores.append(pltpu.make_async_copy(dq_o, dq_ref, io.at[9]))
    stores[1].start()
    for k, x in plan.bwd_last:
        rs_add(0, k, x)
    for x, (buf, ref, factor) in enumerate(((dk_o, dk_ref, SCALE), (dv_o, dv_ref, 1.0))):
        for h in range(2):
            buf[half(h), :] = (stg[0, 0, x, h] * factor).T.astype(bf16)
        stores.append(pltpu.make_async_copy(buf, ref, io.at[10 + x]))
        stores[-1].start()

    for k in range(1, plan.blocks):
        for x in range(2):
            ag_copy(k, x).wait_send()
            rs_copy(k, x).wait_send()
    for copy in x_q + x_m + x_r + x_d:
        copy.wait_send()
    for copy in stores:
        copy.wait()


def relay(*refs):
    count = (len(refs) - 1) // 3
    src, dst, buf, sem = refs[:count], refs[count:2 * count], refs[2 * count:3 * count], refs[3 * count]
    into = [pltpu.make_async_copy(a, b, sem.at[i]) for i, (a, b) in enumerate(zip(src, buf))]
    out = [pltpu.make_async_copy(b, c, sem.at[count + i]) for i, (b, c) in enumerate(zip(buf, dst))]
    for copy in into:
        copy.start()
    for i in range(count):
        into[i].wait()
        out[i].start()
    for copy in out:
        copy.wait()


def solution(mesh):
    size = mesh.shape["ctx"]
    plan = Plan(int(math.log2(size)) - 1)
    spec = P("data", "ctx", None, None)
    n = plan.blocks
    f32, bf16 = jnp.float32, jnp.bfloat16
    vm, sem = pltpu.VMEM, pltpu.SemaphoreType.DMA

    def local(queries, keys, values, grad_out):
        tokens = queries.shape[1]
        q = queries[0].transpose(1, 0, 2)
        g = grad_out[0].transpose(1, 0, 2)
        tile = (128, 128)
        big = jax.ShapeDtypeStruct((HEADS, tokens, HD), bf16)
        small = jax.ShapeDtypeStruct((tokens, HD), bf16)
        anywhere = pl.BlockSpec(memory_space=pl.ANY)
        twenty, ten, stat, few = (2 * TILES,) + tile, (TILES,) + tile, (2 * TILES, 8, 128), (TILES, 8, 128)
        results = pl.pallas_call(
            functools.partial(kernel, plan),
            out_shape=(big, big, small, small),
            in_specs=[anywhere] * 4,
            out_specs=(anywhere,) * 4,
            scratch_shapes=[
                vm((n // 2, 2, 2, 2) + tile, bf16), vm((n // 2, 2, 2, 2) + tile, f32), vm((n, 2, 2) + tile, f32),
                vm((TILES, 256, 256), f32), vm((TILES, 256, 256), f32), vm((TILES * 256, 256), bf16), vm((TILES * 256, 256), bf16),
                vm((TILES, 8, 256), f32),
                vm(twenty, bf16), vm(twenty, bf16), vm((2,) + tile, bf16), vm(twenty, bf16), vm(twenty, bf16),
                vm((2 * TILES, 2) + tile, bf16),
                vm(twenty, f32), vm(stat, f32), vm(stat, f32), vm((TILES, 8, 256), f32),
                vm(ten, f32), vm(few, f32), vm(few, f32), vm(stat, f32), vm(stat, f32), vm(twenty, f32), vm(twenty, f32),
                vm(twenty, f32), vm(ten, f32),
                vm(big.shape, bf16), vm(big.shape, bf16), vm(small.shape, bf16), vm(small.shape, bf16),
                sem((n, 2)), sem((n, 2)), sem((n, 2)), sem((n, 2)), sem((16,)), sem((16,)), sem((12,)),
            ],
            compiler_params=pltpu.CompilerParams(collective_id=0, has_side_effects=True, vmem_limit_bytes=67043328),
            cost_estimate=pl.CostEstimate(flops=14 * 640 * PIECE * n * 2 * HD, bytes_accessed=4 << 20, transcendentals=0),
        )(q, keys[0, :, 0], values[0, :, 0], g)
        o, dq, dk, dv = pl.pallas_call(
            relay,
            out_shape=(big, big, small, small),
            in_specs=[anywhere] * 4,
            out_specs=(anywhere,) * 4,
            scratch_shapes=[vm(x.shape, bf16) for x in (big, big, small, small)] + [sem((8,))],
            cost_estimate=pl.CostEstimate(flops=1 << 20, bytes_accessed=2 << 20, transcendentals=0),
        )(*results)
        return (o.transpose(1, 0, 2)[None], dq.transpose(1, 0, 2)[None], dk[None, :, None], dv[None, :, None])

    return jax.shard_map(local, mesh=mesh, in_specs=(spec,) * 4, out_specs=(spec,) * 4, check_vma=False)
```

```python
import functools
import math

import jax
import jax.numpy as jnp
from jax import lax
from jax.experimental import pallas as pl
from jax.experimental.pallas import tpu as pltpu
from jax.sharding import PartitionSpec as P

MESH = pl.DeviceIdType.MESH
NEG = -1e30
HD = 128
HEADS = 5
PIECE = 128
SCALE = HD ** -0.5
LOG2E = 1.4426950408889634
TILES = 2 * HEADS

KEY_TREE = "010222233102310441124214030442355112212553052304545225430514015"
VALUE_TREE = "011201033303033401044244434301355115220533150515540242154453254"
DK_TREE = "010222230332012401140144034343155105020503552515410521435133551"
DV_TREE = "011221233112231444444123310433250555512333020125545204050434440"
BWD_ORDER = "vtrnuqs7p3colifmejbad495h6k28g1"


def popcount(value):
    return bin(value).count("1")


class Tree:
    def __init__(self, dims, links):
        blocks = 1 << dims
        if dims == 6:
            self.link = [None] + [int(d) for d in links]
        else:
            self.link = [None] * blocks
            count = [0] * dims
            for r in sorted(range(1, blocks), key=popcount):
                self.link[r] = min((d for d in range(dims) if (r >> d) & 1), key=lambda d: count[d])
                count[self.link[r]] += 1
        self.kids = {r: [k for k in range(1, blocks) if k & ~(1 << self.link[k]) == r] for r in range(blocks)}
        height = {}
        for r in sorted(range(blocks), key=popcount, reverse=True):
            height[r] = max([1 + height[k] for k in self.kids[r]], default=0)
        for r in self.kids:
            self.kids[r].sort(key=lambda k: -height[k])


class Plan:
    def __init__(self, dims):
        self.dims = dims
        self.blocks = 1 << dims
        self.turns = self.blocks // 2 + 1
        self.fwd = [Tree(dims, KEY_TREE), Tree(dims, VALUE_TREE)]
        self.bwd = [Tree(dims, DK_TREE), Tree(dims, DV_TREE)]
        self.forward()
        self.backward()

    def forward(self, unit_us=1.41, hop_us=1.9, turn_us=0.84):
        free = [0.0] * self.dims
        due = {}
        done = {(0, 0), (0, 1)}
        now = 1.0
        steps, waits, ready, order = [], [], [0], []

        def send(r, x):
            for k in self.fwd[x].kids[r]:
                d = self.fwd[x].link[k]
                free[d] = max(free[d], now) + unit_us
                due[k, x] = free[d] + hop_us

        now = 0.0
        send(0, 0)
        send(0, 1)
        now = 1.0
        while True:
            for unit in sorted((u for u in due if u not in done and due[u] <= now), key=lambda u: (due[u], u)):
                done.add(unit)
                now += 0.02
                send(*unit)
                waits.append(unit)
                if unit[1] == 0 and (unit[0] ^ 1, 0) in done:
                    ready.append(unit[0] >> 1)
            turn = len(steps)
            late = order[max(turn - 2, 0):turn - 1] if turn < self.turns else order[turn - 2:]
            lacking = [r for pair in late for r in (2 * pair, 2 * pair + 1) if (r, 1) not in done]
            if turn == 2 < self.turns:
                lacking = []
            if lacking or not (ready or turn == self.turns):
                now = max(now, min(due[u] for u in due if u not in done))
                continue
            if turn == self.turns:
                break
            order.append(ready.pop(0))
            steps.append(waits)
            waits = []
            now += turn_us if turn else 0.0
        self.fwd_waits = steps + [waits]
        self.fwd_pairs = order
        self.fwd_mate = max(i for i, pair in enumerate(order) if pair == 0)

    def backward(self, unit_us=2.82, hop_us=2.0, turn_us=1.52, add_us=0.03):
        if self.dims == 6:
            order = [int(c, 32) for c in BWD_ORDER]
        else:
            order = sorted(range(1, self.blocks // 2), key=lambda pair: -popcount(pair))
        order += [0, 0]
        free = [0.0] * self.dims
        due = {}
        waiting = set()
        now = turn_us
        steps, sends = [], []
        position = 0

        def kids(unit):
            return [(k, unit[1]) for k in self.bwd[unit[1]].kids[unit[0]]]

        while True:
            able = True
            while able:
                able = [u for u in waiting if all(due.get(k, 1e9) <= now for k in kids(u))]
                for unit in sorted(able, key=lambda u: (-popcount(u[0]), u)):
                    waiting.discard(unit)
                    now += add_us * len(kids(unit)) + 0.01
                    d = self.bwd[unit[1]].link[unit[0]]
                    free[d] = max(free[d], now) + unit_us
                    due[unit] = free[d] + hop_us
                    sends.append(unit)
            if position < len(order):
                pair = order[position]
                position += 1
                now += turn_us
                if pair:
                    waiting |= {(2 * pair + i, x) for i in range(2) for x in range(2)}
                elif position < len(order):
                    waiting |= {(1, 0), (1, 1)}
                steps.append(sends)
                sends = []
            elif waiting:
                now = max(now, min(max(due.get(k, 1e9) for k in kids(u)) for u in waiting))
            else:
                break
        self.bwd_sends = steps + [sends]
        self.bwd_pairs = order
        self.bwd_last = sorted((u for x in range(2) for u in kids((0, x))), key=lambda u: due[u])


def div(a, b):
    return lax.div(a, jnp.int32(b))


def mod(a, b):
    return lax.rem(a, jnp.int32(b))


def xor(a, b):
    return a + b - 2 * a * b


def lookup(index, table):
    level = [jnp.int32(v) for v in table]
    bit = 1
    while len(level) > 1:
        odd = mod(div(index, bit), 2) == 1
        nxt = [jnp.where(odd, level[i + 1], level[i]) for i in range(0, len(level) - 1, 2)]
        level = nxt + level[2 * len(nxt):]
        bit *= 2
    return level[0]


def branch(index, count, leaf):
    once = div(index, count) + 1

    def pick(low, high):
        if high - low == 1:
            acts = leaf(low)
            if acts:
                pl.loop(0, once)(lambda _: [act() for act in acts] and None)
            return
        mid = (low + high) // 2
        lax.cond(index < mid, lambda: pick(low, mid), lambda: pick(mid, high))

    pick(0, count)


def kernel(plan, q_ref, k_ref, v_ref, g_ref, o_ref, dq_ref, dk_ref, dv_ref,
           kv, stg, land, s_buf, t_buf, p_buf, d_buf, top, q_s, g_s, v_s, q_t, g_t, c_t, acc, mst, lst, dec,
           xacc, xm, xl, lrow, drow, lcol, dcol, dq_s, xdq, o_s, dq_o, dk_o, dv_o,
           ag_send, ag_recv, rs_send, rs_recv, x_send, x_recv, io):
    dims, turns = plan.dims, plan.turns
    pieces = 4 * plan.blocks
    f32, bf16 = jnp.float32, jnp.bfloat16
    me = lax.axis_index("ctx")
    core = mod(me, 2)
    chip = div(me, 2)
    bits = [mod(div(chip, 1 << d), 2) for d in range(dims)]
    gray = [xor(bits[d], bits[d + 1]) if d % 2 == 0 and d + 1 < dims else bits[d] for d in range(dims)]
    nbr = []
    for d in range(dims):
        other = chip + (1 - 2 * bits[d]) * (1 << d)
        if d % 2:
            other = other + (1 - 2 * bits[d - 1]) * (1 << (d - 1))
        nbr.append(2 * other + core)
    mate = me + 1 - 2 * core
    my_pair = div(chip, 2)

    barrier = pltpu.get_barrier_semaphore()
    for dev in nbr + [mate]:
        pl.semaphore_signal(barrier, inc=1, device_id={"ctx": dev}, device_id_type=MESH)

    def half(h):
        return pl.ds(h * PIECE, PIECE)

    loads = []
    for h in range(2):
        loads += [pltpu.make_async_copy(v_ref.at[half(h)], v_s.at[h], io.at[h]),
                  pltpu.make_async_copy(k_ref.at[half(h)], kv.at[0, 0, 0, h], io.at[2 + h])]
    for h in range(2):
        for j, (src, dst) in enumerate(((q_ref, q_s), (g_ref, g_s))):
            loads.append(pltpu.make_async_copy(src.at[:, half(h)], dst.at[pl.ds(h * TILES, HEADS)], io.at[4 + 2 * j + h]))
    for copy in loads:
        copy.start()
    mst[...] = jnp.full(mst.shape, NEG, f32)
    lst[...] = jnp.zeros(lst.shape, f32)
    acc[...] = jnp.zeros(acc.shape, f32)
    for copy in loads[:4]:
        copy.wait()
    for h in range(2):
        kv[0, 0, 1, h] = v_s[h].T

    pl.semaphore_wait(barrier, dims + 1)

    def ag_copy(k, x):
        d = plan.fwd[x].link[k]
        r = k ^ (1 << d)
        return pltpu.make_async_remote_copy(
            src_ref=kv.at[r >> 1, r & 1, x], dst_ref=kv.at[k >> 1, k & 1, x], send_sem=ag_send.at[k, x],
            recv_sem=ag_recv.at[k, x], device_id={"ctx": nbr[d]}, device_id_type=MESH)

    def rs_copy(r, x):
        return pltpu.make_async_remote_copy(
            src_ref=stg.at[r >> 1, r & 1, x], dst_ref=land.at[r, x], send_sem=rs_send.at[r, x], recv_sem=rs_recv.at[r, x],
            device_id={"ctx": nbr[plan.bwd[x].link[r]]}, device_id_type=MESH)

    def mate_copy(src, dst, sem):
        return pltpu.make_async_remote_copy(src_ref=src, dst_ref=dst, send_sem=x_send.at[sem], recv_sem=x_recv.at[sem],
                                            device_id={"ctx": mate}, device_id_type=MESH)

    def own(ref, h):
        return ref.at[pl.ds(h * TILES, HEADS)]

    def theirs(ref, h):
        return ref.at[pl.ds(h * TILES + HEADS, HEADS)]

    for x in range(2):
        for k in plan.fwd[x].kids[0]:
            ag_copy(k, x).start()
    for copy in loads[4:]:
        copy.wait()
    x_q = [mate_copy(own(ref, h), theirs(ref, h), 2 * j + h) for j, ref in enumerate((q_s, g_s)) for h in range(2)]
    for copy in x_q:
        copy.start()

    def ag_events(waits):
        return [act for r, x in waits for act in [ag_copy(r, x).wait_recv] + [ag_copy(k, x).start for k in plan.fwd[x].kids[r]]]

    coef = SCALE * LOG2E

    def transposes(c):
        turned = q_s[c].T
        q_t[c] = turned
        g_t[c] = g_s[c].T
        scaled = turned.astype(f32) * coef
        high = scaled.astype(bf16)
        c_t[c, 0] = high
        c_t[c, 1] = (scaled - high.astype(f32)).astype(bf16)

    for h in range(2):
        pl.loop(h * TILES, h * TILES + HEADS)(transposes)
    for copy in x_q:
        copy.wait_recv()
    for h in range(2):
        pl.loop(h * TILES + HEADS, h * TILES + TILES)(transposes)

    def is_future(pair):
        rel = [mod(div(pair, 1 << (d - 1)), 2) for d in range(1, dims)]
        gp = [None] + [xor(gray[d], rel[d - 1]) for d in range(1, dims)]
        other = gp[1] if dims > 1 else 0
        for d in range(2, dims):
            bit = xor(gp[d], gp[d + 1]) if d % 2 == 0 and d + 1 < dims else gp[d]
            other = other + bit * (1 << (d - 1))
        return div(other - my_pair + plan.blocks, plan.blocks)

    def place(pair, a):
        mine = div(plan.blocks // 2 - pair, plan.blocks // 2)
        fut = is_future(pair)
        turn = (pair,)
        for slot in range(2):
            h = (1 - mine) * fut * slot
            turn += (mine * a, h, mine * a + 1 - mine, mine + h, mine * slot + (1 - mine) * (fut + (1 - fut) * slot))
        return turn

    def groups(turn, some):
        for slot in range(2):
            if not any(slot * HEADS <= b < slot * HEADS + HEADS for b in some):
                continue
            p0, h0, p1, h1, qg = turn[1 + 5 * slot:6 + 5 * slot]
            yield slot, ((turn[0], p0, h0), (turn[0], p1, h1)), qg * TILES

    def key_tile(where):
        return jnp.concatenate([kv[pair, par, 0, h] for pair, par, h in where], axis=0)

    def value_tile_t(where):
        return jnp.concatenate([kv[pair, par, 1, h] for pair, par, h in where], axis=1)

    def wide(ref, c):
        return jnp.concatenate([ref[c], ref[c + 1]], axis=1)

    def tall(ref, c):
        return jnp.concatenate([ref[c], ref[c + 1]], axis=0)

    def rows(b):
        return pl.ds(b * 256, 256)

    def mask_scores(a, keys_axis):
        key_low = me + a * (2 * (1 - 2 * mod(chip, 2)))

        def two(base0, base1, axis):
            i = lax.broadcasted_iota(jnp.int32, (256, 256), axis)
            return i + jnp.where(i < PIECE, base0, base1 - PIECE)

        def query_base(c):
            h, par = div(c, TILES), mod(div(c, HEADS), 2)
            low = me + par * (mate - me)
            return (low + h * (pieces - 1 - 2 * low)) * PIECE

        @pl.loop(0, TILES)
        def _(b):
            kpos = two(key_low * PIECE, (pieces - 1 - key_low) * PIECE, keys_axis)
            qpos = two(query_base(2 * b), query_base(2 * b + 1), 1 - keys_axis)
            s = jnp.where(qpos >= kpos, s_buf[b], NEG)
            s_buf[b] = s
            if keys_axis == 0:
                top[b] = jnp.max(s.reshape(32, 8, 256), axis=0)

    def fwd_scores(turn, some=range(TILES)):
        for slot, where, base in groups(turn, some):
            kt = key_tile(where)
            twice = jnp.concatenate([kt, kt], axis=1)
            for t in range(HEADS):
                b, c = slot * HEADS + t, base + 2 * t
                if b in some:
                    scaled = jnp.concatenate([wide(c_t.at[:, i], c) for i in range(2)], axis=0)
                    s = jnp.dot(twice, scaled, preferred_element_type=f32)
                    s_buf[b] = s
                    top[b] = jnp.max(s.reshape(32, 8, 256), axis=0)

    def fwd_softmax(turn, some):
        for slot, _, base in groups(turn, some):
            for t in range(HEADS):
                b, c = slot * HEADS + t, base + 2 * t
                if b not in some:
                    continue
                m_old = wide(mst, c)
                m_new = jnp.maximum(m_old, jnp.max(top[b], axis=0, keepdims=True))
                p = jnp.exp2(s_buf[b] - m_new[0:1])
                decay = jnp.exp2(m_old - m_new)
                l_new = wide(lst, c) * decay + jnp.sum(p.reshape(32, 8, 256), axis=0)
                p_buf[rows(b), :] = p.astype(bf16)
                dec[b] = decay
                for j in range(2):
                    cols = slice(j * 128, j * 128 + 128)
                    mst[c + j] = m_new[:, cols]
                    lst[c + j] = l_new[:, cols]

    def fwd_out(turn, some=range(TILES)):
        for slot, where, base in groups(turn, some):
            vt = value_tile_t(where)
            for t in range(HEADS):
                b, c = slot * HEADS + t, base + 2 * t
                if b in some:
                    pv = jnp.dot(vt, p_buf[rows(b), :], preferred_element_type=f32)
                    for j in range(2):
                        cols = slice(j * 128, j * 128 + 128)
                        acc[c + j] = acc[c + j] * dec[b, 0:1, cols] + pv[:, cols]

    def fwd_place(j):
        return place(lookup(jnp.minimum(j, turns - 1), plan.fwd_pairs), jnp.minimum(j, 1))

    for act in ag_events(plan.fwd_waits[0]):
        act()
    old = fwd_place(me * 0)
    fwd_scores(old)
    mask_scores(0, 0)
    for act in ag_events(plan.fwd_waits[1]):
        act()
    cur = fwd_place(me * 0 + 1)
    for b in range(TILES + 1):
        fwd_scores(cur, (b - 1,))
        fwd_softmax(old, (b,))

    def fwd_turn(j, carry):
        old, cur, new = carry
        branch(j, turns, lambda i: ag_events(plan.fwd_waits[i + 1]) if i else [])

        @pl.when(j == plan.fwd_mate)
        def _():
            mask_scores(1, 0)

        after = fwd_place(j + 2)
        for b in range(TILES + 2):
            fwd_scores(new, (b - 2,))
            fwd_softmax(cur, (b - 1,))
            fwd_out(old, (b,))
        return cur, new, after

    last = lax.fori_loop(1, turns, fwd_turn, (old, cur, fwd_place(me * 0 + 2)))[0]
    fwd_out(last)

    def bwd_scores(turn, some=range(TILES), parts=(0, 1)):
        for slot, where, base in groups(turn, some):
            kt_t, vt = key_tile(where).T, value_tile_t(where)
            for t in range(HEADS):
                b, c = slot * HEADS + t, base + 2 * t
                for part in parts if b in some else ():
                    buf, lhs, rhs = ((s_buf, q_s, kt_t), (t_buf, g_s, vt))[part]
                    buf[b] = jnp.dot(tall(lhs, c), rhs, preferred_element_type=f32)

    def bwd_softmax(turn, some):
        for slot, _, base in groups(turn, some):
            for t in range(HEADS):
                b, c = slot * HEADS + t, base + 2 * t
                if b in some:
                    lse, dr = tall(lcol, c), tall(dcol, c)
                    p = jnp.exp2(s_buf[b] * coef - jnp.concatenate([lse, lse], axis=1))
                    p_buf[rows(b), :] = p.astype(bf16)
                    d_buf[rows(b), :] = (p * (t_buf[b] - jnp.concatenate([dr, dr], axis=1))).astype(bf16)

    def bwd_out(turn, sums, some=range(TILES), parts=(0, 1)):
        for slot, where, base in groups(turn, some):
            kt_t = key_tile(where).T
            for t in range(HEADS):
                b, c = slot * HEADS + t, base + 2 * t
                if b not in some:
                    continue
                ds = d_buf[rows(b), :]
                if 0 in parts:
                    dq = lax.dot_general(kt_t, ds, (((1,), (1,)), ((), ())), preferred_element_type=f32)
                    for j in range(2):
                        dq_s[c + j] += dq[:, j * 128:j * 128 + 128]
                for x, (ref, buf) in enumerate(((q_t, ds), (g_t, p_buf[rows(b), :])) if 1 in parts else ()):
                    grad = jnp.dot(wide(ref, c), buf, preferred_element_type=f32)
                    sums[x] = sums[x] + grad if t else grad
                    for j, (pair, par, h) in enumerate(where if t == HEADS - 1 else ()):
                        value = sums[x][:, j * 128:j * 128 + 128]
                        if slot:
                            value = value + stg[pair, par, x, h]
                        stg[pair, par, x, h] = value

    def bwd_place(j):
        at = jnp.minimum(j, turns - 1)
        return place(lookup(at, plan.bwd_pairs), 1 - div(at + 1, turns))

    x_m = []
    for h in range(2):
        inbox = pl.ds(h * HEADS, HEADS)
        x_m += [mate_copy(theirs(ref, h), box.at[inbox], 4 + 3 * h + i)
                for i, (ref, box) in enumerate(((acc, xacc), (mst, xm), (lst, xl)))]
    for copy in x_m:
        copy.start()
    first = bwd_place(me * 0)
    bwd_scores(first)
    dq_s[...] = jnp.zeros(dq_s.shape, f32)
    x_r = [mate_copy(own(ref, h), theirs(ref, h), 10 + 2 * j + h) for j, ref in enumerate((lrow, drow)) for h in range(2)]

    for h in range(2):
        for copy in x_m[3 * h:3 * h + 3]:
            copy.wait_recv()
        for head in range(HEADS):
            c, i = h * TILES + head, h * HEADS + head
            m1, m2 = mst[c], xm[i]
            m = jnp.maximum(m1, m2)
            w1, w2 = jnp.exp2(m1 - m), jnp.exp2(m2 - m)
            total = jnp.sum(lst[c] * w1 + xl[i] * w2, axis=0, keepdims=True)
            out = (acc[c] * w1[0:1] + xacc[i] * w2[0:1]) / total
            o_s[head, half(h), :] = out.T.astype(bf16)
            lrow[c] = m + jnp.log2(total)
            rounded = out.astype(bf16).astype(f32)
            drow[c] = jnp.broadcast_to(jnp.sum(rounded * g_t[c].astype(f32), axis=0, keepdims=True), (8, 128))
        for copy in x_r[h::2]:
            copy.start()
    stores = [pltpu.make_async_copy(o_s, o_ref, io.at[8])]
    stores[0].start()

    def columns(c):
        lcol[c] = jnp.broadcast_to(lrow[c, 0:1], (128, 128)).T
        dcol[c] = jnp.broadcast_to(drow[c, 0:1], (128, 128)).T

    for h in range(2):
        pl.loop(h * TILES, h * TILES + HEADS)(columns)
    for copy in x_r:
        copy.wait_recv()
    for h in range(2):
        pl.loop(h * TILES + HEADS, h * TILES + TILES)(columns)

    def rs_add(r, k, x):
        rs_copy(k, x).wait_recv()
        for h in range(2):
            stg[r >> 1, r & 1, x, h] += land[k, x, h]

    def rs_events(sends):
        return ([functools.partial(rs_add, r, k, x) for r, x in sends for k in plan.bwd[x].kids[r]]
                + [rs_copy(r, x).start for r, x in sends])

    if turns == 2:
        mask_scores(1, 1)
    cur = bwd_place(me * 0 + 1)
    for b in range(TILES + 1):
        bwd_softmax(first, (b,))
        bwd_scores(cur, (b - 1,))

    def bwd_turn(j, carry):
        old, cur, new = carry
        branch(j, turns, lambda i: rs_events(plan.bwd_sends[i - 1]) if i else [])

        @pl.when(j < turns - 1)
        def _():
            for i in range(4):
                stg[old[0], i // 2, i % 2, 1] = jnp.zeros((128, 128), f32)

        @pl.when(j >= turns - 2)
        def _():
            mask_scores(turns - 1 - j, 1)

        after = bwd_place(j + 2)
        sums = {}
        for b in range(TILES + 2):
            bwd_out(old, sums, (b,))
            bwd_softmax(cur, (b - 1,))
            bwd_scores(new, (b - 2,))
        return cur, new, after

    last = lax.fori_loop(1, turns, bwd_turn, (first, cur, bwd_place(me * 0 + 2)))[0]
    for act in rs_events(plan.bwd_sends[turns - 1]):
        act()
    bwd_out(last, {})

    x_d = [mate_copy(theirs(dq_s, h), xdq.at[pl.ds(h * HEADS, HEADS)], 14 + h) for h in range(2)]
    for copy in x_d:
        copy.start()
    for unit in plan.bwd_sends[turns]:
        for act in rs_events([unit]):
            act()
    for h in range(2):
        x_d[h].wait_recv()
        for head in range(HEADS):
            total = (dq_s[h * TILES + head] + xdq[h * HEADS + head]) * SCALE
            dq_o[head, half(h), :] = total.T.astype(bf16)
    stores.append(pltpu.make_async_copy(dq_o, dq_ref, io.at[9]))
    stores[1].start()
    for k, x in plan.bwd_last:
        rs_add(0, k, x)
    for x, (buf, ref, factor) in enumerate(((dk_o, dk_ref, SCALE), (dv_o, dv_ref, 1.0))):
        for h in range(2):
            buf[half(h), :] = (stg[0, 0, x, h] * factor).T.astype(bf16)
        stores.append(pltpu.make_async_copy(buf, ref, io.at[10 + x]))
        stores[-1].start()

    for k in range(1, plan.blocks):
        for x in range(2):
            ag_copy(k, x).wait_send()
            rs_copy(k, x).wait_send()
    for copy in x_q + x_m + x_r + x_d:
        copy.wait_send()
    for copy in stores:
        copy.wait()


def relay(*refs):
    count = (len(refs) - 1) // 3
    src, dst, buf, sem = refs[:count], refs[count:2 * count], refs[2 * count:3 * count], refs[3 * count]
    into = [pltpu.make_async_copy(a, b, sem.at[i]) for i, (a, b) in enumerate(zip(src, buf))]
    out = [pltpu.make_async_copy(b, c, sem.at[count + i]) for i, (b, c) in enumerate(zip(buf, dst))]
    for copy in into:
        copy.start()
    for i in range(count):
        into[i].wait()
        out[i].start()
    for copy in out:
        copy.wait()


def solution(mesh):
    size = mesh.shape["ctx"]
    plan = Plan(int(math.log2(size)) - 1)
    spec = P("data", "ctx", None, None)
    n = plan.blocks
    f32, bf16 = jnp.float32, jnp.bfloat16
    vm, sem = pltpu.VMEM, pltpu.SemaphoreType.DMA

    def local(queries, keys, values, grad_out):
        tokens = queries.shape[1]
        q = queries[0].transpose(1, 0, 2)
        g = grad_out[0].transpose(1, 0, 2)
        tile = (128, 128)
        big = jax.ShapeDtypeStruct((HEADS, tokens, HD), bf16)
        small = jax.ShapeDtypeStruct((tokens, HD), bf16)
        anywhere = pl.BlockSpec(memory_space=pl.ANY)
        twenty, ten, stat, few = (2 * TILES,) + tile, (TILES,) + tile, (2 * TILES, 8, 128), (TILES, 8, 128)
        results = pl.pallas_call(
            functools.partial(kernel, plan),
            out_shape=(big, big, small, small),
            in_specs=[anywhere] * 4,
            out_specs=(anywhere,) * 4,
            scratch_shapes=[
                vm((n // 2, 2, 2, 2) + tile, bf16), vm((n // 2, 2, 2, 2) + tile, f32), vm((n, 2, 2) + tile, f32),
                vm((TILES, 256, 256), f32), vm((TILES, 256, 256), f32), vm((TILES * 256, 256), bf16), vm((TILES * 256, 256), bf16),
                vm((TILES, 8, 256), f32),
                vm(twenty, bf16), vm(twenty, bf16), vm((2,) + tile, bf16), vm(twenty, bf16), vm(twenty, bf16),
                vm((2 * TILES, 2) + tile, bf16),
                vm(twenty, f32), vm(stat, f32), vm(stat, f32), vm((TILES, 8, 256), f32),
                vm(ten, f32), vm(few, f32), vm(few, f32), vm(stat, f32), vm(stat, f32), vm(twenty, f32), vm(twenty, f32),
                vm(twenty, f32), vm(ten, f32),
                vm(big.shape, bf16), vm(big.shape, bf16), vm(small.shape, bf16), vm(small.shape, bf16),
                sem((n, 2)), sem((n, 2)), sem((n, 2)), sem((n, 2)), sem((16,)), sem((16,)), sem((12,)),
            ],
            compiler_params=pltpu.CompilerParams(collective_id=0, has_side_effects=True, vmem_limit_bytes=67043328),
            cost_estimate=pl.CostEstimate(flops=14 * 640 * PIECE * n * 2 * HD, bytes_accessed=4 << 20, transcendentals=0),
        )(q, keys[0, :, 0], values[0, :, 0], g)
        o, dq, dk, dv = pl.pallas_call(
            relay,
            out_shape=(big, big, small, small),
            in_specs=[anywhere] * 4,
            out_specs=(anywhere,) * 4,
            scratch_shapes=[vm(x.shape, bf16) for x in (big, big, small, small)] + [sem((8,))],
            cost_estimate=pl.CostEstimate(flops=1 << 20, bytes_accessed=2 << 20, transcendentals=0),
        )(*results)
        return (o.transpose(1, 0, 2)[None], dq.transpose(1, 0, 2)[None], dk[None, :, None], dv[None, :, None])

    return jax.shard_map(local, mesh=mesh, in_specs=(spec,) * 4, out_specs=(spec,) * 4, check_vma=False)
```

```python
import functools
import math

import jax
import jax.numpy as jnp
from jax import lax
from jax.experimental import pallas as pl
from jax.experimental.pallas import tpu as pltpu
from jax.sharding import PartitionSpec as P

MESH = pl.DeviceIdType.MESH
NEG = -1e30
HD = 128
HEADS = 5
PIECE = 128
SCALE = HD ** -0.5
LOG2E = 1.4426950408889634
TILES = 2 * HEADS

KEY_TREE = "011222233332220401120144343324455112221331530525044554535415311"
VALUE_TREE = "010202030312010444044424310243155552011305020335411555543543021"
DK_TREE = "011202030133312401444244343301355152021301322315050445445404320"
DV_TREE = "011222133132330444122243010422050155555551523155450502240135413"
BWD_ORDER = "vrndou7tmjqflpsh6ebk9ac35i4g128"


def popcount(value):
    return bin(value).count("1")


class Tree:
    def __init__(self, dims, links):
        blocks = 1 << dims
        if dims == 6:
            self.link = [None] + [int(d) for d in links]
        else:
            self.link = [None] * blocks
            count = [0] * dims
            for r in sorted(range(1, blocks), key=popcount):
                self.link[r] = min((d for d in range(dims) if (r >> d) & 1), key=lambda d: count[d])
                count[self.link[r]] += 1
        self.kids = {r: [k for k in range(1, blocks) if k & ~(1 << self.link[k]) == r] for r in range(blocks)}
        height = {}
        for r in sorted(range(blocks), key=popcount, reverse=True):
            height[r] = max([1 + height[k] for k in self.kids[r]], default=0)
        for r in self.kids:
            self.kids[r].sort(key=lambda k: -height[k])


class Plan:
    def __init__(self, dims):
        self.dims = dims
        self.blocks = 1 << dims
        self.turns = self.blocks // 2 + 1
        self.fwd = [Tree(dims, KEY_TREE), Tree(dims, VALUE_TREE)]
        self.bwd = [Tree(dims, DK_TREE), Tree(dims, DV_TREE)]
        self.forward()
        self.backward()

    def forward(self, unit_us=1.41, hop_us=1.9, turn_us=0.87):
        free = [0.0] * self.dims
        due = {}
        done = {(0, 0), (0, 1)}
        now = 1.0
        steps, waits, ready, order = [], [], [0], []

        def send(r, x):
            for k in self.fwd[x].kids[r]:
                d = self.fwd[x].link[k]
                free[d] = max(free[d], now) + unit_us
                due[k, x] = free[d] + hop_us

        now = 0.0
        send(0, 0)
        send(0, 1)
        now = 1.0
        while True:
            for unit in sorted((u for u in due if u not in done and due[u] <= now), key=lambda u: (due[u], u)):
                done.add(unit)
                now += 0.02
                send(*unit)
                waits.append(unit)
                if unit[1] == 0 and (unit[0] ^ 1, 0) in done:
                    ready.append(unit[0] >> 1)
            turn = len(steps)
            late = order[max(turn - 2, 0):turn - 1] if turn < self.turns else order[turn - 2:]
            lacking = [r for pair in late for r in (2 * pair, 2 * pair + 1) if (r, 1) not in done]
            if turn == 2 < self.turns:
                lacking = []
            if lacking or not (ready or turn == self.turns):
                now = max(now, min(due[u] for u in due if u not in done))
                continue
            if turn == self.turns:
                break
            order.append(ready.pop(0))
            steps.append(waits)
            waits = []
            now += turn_us if turn else 0.0
        self.fwd_waits = steps + [waits]
        self.fwd_pairs = order
        self.fwd_mate = max(i for i, pair in enumerate(order) if pair == 0)

    def backward(self, unit_us=2.86, hop_us=2.1, turn_us=1.55, add_us=0.035):
        if self.dims == 6:
            order = [int(c, 32) for c in BWD_ORDER]
        else:
            order = sorted(range(1, self.blocks // 2), key=lambda pair: -popcount(pair))
        order += [0, 0]
        free = [0.0] * self.dims
        due = {}
        waiting, sends, steps = set(), [], []
        now = 1.35

        def kids(unit):
            return [(k, unit[1]) for k in self.bwd[unit[1]].kids[unit[0]]]

        def flush():
            nonlocal now
            able = True
            while able:
                able = [u for u in waiting if all(due.get(k, 1e9) <= now for k in kids(u))]
                for unit in sorted(able, key=lambda u: (-popcount(u[0]), u)):
                    waiting.discard(unit)
                    now += add_us * len(kids(unit)) + 0.01
                    d = self.bwd[unit[1]].link[unit[0]]
                    free[d] = max(free[d], now) + unit_us
                    due[unit] = free[d] + hop_us
                    sends.append(unit)

        for i, pair in enumerate(order):
            waiting |= {(r, x) for r in (2 * pair, 2 * pair + 1) for x in range(2) if r} if i < len(order) - 1 else set()
            flush()
            steps.append(sends)
            sends = []
            if i == 0:
                now += 0.85
                flush()
                steps.append(sends)
                sends = []
            now += turn_us if i < len(order) - 1 else 0.0
        while waiting:
            now = max(now, min(max(due.get(k, 1e9) for k in kids(u)) for u in waiting))
            flush()
        self.bwd_sends = steps[:-1] + [steps[-1] + sends]
        self.bwd_pairs = order
        self.bwd_last = sorted((u for x in range(2) for u in kids((0, x))), key=lambda u: due[u])


def div(a, b):
    return lax.div(a, jnp.int32(b))


def mod(a, b):
    return lax.rem(a, jnp.int32(b))


def xor(a, b):
    return a + b - 2 * a * b


def lookup(index, table):
    level = [jnp.int32(v) for v in table]
    bit = 1
    while len(level) > 1:
        odd = mod(div(index, bit), 2) == 1
        nxt = [jnp.where(odd, level[i + 1], level[i]) for i in range(0, len(level) - 1, 2)]
        level = nxt + level[2 * len(nxt):]
        bit *= 2
    return level[0]


def branch(index, count, leaf):
    once = div(index, count) + 1

    def pick(low, high):
        if high - low == 1:
            acts = leaf(low)
            if acts:
                pl.loop(0, once)(lambda _: [act() for act in acts] and None)
            return
        mid = (low + high) // 2
        lax.cond(index < mid, lambda: pick(low, mid), lambda: pick(mid, high))

    pick(0, count)


def kernel(plan, q_ref, k_ref, v_ref, g_ref, o_ref, dq_ref, dk_ref, dv_ref,
           kv, stg, land, s_buf, t_buf, p_buf, d_buf, top, q_s, g_s, v_s, q_t, g_t, c_t, acc, mst, lst, dec,
           xacc, xm, xl, lrow, drow, lcol, dcol, dq_s, xdq, o_s, dq_o, dk_o, dv_o,
           ag_send, ag_recv, rs_send, rs_recv, x_send, x_recv, io):
    dims, turns = plan.dims, plan.turns
    pieces = 4 * plan.blocks
    f32, bf16 = jnp.float32, jnp.bfloat16
    me = lax.axis_index("ctx")
    core = mod(me, 2)
    chip = div(me, 2)
    bits = [mod(div(chip, 1 << d), 2) for d in range(dims)]
    gray = [xor(bits[d], bits[d + 1]) if d % 2 == 0 and d + 1 < dims else bits[d] for d in range(dims)]
    nbr = []
    for d in range(dims):
        other = chip + (1 - 2 * bits[d]) * (1 << d)
        if d % 2:
            other = other + (1 - 2 * bits[d - 1]) * (1 << (d - 1))
        nbr.append(2 * other + core)
    mate = me + 1 - 2 * core
    my_pair = div(chip, 2)

    barrier = pltpu.get_barrier_semaphore()
    for dev in nbr + [mate]:
        pl.semaphore_signal(barrier, inc=1, device_id={"ctx": dev}, device_id_type=MESH)

    def half(h):
        return pl.ds(h * PIECE, PIECE)

    loads = []
    for h in range(2):
        loads += [pltpu.make_async_copy(v_ref.at[half(h)], v_s.at[h], io.at[h]),
                  pltpu.make_async_copy(k_ref.at[half(h)], kv.at[0, 0, 0, h], io.at[2 + h])]
    for h in range(2):
        for j, (src, dst) in enumerate(((q_ref, q_s), (g_ref, g_s))):
            loads.append(pltpu.make_async_copy(src.at[:, half(h)], dst.at[pl.ds(h * TILES, HEADS)], io.at[4 + 2 * j + h]))
    for copy in loads:
        copy.start()
    mst[...] = jnp.full(mst.shape, NEG, f32)
    lst[...] = jnp.zeros(lst.shape, f32)
    acc[...] = jnp.zeros(acc.shape, f32)
    for copy in loads[:4]:
        copy.wait()
    for h in range(2):
        kv[0, 0, 1, h] = v_s[h].T

    pl.semaphore_wait(barrier, dims + 1)

    def ag_copy(k, x):
        d = plan.fwd[x].link[k]
        r = k ^ (1 << d)
        return pltpu.make_async_remote_copy(
            src_ref=kv.at[r >> 1, r & 1, x], dst_ref=kv.at[k >> 1, k & 1, x], send_sem=ag_send.at[k, x],
            recv_sem=ag_recv.at[k, x], device_id={"ctx": nbr[d]}, device_id_type=MESH)

    def rs_copy(r, x):
        return pltpu.make_async_remote_copy(
            src_ref=stg.at[r >> 1, r & 1, x], dst_ref=land.at[r, x], send_sem=rs_send.at[r, x], recv_sem=rs_recv.at[r, x],
            device_id={"ctx": nbr[plan.bwd[x].link[r]]}, device_id_type=MESH)

    def mate_copy(src, dst, sem):
        return pltpu.make_async_remote_copy(src_ref=src, dst_ref=dst, send_sem=x_send.at[sem], recv_sem=x_recv.at[sem],
                                            device_id={"ctx": mate}, device_id_type=MESH)

    def own(ref, h):
        return ref.at[pl.ds(h * TILES, HEADS)]

    def theirs(ref, h):
        return ref.at[pl.ds(h * TILES + HEADS, HEADS)]

    for x in range(2):
        for k in plan.fwd[x].kids[0]:
            ag_copy(k, x).start()
    for copy in loads[4:]:
        copy.wait()
    x_q = [mate_copy(own(ref, h), theirs(ref, h), 2 * j + h) for j, ref in enumerate((q_s, g_s)) for h in range(2)]
    for copy in x_q:
        copy.start()

    def ag_events(waits):
        return [act for r, x in waits for act in [ag_copy(r, x).wait_recv] + [ag_copy(k, x).start for k in plan.fwd[x].kids[r]]]

    coef = SCALE * LOG2E

    def transposes(c):
        turned = q_s[c].T
        q_t[c] = turned
        g_t[c] = g_s[c].T
        scaled = turned.astype(f32) * coef
        high = scaled.astype(bf16)
        c_t[c, 0] = high
        c_t[c, 1] = (scaled - high.astype(f32)).astype(bf16)

    for h in range(2):
        pl.loop(h * TILES, h * TILES + HEADS)(transposes)
    for copy in x_q:
        copy.wait_recv()
    for h in range(2):
        pl.loop(h * TILES + HEADS, h * TILES + TILES)(transposes)

    def is_future(pair):
        rel = [mod(div(pair, 1 << (d - 1)), 2) for d in range(1, dims)]
        gp = [None] + [xor(gray[d], rel[d - 1]) for d in range(1, dims)]
        other = gp[1] if dims > 1 else 0
        for d in range(2, dims):
            bit = xor(gp[d], gp[d + 1]) if d % 2 == 0 and d + 1 < dims else gp[d]
            other = other + bit * (1 << (d - 1))
        return div(other - my_pair + plan.blocks, plan.blocks)

    def place(pair, a):
        mine = div(plan.blocks // 2 - pair, plan.blocks // 2)
        fut = is_future(pair)
        turn = (pair,)
        for slot in range(2):
            h = (1 - mine) * fut * slot
            turn += (mine * a, h, mine * a + 1 - mine, mine + h, mine * slot + (1 - mine) * (fut + (1 - fut) * slot))
        return turn

    def groups(turn, some):
        for slot in range(2):
            if not any(slot * HEADS <= b < slot * HEADS + HEADS for b in some):
                continue
            p0, h0, p1, h1, qg = turn[1 + 5 * slot:6 + 5 * slot]
            yield slot, ((turn[0], p0, h0), (turn[0], p1, h1)), qg * TILES

    def key_tile(where):
        return jnp.concatenate([kv[pair, par, 0, h] for pair, par, h in where], axis=0)

    def value_tile_t(where):
        return jnp.concatenate([kv[pair, par, 1, h] for pair, par, h in where], axis=1)

    def tile_of(memo, slot, kind, where):
        key = (kind, slot)
        if key not in memo:
            memo[key] = value_tile_t(where) if kind == "v" else key_tile(where) if kind == "k" else key_tile(where).T
        return memo[key]

    def wide(ref, c):
        return jnp.concatenate([ref[c], ref[c + 1]], axis=1)

    def tall(ref, c):
        return jnp.concatenate([ref[c], ref[c + 1]], axis=0)

    def rows(b):
        return pl.ds(b * 256, 256)

    def mask_scores(a, keys_axis):
        key_low = me + a * (2 * (1 - 2 * mod(chip, 2)))

        def two(base0, base1, axis):
            i = lax.broadcasted_iota(jnp.int32, (256, 256), axis)
            return i + jnp.where(i < PIECE, base0, base1 - PIECE)

        def query_base(c):
            h, par = div(c, TILES), mod(div(c, HEADS), 2)
            low = me + par * (mate - me)
            return (low + h * (pieces - 1 - 2 * low)) * PIECE

        @pl.loop(0, TILES)
        def _(b):
            kpos = two(key_low * PIECE, (pieces - 1 - key_low) * PIECE, keys_axis)
            qpos = two(query_base(2 * b), query_base(2 * b + 1), 1 - keys_axis)
            s = jnp.where(qpos >= kpos, s_buf[b], NEG)
            s_buf[b] = s
            if keys_axis == 0:
                top[b] = jnp.max(s.reshape(32, 8, 256), axis=0)

    def fwd_scores(turn, some, memo):
        for slot, where, base in groups(turn, some):
            kt = tile_of(memo, slot, "k", where)
            twice = jnp.concatenate([kt, kt], axis=1)
            for t in range(HEADS):
                b, c = slot * HEADS + t, base + 2 * t
                if b in some:
                    scaled = jnp.concatenate([wide(c_t.at[:, i], c) for i in range(2)], axis=0)
                    s = jnp.dot(twice, scaled, preferred_element_type=f32)
                    s_buf[b] = s
                    top[b] = jnp.max(s.reshape(32, 8, 256), axis=0)

    def fwd_softmax(turn, some):
        for slot, _, base in groups(turn, some):
            for t in range(HEADS):
                b, c = slot * HEADS + t, base + 2 * t
                if b not in some:
                    continue
                m_old = wide(mst, c)
                m_new = jnp.maximum(m_old, jnp.max(top[b], axis=0, keepdims=True))
                p = jnp.exp2(s_buf[b] - m_new[0:1])
                decay = jnp.exp2(m_old - m_new)
                l_new = wide(lst, c) * decay + jnp.sum(p.reshape(32, 8, 256), axis=0)
                p_buf[rows(b), :] = p.astype(bf16)
                dec[b] = decay
                for j in range(2):
                    cols = slice(j * 128, j * 128 + 128)
                    mst[c + j] = m_new[:, cols]
                    lst[c + j] = l_new[:, cols]

    def fwd_out(turn, some, memo):
        for slot, where, base in groups(turn, some):
            vt = tile_of(memo, slot, "v", where)
            for t in range(HEADS):
                b, c = slot * HEADS + t, base + 2 * t
                if b in some:
                    pv = jnp.dot(vt, p_buf[rows(b), :], preferred_element_type=f32)
                    for j in range(2):
                        cols = slice(j * 128, j * 128 + 128)
                        acc[c + j] = acc[c + j] * dec[b, 0:1, cols] + pv[:, cols]

    def fwd_place(j):
        return place(lookup(jnp.minimum(j, turns - 1), plan.fwd_pairs), jnp.minimum(j, 1))

    every = range(TILES)
    for act in ag_events(plan.fwd_waits[0]):
        act()
    old = fwd_place(me * 0)
    fwd_scores(old, every, {})
    mask_scores(0, 0)
    for act in ag_events(plan.fwd_waits[1]):
        act()
    cur = fwd_place(me * 0 + 1)
    memo = {}
    for b in range(TILES + 1):
        fwd_scores(cur, (b - 1,), memo)
        fwd_softmax(old, (b,))

    def fwd_turn(j, carry):
        old, cur, new = carry
        branch(j, turns, lambda i: ag_events(plan.fwd_waits[i + 1]) if i else [])

        @pl.when(j == plan.fwd_mate)
        def _():
            mask_scores(1, 0)

        after = fwd_place(j + 2)
        memo, memo_old = {}, {}
        for b in range(TILES + 2):
            fwd_scores(new, (b - 2,), memo)
            fwd_softmax(cur, (b - 1,))
            fwd_out(old, (b,), memo_old)
        return cur, new, after

    last = lax.fori_loop(1, turns, fwd_turn, (old, cur, fwd_place(me * 0 + 2)))[0]
    fwd_out(last, every, {})

    def bwd_scores(turn, some, memo):
        for slot, where, base in groups(turn, some):
            for t in range(HEADS):
                b, c = slot * HEADS + t, base + 2 * t
                if b in some:
                    for buf, lhs, kind in ((s_buf, q_s, "t"), (t_buf, g_s, "v")):
                        buf[b] = jnp.dot(tall(lhs, c), tile_of(memo, slot, kind, where), preferred_element_type=f32)

    def bwd_softmax(turn, some):
        for slot, _, base in groups(turn, some):
            for t in range(HEADS):
                b, c = slot * HEADS + t, base + 2 * t
                if b in some:
                    lse, dr = tall(lcol, c), tall(dcol, c)
                    p = jnp.exp2(s_buf[b] * coef - jnp.concatenate([lse, lse], axis=1))
                    p_buf[rows(b), :] = p.astype(bf16)
                    d_buf[rows(b), :] = (p * (t_buf[b] - jnp.concatenate([dr, dr], axis=1))).astype(bf16)

    def bwd_out(turn, some, memo):
        for slot, where, base in groups(turn, some):
            for t in range(HEADS):
                b, c = slot * HEADS + t, base + 2 * t
                if b not in some:
                    continue
                ds = d_buf[rows(b), :]
                dq = lax.dot_general(tile_of(memo, slot, "t", where), ds, (((1,), (1,)), ((), ())), preferred_element_type=f32)
                for j in range(2):
                    dq_s[c + j] += dq[:, j * 128:j * 128 + 128]
                for x, (ref, buf) in enumerate(((q_t, ds), (g_t, p_buf[rows(b), :]))):
                    grad = jnp.dot(wide(ref, c), buf, preferred_element_type=f32)
                    memo[x] = memo[x] + grad if t else grad
                    for j, (pair, par, h) in enumerate(where if t == HEADS - 1 else ()):
                        value = memo[x][:, j * 128:j * 128 + 128]
                        stg[pair, par, x, h] = value + stg[pair, par, x, h] if slot else value

    def bwd_place(j):
        at = jnp.minimum(j, turns - 1)
        return place(lookup(at, plan.bwd_pairs), 1 - div(at + 1, turns))

    x_m = []
    for h in range(2):
        inbox = pl.ds(h * HEADS, HEADS)
        x_m += [mate_copy(theirs(ref, h), box.at[inbox], 4 + 3 * h + i)
                for i, (ref, box) in enumerate(((acc, xacc), (mst, xm), (lst, xl)))]
    for copy in x_m:
        copy.start()
    first = bwd_place(me * 0)
    bwd_scores(first, every, {})
    dq_s[...] = jnp.zeros(dq_s.shape, f32)
    x_r = [mate_copy(own(ref, h), theirs(ref, h), 10 + 2 * j + h) for j, ref in enumerate((lrow, drow)) for h in range(2)]

    for h in range(2):
        for copy in x_m[3 * h:3 * h + 3]:
            copy.wait_recv()
        for head in range(HEADS):
            c, i = h * TILES + head, h * HEADS + head
            m1, m2 = mst[c], xm[i]
            m = jnp.maximum(m1, m2)
            w1, w2 = jnp.exp2(m1 - m), jnp.exp2(m2 - m)
            total = jnp.sum(lst[c] * w1 + xl[i] * w2, axis=0, keepdims=True)
            out = (acc[c] * w1[0:1] + xacc[i] * w2[0:1]) / total
            o_s[head, half(h), :] = out.T.astype(bf16)
            lrow[c] = m + jnp.log2(total)
            rounded = out.astype(bf16).astype(f32)
            drow[c] = jnp.broadcast_to(jnp.sum(rounded * g_t[c].astype(f32), axis=0, keepdims=True), (8, 128))
        for copy in x_r[h::2]:
            copy.start()
    stores = [pltpu.make_async_copy(o_s, o_ref, io.at[8])]
    stores[0].start()

    def columns(c):
        lcol[c] = jnp.broadcast_to(lrow[c, 0:1], (128, 128)).T
        dcol[c] = jnp.broadcast_to(drow[c, 0:1], (128, 128)).T

    for h in range(2):
        pl.loop(h * TILES, h * TILES + HEADS)(columns)
    for copy in x_r:
        copy.wait_recv()
    for h in range(2):
        pl.loop(h * TILES + HEADS, h * TILES + TILES)(columns)

    def rs_add(r, k, x):
        rs_copy(k, x).wait_recv()
        for h in range(2):
            stg[r >> 1, r & 1, x, h] += land[k, x, h]

    def rs_events(sends):
        return ([functools.partial(rs_add, r, k, x) for r, x in sends for k in plan.bwd[x].kids[r]]
                + [rs_copy(r, x).start for r, x in sends])

    def clear(pair):
        for i in range(4):
            stg[pair, i // 2, i % 2, 1] = jnp.zeros((128, 128), f32)

    def bwd_start(j, carry):
        _, cur, new = carry
        if turns < 4:
            mask_scores(turns - 1 - j, 1)
        after = bwd_place(j + 2)
        memo = {}
        for b in range(TILES + 1):
            bwd_softmax(cur, (b,))
            bwd_scores(new, (b - 1,), memo)

        @pl.when(j == 0)
        def _():
            clear(cur[0])
            bwd_out(cur, every, {})
            for act in rs_events(plan.bwd_sends[0]):
                act()

        return cur, new, after

    def bwd_turn(j, carry):
        old, cur, new = carry
        branch(j, turns, lambda i: rs_events(plan.bwd_sends[i - 1]) if i > 1 else [])

        @pl.when(j < turns - 1)
        def _():
            clear(old[0])

        @pl.when(j >= turns - 2)
        def _():
            mask_scores(turns - 1 - j, 1)

        after = bwd_place(j + 2)
        memo, memo_old = {}, {}
        for b in range(TILES + 2):
            bwd_out(old, (b,), memo_old)
            bwd_softmax(cur, (b - 1,))
            bwd_scores(new, (b - 2,), memo)
        return cur, new, after

    start = lax.fori_loop(0, 2, bwd_start, (first, first, bwd_place(me * 0 + 1)))
    last = lax.fori_loop(2, turns, bwd_turn, start)[0]
    for act in rs_events(plan.bwd_sends[turns - 1]):
        act()
    bwd_out(last, every, {})

    x_d = [mate_copy(theirs(dq_s, h), xdq.at[pl.ds(h * HEADS, HEADS)], 14 + h) for h in range(2)]
    for copy in x_d:
        copy.start()
    for unit in plan.bwd_sends[turns]:
        for act in rs_events([unit]):
            act()
    for h in range(2):
        x_d[h].wait_recv()
        for head in range(HEADS):
            total = (dq_s[h * TILES + head] + xdq[h * HEADS + head]) * SCALE
            dq_o[head, half(h), :] = total.T.astype(bf16)
    stores.append(pltpu.make_async_copy(dq_o, dq_ref, io.at[9]))
    stores[1].start()
    for k, x in plan.bwd_last:
        rs_add(0, k, x)
    for x, (buf, ref, factor) in enumerate(((dk_o, dk_ref, SCALE), (dv_o, dv_ref, 1.0))):
        for h in range(2):
            buf[half(h), :] = (stg[0, 0, x, h] * factor).T.astype(bf16)
        stores.append(pltpu.make_async_copy(buf, ref, io.at[10 + x]))
        stores[-1].start()

    for k in range(1, plan.blocks):
        for x in range(2):
            ag_copy(k, x).wait_send()
            rs_copy(k, x).wait_send()
    for copy in x_q + x_m + x_r + x_d:
        copy.wait_send()
    for copy in stores:
        copy.wait()


def relay(*refs):
    count = (len(refs) - 1) // 3
    src, dst, buf, sem = refs[:count], refs[count:2 * count], refs[2 * count:3 * count], refs[3 * count]
    into = [pltpu.make_async_copy(a, b, sem.at[i]) for i, (a, b) in enumerate(zip(src, buf))]
    out = [pltpu.make_async_copy(b, c, sem.at[count + i]) for i, (b, c) in enumerate(zip(buf, dst))]
    for copy in into:
        copy.start()
    for i in range(count):
        into[i].wait()
        out[i].start()
    for copy in out:
        copy.wait()


def solution(mesh):
    size = mesh.shape["ctx"]
    plan = Plan(int(math.log2(size)) - 1)
    spec = P("data", "ctx", None, None)
    n = plan.blocks
    f32, bf16 = jnp.float32, jnp.bfloat16
    vm, sem = pltpu.VMEM, pltpu.SemaphoreType.DMA

    def local(queries, keys, values, grad_out):
        tokens = queries.shape[1]
        q = queries[0].transpose(1, 0, 2)
        g = grad_out[0].transpose(1, 0, 2)
        tile = (128, 128)
        big = jax.ShapeDtypeStruct((HEADS, tokens, HD), bf16)
        small = jax.ShapeDtypeStruct((tokens, HD), bf16)
        anywhere = pl.BlockSpec(memory_space=pl.ANY)
        twenty, ten, stat, few = (2 * TILES,) + tile, (TILES,) + tile, (2 * TILES, 8, 128), (TILES, 8, 128)
        results = pl.pallas_call(
            functools.partial(kernel, plan),
            out_shape=(big, big, small, small),
            in_specs=[anywhere] * 4,
            out_specs=(anywhere,) * 4,
            scratch_shapes=[
                vm((n // 2, 2, 2, 2) + tile, bf16), vm((n // 2, 2, 2, 2) + tile, f32), vm((n, 2, 2) + tile, f32),
                vm((TILES, 256, 256), f32), vm((TILES, 256, 256), f32), vm((TILES * 256, 256), bf16), vm((TILES * 256, 256), bf16),
                vm((TILES, 8, 256), f32),
                vm(twenty, bf16), vm(twenty, bf16), vm((2,) + tile, bf16), vm(twenty, bf16), vm(twenty, bf16),
                vm((2 * TILES, 2) + tile, bf16),
                vm(twenty, f32), vm(stat, f32), vm(stat, f32), vm((TILES, 8, 256), f32),
                vm(ten, f32), vm(few, f32), vm(few, f32), vm(stat, f32), vm(stat, f32), vm(twenty, f32), vm(twenty, f32),
                vm(twenty, f32), vm(ten, f32),
                vm(big.shape, bf16), vm(big.shape, bf16), vm(small.shape, bf16), vm(small.shape, bf16),
                sem((n, 2)), sem((n, 2)), sem((n, 2)), sem((n, 2)), sem((16,)), sem((16,)), sem((12,)),
            ],
            compiler_params=pltpu.CompilerParams(collective_id=0, has_side_effects=True, vmem_limit_bytes=67043328),
            cost_estimate=pl.CostEstimate(flops=14 * 640 * PIECE * n * 2 * HD, bytes_accessed=4 << 20, transcendentals=0),
        )(q, keys[0, :, 0], values[0, :, 0], g)
        o, dq, dk, dv = pl.pallas_call(
            relay,
            out_shape=(big, big, small, small),
            in_specs=[anywhere] * 4,
            out_specs=(anywhere,) * 4,
            scratch_shapes=[vm(x.shape, bf16) for x in (big, big, small, small)] + [sem((8,))],
            cost_estimate=pl.CostEstimate(flops=1 << 20, bytes_accessed=2 << 20, transcendentals=0),
        )(*results)
        return (o.transpose(1, 0, 2)[None], dq.transpose(1, 0, 2)[None], dk[None, :, None], dv[None, :, None])

    return jax.shard_map(local, mesh=mesh, in_specs=(spec,) * 4, out_specs=(spec,) * 4, check_vma=False)
```

```python
import functools
import math

import jax
import jax.numpy as jnp
from jax import lax
from jax.experimental import pallas as pl
from jax.experimental.pallas import tpu as pltpu
from jax.sharding import PartitionSpec as P

MESH = pl.DeviceIdType.MESH
NEG = -1e30
HD = 128
HEADS = 5
PIECE = 128
SCALE = HD ** -0.5
LOG2E = 1.4426950408889634
TILES = 2 * HEADS
SPAN = HEADS * PIECE

KEY_TREE = "011222133332330444044204331303450512252553132154554251534405024"
VALUE_TREE = "011202133303032404124114441201150505210501022525540551434312353"
DK_TREE = "010222133132320404040144013222455152212303525124550544534132251"
DV_TREE = "011221233112332404420104340431355155511535030505014404035353440"
BWD_ORDER = "vuntrfmplsj7beodk6cq35haig98241"


def popcount(value):
    return bin(value).count("1")


class Tree:
    def __init__(self, dims, links):
        blocks = 1 << dims
        if dims == 6:
            self.link = [None] + [int(d) for d in links]
        else:
            self.link = [None] * blocks
            count = [0] * dims
            for r in sorted(range(1, blocks), key=popcount):
                self.link[r] = min((d for d in range(dims) if (r >> d) & 1), key=lambda d: count[d])
                count[self.link[r]] += 1
        self.kids = {r: [k for k in range(1, blocks) if k & ~(1 << self.link[k]) == r] for r in range(blocks)}
        height = {}
        for r in sorted(range(blocks), key=popcount, reverse=True):
            height[r] = max([1 + height[k] for k in self.kids[r]], default=0)
        for r in self.kids:
            self.kids[r].sort(key=lambda k: -height[k])


class Plan:
    def __init__(self, dims):
        self.dims = dims
        self.blocks = 1 << dims
        self.turns = self.blocks // 2 + 1
        self.fwd = [Tree(dims, KEY_TREE), Tree(dims, VALUE_TREE)]
        self.bwd = [Tree(dims, DK_TREE), Tree(dims, DV_TREE)]
        self.forward()
        self.backward()

    def forward(self, unit_us=1.41, hop_us=1.9, turn_us=0.78):
        free = [0.0] * self.dims
        due = {}
        done = {(0, 0), (0, 1)}
        now = 1.0
        steps, waits, ready, order = [], [], [0], []

        def send(r, x):
            for k in self.fwd[x].kids[r]:
                d = self.fwd[x].link[k]
                free[d] = max(free[d], now) + unit_us
                due[k, x] = free[d] + hop_us

        now = 0.0
        send(0, 0)
        send(0, 1)
        now = 1.0
        while True:
            for unit in sorted((u for u in due if u not in done and due[u] <= now), key=lambda u: (due[u], u)):
                done.add(unit)
                now += 0.02
                send(*unit)
                waits.append(unit)
                if unit[1] == 0 and (unit[0] ^ 1, 0) in done:
                    ready.append(unit[0] >> 1)
            turn = len(steps)
            late = order[max(turn - 2, 0):turn - 1] if turn < self.turns else order[turn - 2:]
            lacking = [r for pair in late for r in (2 * pair, 2 * pair + 1) if (r, 1) not in done]
            if turn == 2 < self.turns:
                lacking = []
            if lacking or not (ready or turn == self.turns):
                now = max(now, min(due[u] for u in due if u not in done))
                continue
            if turn == self.turns:
                break
            order.append(ready.pop(0))
            steps.append(waits)
            waits = []
            now += turn_us if turn else 0.0
        self.fwd_waits = steps + [waits]
        self.fwd_pairs = order
        self.fwd_mate = max(i for i, pair in enumerate(order) if pair == 0)

    def backward(self, unit_us=2.9, hop_us=2.1, turn_us=1.55, add_us=0.035):
        if self.dims == 6:
            order = [int(c, 32) for c in BWD_ORDER]
        else:
            order = sorted(range(1, self.blocks // 2), key=lambda pair: -popcount(pair))
        order += [0, 0]
        free = [0.0] * self.dims
        due = {}
        waiting, sends, steps = set(), [], []
        now = 1.57

        def kids(unit):
            return [(k, unit[1]) for k in self.bwd[unit[1]].kids[unit[0]]]

        def flush():
            nonlocal now
            able = True
            while able:
                able = [u for u in waiting if all(due.get(k, 1e9) <= now for k in kids(u))]
                for unit in sorted(able, key=lambda u: (-popcount(u[0]), u)):
                    waiting.discard(unit)
                    now += add_us * len(kids(unit)) + 0.01
                    d = self.bwd[unit[1]].link[unit[0]]
                    free[d] = max(free[d], now) + unit_us
                    due[unit] = free[d] + hop_us
                    sends.append(unit)

        for i, pair in enumerate(order):
            waiting |= {(r, x) for r in (2 * pair, 2 * pair + 1) for x in range(2) if r} if i < len(order) - 1 else set()
            flush()
            steps.append(sends)
            sends = []
            if i == 0:
                now += 0.85
                flush()
                steps.append(sends)
                sends = []
            now += turn_us if i < len(order) - 1 else 0.0
        while waiting:
            now = max(now, min(max(due.get(k, 1e9) for k in kids(u)) for u in waiting))
            flush()
        self.bwd_sends = steps[:-1] + [steps[-1] + sends]
        self.bwd_pairs = order
        self.bwd_last = sorted((u for x in range(2) for u in kids((0, x))), key=lambda u: due[u])


def div(a, b):
    return lax.div(a, jnp.int32(b))


def mod(a, b):
    return lax.rem(a, jnp.int32(b))


def xor(a, b):
    return a + b - 2 * a * b


def lookup(index, table):
    level = [jnp.int32(v) for v in table]
    bit = 1
    while len(level) > 1:
        odd = mod(div(index, bit), 2) == 1
        nxt = [jnp.where(odd, level[i + 1], level[i]) for i in range(0, len(level) - 1, 2)]
        level = nxt + level[2 * len(nxt):]
        bit *= 2
    return level[0]


def branch(index, count, leaf):
    once = div(index, count) + 1

    def pick(low, high):
        if high - low == 1:
            acts = leaf(low)
            if acts:
                pl.loop(0, once)(lambda _: [act() for act in acts] and None)
            return
        mid = (low + high) // 2
        lax.cond(index < mid, lambda: pick(low, mid), lambda: pick(mid, high))

    pick(0, count)


def kernel(plan, q_ref, k_ref, v_ref, g_ref, o_ref, dq_ref, dk_ref, dv_ref,
           kv, stg, land, s_buf, t_buf, p_buf, d_buf, top, q_s, g_s, v_s, q_t, g_t, c_t, acc, mst, lst, dec,
           xacc, xm, xl, lrow, drow, lcol, dcol, dq_s, xdq, o_s, dq_o, dk_o, dv_o,
           ag_send, ag_recv, rs_send, rs_recv, x_send, x_recv, io):
    dims, turns = plan.dims, plan.turns
    pieces = 4 * plan.blocks
    f32, bf16 = jnp.float32, jnp.bfloat16
    me = lax.axis_index("ctx")
    core = mod(me, 2)
    chip = div(me, 2)
    bits = [mod(div(chip, 1 << d), 2) for d in range(dims)]
    gray = [xor(bits[d], bits[d + 1]) if d % 2 == 0 and d + 1 < dims else bits[d] for d in range(dims)]
    nbr = []
    for d in range(dims):
        other = chip + (1 - 2 * bits[d]) * (1 << d)
        if d % 2:
            other = other + (1 - 2 * bits[d - 1]) * (1 << (d - 1))
        nbr.append(2 * other + core)
    mate = me + 1 - 2 * core
    my_pair = div(chip, 2)

    barrier = pltpu.get_barrier_semaphore()
    for dev in nbr + [mate]:
        pl.semaphore_signal(barrier, inc=1, device_id={"ctx": dev}, device_id_type=MESH)

    def half(h):
        return pl.ds(h * PIECE, PIECE)

    loads = []
    for h in range(2):
        loads += [pltpu.make_async_copy(v_ref.at[half(h)], v_s.at[h], io.at[h]),
                  pltpu.make_async_copy(k_ref.at[half(h)], kv.at[0, 0, 0, h], io.at[2 + h])]
    for h in range(2):
        for j, (src, dst) in enumerate(((q_ref, q_s), (g_ref, g_s))):
            loads.append(pltpu.make_async_copy(src.at[:, half(h)], dst.at[h, pl.ds(0, HEADS)], io.at[4 + 2 * j + h]))
    for copy in loads:
        copy.start()
    mst[...] = jnp.full(mst.shape, NEG, f32)
    lst[...] = jnp.zeros(lst.shape, f32)
    acc[...] = jnp.zeros(acc.shape, f32)
    dec[...] = jnp.ones(dec.shape, f32)
    p_buf[...] = jnp.zeros(p_buf.shape, bf16)
    for copy in loads[:4]:
        copy.wait()
    for h in range(2):
        kv[0, 0, 1, h] = v_s[h].T

    pl.semaphore_wait(barrier, dims + 1)

    def ag_copy(k, x):
        d = plan.fwd[x].link[k]
        r = k ^ (1 << d)
        return pltpu.make_async_remote_copy(
            src_ref=kv.at[r >> 1, r & 1, x], dst_ref=kv.at[k >> 1, k & 1, x], send_sem=ag_send.at[k, x],
            recv_sem=ag_recv.at[k, x], device_id={"ctx": nbr[d]}, device_id_type=MESH)

    def rs_copy(r, x):
        return pltpu.make_async_remote_copy(
            src_ref=stg.at[r >> 1, r & 1, x], dst_ref=land.at[r, x], send_sem=rs_send.at[r, x], recv_sem=rs_recv.at[r, x],
            device_id={"ctx": nbr[plan.bwd[x].link[r]]}, device_id_type=MESH)

    def mate_copy(src, dst, sem):
        return pltpu.make_async_remote_copy(src_ref=src, dst_ref=dst, send_sem=x_send.at[sem], recv_sem=x_recv.at[sem],
                                            device_id={"ctx": mate}, device_id_type=MESH)

    ours, theirs = pl.ds(0, SPAN), pl.ds(SPAN, SPAN)

    for x in range(2):
        for k in plan.fwd[x].kids[0]:
            ag_copy(k, x).start()
    for copy in loads[4:]:
        copy.wait()
    x_q = [mate_copy(ref.at[h, pl.ds(0, HEADS)], ref.at[h, pl.ds(HEADS, HEADS)], 2 * j + h)
           for j, ref in enumerate((q_s, g_s)) for h in range(2)]
    for copy in x_q:
        copy.start()

    def ag_events(waits):
        return [act for r, x in waits for act in [ag_copy(r, x).wait_recv] + [ag_copy(k, x).start for k in plan.fwd[x].kids[r]]]

    coef = SCALE * LOG2E

    def transposes(h):
        def turn(i):
            cols = pl.ds(pl.multiple_of(i * 128, 128), 128)
            turned = q_s[h, i].T
            q_t[h, :, cols] = turned
            g_t[h, :, cols] = g_s[h, i].T
            scaled = turned.astype(f32) * coef
            high = scaled.astype(bf16)
            c_t[h, pl.ds(0, HD), cols] = high
            c_t[h, pl.ds(HD, HD), cols] = (scaled - high.astype(f32)).astype(bf16)

        return turn

    for h in range(2):
        pl.loop(0, HEADS)(transposes(h))
    for copy in x_q:
        copy.wait_recv()
    for h in range(2):
        pl.loop(HEADS, TILES)(transposes(h))

    def is_future(pair):
        rel = [mod(div(pair, 1 << (d - 1)), 2) for d in range(1, dims)]
        gp = [None] + [xor(gray[d], rel[d - 1]) for d in range(1, dims)]
        other = gp[1] if dims > 1 else 0
        for d in range(2, dims):
            bit = xor(gp[d], gp[d + 1]) if d % 2 == 0 and d + 1 < dims else gp[d]
            other = other + bit * (1 << (d - 1))
        return div(other - my_pair + plan.blocks, plan.blocks)

    def place(pair, a):
        mine = div(plan.blocks // 2 - pair, plan.blocks // 2)
        fut = is_future(pair)
        turn = (pair,)
        for slot in range(2):
            h = (1 - mine) * fut * slot
            turn += (mine * a, h, mine * a + 1 - mine, mine + h, mine * slot + (1 - mine) * (fut + (1 - fut) * slot))
        return turn

    def groups(turn, some):
        for slot in range(2):
            if not any(slot * HEADS <= b < slot * HEADS + HEADS for b in some):
                continue
            p0, h0, p1, h1, qg = turn[1 + 5 * slot:6 + 5 * slot]
            yield slot, ((turn[0], p0, h0), (turn[0], p1, h1)), qg

    def key_tile(where):
        return jnp.concatenate([kv[pair, par, 0, h] for pair, par, h in where], axis=0)

    def value_tile_t(where):
        return jnp.concatenate([kv[pair, par, 1, h] for pair, par, h in where], axis=1)

    def tile_of(memo, slot, kind, where):
        key = (kind, slot)
        if key not in memo:
            memo[key] = value_tile_t(where) if kind == "v" else key_tile(where) if kind == "k" else key_tile(where).T
        return memo[key]

    def tall(ref, qg, t):
        return ref[qg, pl.ds(2 * t, 2)].reshape(256, 128)

    def cols_of(t):
        return pl.ds(t * 256, 256)

    def rows(b):
        return pl.ds(b * 256, 256)

    def mask_scores(a, keys_axis):
        key_low = me + a * (2 * (1 - 2 * mod(chip, 2)))

        def two(base0, base1, axis):
            i = lax.broadcasted_iota(jnp.int32, (256, 256), axis)
            return i + jnp.where(i < PIECE, base0, base1 - PIECE)

        def query_base(c):
            h, par = div(c, TILES), mod(div(c, HEADS), 2)
            low = me + par * (mate - me)
            return (low + h * (pieces - 1 - 2 * low)) * PIECE

        @pl.loop(0, TILES)
        def _(b):
            kpos = two(key_low * PIECE, (pieces - 1 - key_low) * PIECE, keys_axis)
            qpos = two(query_base(2 * b), query_base(2 * b + 1), 1 - keys_axis)
            s = jnp.where(qpos >= kpos, s_buf[b], NEG)
            s_buf[b] = s
            if keys_axis == 0:
                top[b] = jnp.max(s.reshape(32, 8, 256), axis=0)

    def fwd_scores(turn, some, memo):
        for slot, where, qg in groups(turn, some):
            kt = tile_of(memo, slot, "k", where)
            twice = jnp.concatenate([kt, kt], axis=1)
            for t in range(HEADS):
                b, cols = slot * HEADS + t, cols_of(t)
                if b in some:
                    s = jnp.dot(twice, c_t[qg, :, cols], preferred_element_type=f32)
                    s_buf[b] = s
                    top[b] = jnp.max(s.reshape(32, 8, 256), axis=0)

    def fwd_softmax(turn, some):
        for slot, _, qg in groups(turn, some):
            for t in range(HEADS):
                b, cols = slot * HEADS + t, cols_of(t)
                if b not in some:
                    continue
                m_old = mst[qg, :, cols]
                m_new = jnp.maximum(m_old, jnp.max(top[b], axis=0, keepdims=True))
                p = jnp.exp2(s_buf[b] - m_new[0:1])
                decay = jnp.exp2(m_old - m_new)
                lst[qg, :, cols] = lst[qg, :, cols] * decay + jnp.sum(p.reshape(32, 8, 256), axis=0)
                p_buf[rows(b), :] = p.astype(bf16)
                dec[b] = decay
                mst[qg, :, cols] = m_new

    def fwd_out(turn, some, memo):
        for slot, where, qg in groups(turn, some):
            vt = tile_of(memo, slot, "v", where)
            for t in range(HEADS):
                b, cols = slot * HEADS + t, cols_of(t)
                if b in some:
                    pv = jnp.dot(vt, p_buf[rows(b), :], preferred_element_type=f32)
                    acc[qg, :, cols] = acc[qg, :, cols] * dec[b, 0:1] + pv

    def fwd_place(j):
        return place(lookup(jnp.minimum(j, turns - 1), plan.fwd_pairs), jnp.minimum(j, 1))

    every = range(TILES)
    for act in ag_events(plan.fwd_waits[0]):
        act()
    first = fwd_place(me * 0)
    fwd_scores(first, every, {})

    def fwd_turn(j, carry):
        old, cur, new = carry
        branch(j, turns, lambda i: ag_events(plan.fwd_waits[i + 1]))

        @pl.when((j == 0) | (j == plan.fwd_mate))
        def _():
            mask_scores(jnp.minimum(j, 1), 0)

        after = fwd_place(j + 2)
        memo, memo_old = {}, {}
        for b in range(TILES + 2):
            fwd_scores(new, (b - 2,), memo)
            fwd_softmax(cur, (b - 1,))
            fwd_out(old, (b,), memo_old)
        return cur, new, after

    old, cur, _ = lax.fori_loop(0, turns - 1, fwd_turn, (first, first, fwd_place(me * 0 + 1)))
    for act in ag_events(plan.fwd_waits[turns]):
        act()
    if plan.fwd_mate == turns - 1:
        mask_scores(1, 0)
    memo = {}
    for b in range(TILES + 1):
        fwd_softmax(cur, (b - 1,))
        fwd_out(old, (b,), memo)
    fwd_out(cur, every, {})

    def bwd_scores(turn, some, memo):
        for slot, where, qg in groups(turn, some):
            for t in range(HEADS):
                b, cols = slot * HEADS + t, cols_of(t)
                if b in some:
                    for buf, lhs, kind in ((s_buf, q_s, "t"), (t_buf, g_s, "v")):
                        buf[b] = jnp.dot(tall(lhs, qg, t), tile_of(memo, slot, kind, where), preferred_element_type=f32)

    def bwd_softmax(turn, some):
        for slot, _, qg in groups(turn, some):
            for t in range(HEADS):
                b, cols = slot * HEADS + t, cols_of(t)
                if b in some:
                    lse, dr = tall(lcol, qg, t), tall(dcol, qg, t)
                    p = jnp.exp2(s_buf[b] * coef - jnp.concatenate([lse, lse], axis=1))
                    p_buf[rows(b), :] = p.astype(bf16)
                    d_buf[rows(b), :] = (p * (t_buf[b] - jnp.concatenate([dr, dr], axis=1))).astype(bf16)

    def bwd_out(turn, some, memo):
        for slot, where, qg in groups(turn, some):
            for t in range(HEADS):
                b, cols = slot * HEADS + t, cols_of(t)
                if b not in some:
                    continue
                ds = d_buf[rows(b), :]
                dq = lax.dot_general(tile_of(memo, slot, "t", where), ds, (((1,), (1,)), ((), ())), preferred_element_type=f32)
                dq_s[qg, :, cols] += dq
                for x, (ref, buf) in enumerate(((q_t, ds), (g_t, p_buf[rows(b), :]))):
                    grad = jnp.dot(ref[qg, :, cols], buf, preferred_element_type=f32)
                    memo[x] = memo[x] + grad if t else grad
                    for j, (pair, par, h) in enumerate(where if t == HEADS - 1 else ()):
                        value = memo[x][:, j * 128:j * 128 + 128]
                        stg[pair, par, x, h] = value + stg[pair, par, x, h] if slot else value

    def bwd_place(j):
        at = jnp.minimum(j, turns - 1)
        return place(lookup(at, plan.bwd_pairs), 1 - div(at + 1, turns))

    x_m = [mate_copy(ref.at[h, :, theirs], box.at[h], 4 + 3 * h + i)
           for h in range(2) for i, (ref, box) in enumerate(((acc, xacc), (mst, xm), (lst, xl)))]
    for copy in x_m:
        copy.start()
    first = bwd_place(me * 0)
    bwd_scores(first, every, {})
    dq_s[...] = jnp.zeros(dq_s.shape, f32)
    x_r = [mate_copy(ref.at[h, :, ours], ref.at[h, :, theirs], 10 + 2 * j + h) for j, ref in enumerate((lrow, drow)) for h in range(2)]

    for h in range(2):
        for copy in x_m[3 * h:3 * h + 3]:
            copy.wait_recv()
        for head in range(HEADS):
            cols = pl.ds(head * PIECE, PIECE)
            m1, m2 = mst[h, :, cols], xm[h, :, cols]
            m = jnp.maximum(m1, m2)
            w1, w2 = jnp.exp2(m1 - m), jnp.exp2(m2 - m)
            total = jnp.sum(lst[h, :, cols] * w1 + xl[h, :, cols] * w2, axis=0, keepdims=True)
            out = (acc[h, :, cols] * w1[0:1] + xacc[h, :, cols] * w2[0:1]) / total
            o_s[head, half(h), :] = out.T.astype(bf16)
            lrow[h, :, cols] = m + jnp.log2(total)
            rounded = out.astype(bf16).astype(f32)
            d = jnp.sum(rounded * g_t[h, :, cols].astype(f32), axis=0, keepdims=True)
            drow[h, :, cols] = jnp.broadcast_to(d, (8, 128))
        for copy in x_r[h::2]:
            copy.start()
    stores = [pltpu.make_async_copy(o_s, o_ref, io.at[8])]
    stores[0].start()

    def columns(h, i):
        cols = pl.ds(i * 128, 128)
        for row, col in ((lrow, lcol), (drow, dcol)):
            col[h, i] = jnp.broadcast_to(row[h, 0:1, cols], (128, 128)).T

    def rs_add(r, k, x):
        rs_copy(k, x).wait_recv()
        for h in range(2):
            stg[r >> 1, r & 1, x, h] += land[k, x, h]

    def rs_events(sends):
        return ([functools.partial(rs_add, r, k, x) for r, x in sends for k in plan.bwd[x].kids[r]]
                + [rs_copy(r, x).start for r, x in sends])

    def clear(pair):
        for i in range(4):
            stg[pair, i // 2, i % 2, 1] = jnp.zeros((128, 128), f32)

    for i in range(TILES):
        columns(i // HEADS, i % HEADS)
    if turns < 4:
        mask_scores(turns - 1, 1)
    second, third = bwd_place(me * 0 + 1), bwd_place(me * 0 + 2)
    memo = {}
    early = [b for b in every if b % HEADS < HEADS // 2]
    for b in early:
        bwd_softmax(first, (b,))
        bwd_scores(second, (b,), memo)
    for copy in x_r:
        copy.wait_recv()
    for i in range(TILES):
        columns(i // HEADS, HEADS + i % HEADS)
    memo = {}
    for b in every:
        if b not in early:
            bwd_softmax(first, (b,))
            bwd_scores(second, (b,), memo)
    clear(first[0])
    bwd_out(first, every, {})
    for act in rs_events(plan.bwd_sends[0]):
        act()
    if turns < 4:
        mask_scores(turns - 2, 1)
    memo = {}
    for b in range(TILES + 1):
        bwd_softmax(second, (b,))
        bwd_scores(third, (b - 1,), memo)

    def bwd_turn(j, carry):
        old, cur, new = carry
        branch(j, turns, lambda i: rs_events(plan.bwd_sends[i - 1]) if i > 1 else [])

        @pl.when(j < turns - 1)
        def _():
            clear(old[0])

        @pl.when(j >= turns - 2)
        def _():
            mask_scores(turns - 1 - j, 1)

        after = bwd_place(j + 2)
        memo, memo_old = {}, {}
        for b in range(TILES + 2):
            bwd_out(old, (b,), memo_old)
            bwd_softmax(cur, (b - 1,))
            bwd_scores(new, (b - 2,), memo)
        return cur, new, after

    last = lax.fori_loop(2, turns, bwd_turn, (second, third, bwd_place(me * 0 + 3)))[0]
    for act in rs_events(plan.bwd_sends[turns - 1]):
        act()
    bwd_out(last, every, {})

    x_d = [mate_copy(dq_s.at[h, :, theirs], xdq.at[h], 14 + h) for h in range(2)]
    for copy in x_d:
        copy.start()
    for unit in plan.bwd_sends[turns]:
        for act in rs_events([unit]):
            act()
    for h in range(2):
        x_d[h].wait_recv()
        for head in range(HEADS):
            cols = pl.ds(head * PIECE, PIECE)
            total = (dq_s[h, :, cols] + xdq[h, :, cols]) * SCALE
            dq_o[head, half(h), :] = total.T.astype(bf16)
    stores.append(pltpu.make_async_copy(dq_o, dq_ref, io.at[9]))
    stores[1].start()
    for k, x in plan.bwd_last:
        rs_add(0, k, x)
    for x, (buf, ref, factor) in enumerate(((dk_o, dk_ref, SCALE), (dv_o, dv_ref, 1.0))):
        for h in range(2):
            buf[half(h), :] = (stg[0, 0, x, h] * factor).T.astype(bf16)
        stores.append(pltpu.make_async_copy(buf, ref, io.at[10 + x]))
        stores[-1].start()

    for k in range(1, plan.blocks):
        for x in range(2):
            ag_copy(k, x).wait_send()
            rs_copy(k, x).wait_send()
    for copy in x_q + x_m + x_r + x_d:
        copy.wait_send()
    for copy in stores:
        copy.wait()


def relay(*refs):
    count = (len(refs) - 1) // 3
    src, dst, buf, sem = refs[:count], refs[count:2 * count], refs[2 * count:3 * count], refs[3 * count]
    into = [pltpu.make_async_copy(a, b, sem.at[i]) for i, (a, b) in enumerate(zip(src, buf))]
    out = [pltpu.make_async_copy(b, c, sem.at[count + i]) for i, (b, c) in enumerate(zip(buf, dst))]
    for copy in into:
        copy.start()
    for i in range(count):
        into[i].wait()
        out[i].start()
    for copy in out:
        copy.wait()


def solution(mesh):
    size = mesh.shape["ctx"]
    plan = Plan(int(math.log2(size)) - 1)
    spec = P("data", "ctx", None, None)
    n = plan.blocks
    f32, bf16 = jnp.float32, jnp.bfloat16
    vm, sem = pltpu.VMEM, pltpu.SemaphoreType.DMA

    def local(queries, keys, values, grad_out):
        tokens = queries.shape[1]
        q = queries[0].transpose(1, 0, 2)
        g = grad_out[0].transpose(1, 0, 2)
        tile = (128, 128)
        big = jax.ShapeDtypeStruct((HEADS, tokens, HD), bf16)
        small = jax.ShapeDtypeStruct((tokens, HD), bf16)
        anywhere = pl.BlockSpec(memory_space=pl.ANY)
        rows, wide, half_wide = (2, TILES) + tile, (2, HD, 2 * SPAN), (2, HD, SPAN)
        stat, few = (2, 8, 2 * SPAN), (2, 8, SPAN)
        results = pl.pallas_call(
            functools.partial(kernel, plan),
            out_shape=(big, big, small, small),
            in_specs=[anywhere] * 4,
            out_specs=(anywhere,) * 4,
            scratch_shapes=[
                vm((n // 2, 2, 2, 2) + tile, bf16), vm((n // 2, 2, 2, 2) + tile, f32), vm((n, 2, 2) + tile, f32),
                vm((TILES, 256, 256), f32), vm((TILES, 256, 256), f32), vm((TILES * 256, 256), bf16), vm((TILES * 256, 256), bf16),
                vm((TILES, 8, 256), f32),
                vm(rows, bf16), vm(rows, bf16), vm((2,) + tile, bf16), vm(wide, bf16), vm(wide, bf16), vm((2, 2 * HD, 2 * SPAN), bf16),
                vm(wide, f32), vm(stat, f32), vm(stat, f32), vm((TILES, 8, 256), f32),
                vm(half_wide, f32), vm(few, f32), vm(few, f32), vm(stat, f32), vm(stat, f32), vm(rows, f32), vm(rows, f32),
                vm(wide, f32), vm(half_wide, f32),
                vm(big.shape, bf16), vm(big.shape, bf16), vm(small.shape, bf16), vm(small.shape, bf16),
                sem((n, 2)), sem((n, 2)), sem((n, 2)), sem((n, 2)), sem((16,)), sem((16,)), sem((12,)),
            ],
            compiler_params=pltpu.CompilerParams(collective_id=0, has_side_effects=True, vmem_limit_bytes=67043328),
            cost_estimate=pl.CostEstimate(flops=14 * 640 * PIECE * n * 2 * HD, bytes_accessed=4 << 20, transcendentals=0),
        )(q, keys[0, :, 0], values[0, :, 0], g)
        o, dq, dk, dv = pl.pallas_call(
            relay,
            out_shape=(big, big, small, small),
            in_specs=[anywhere] * 4,
            out_specs=(anywhere,) * 4,
            scratch_shapes=[vm(x.shape, bf16) for x in (big, big, small, small)] + [sem((8,))],
            cost_estimate=pl.CostEstimate(flops=1 << 20, bytes_accessed=2 << 20, transcendentals=0),
        )(*results)
        return (o.transpose(1, 0, 2)[None], dq.transpose(1, 0, 2)[None], dk[None, :, None], dv[None, :, None])

    return jax.shard_map(local, mesh=mesh, in_specs=(spec,) * 4, out_specs=(spec,) * 4, check_vma=False)
```

```python
import functools
import math

import jax
import jax.numpy as jnp
from jax import lax
from jax.experimental import pallas as pl
from jax.experimental.pallas import tpu as pltpu
from jax.sharding import PartitionSpec as P

MESH = pl.DeviceIdType.MESH
NEG = -1e30
HD = 128
HEADS = 5
PIECE = 128
SCALE = HD ** -0.5
LOG2E = 1.4426950408889634
TILES = 2 * HEADS
SPAN = HEADS * PIECE

KEY_TREE = "011222133332330444044204331303450512252553132154554251534405024"
VALUE_TREE = "011202133303032404124114441201150505210501022525540551434312353"
DK_TREE = "010222133132320404040144013222455152212303525124550544534132251"
DV_TREE = "011221233112332404420104340431355155511535030505014404035353440"
BWD_ORDER = "vuntrfmplsj7beodk6cq35haig98241"


def popcount(value):
    return bin(value).count("1")


class Tree:
    def __init__(self, dims, links):
        blocks = 1 << dims
        if dims == 6:
            self.link = [None] + [int(d) for d in links]
        else:
            self.link = [None] * blocks
            count = [0] * dims
            for r in sorted(range(1, blocks), key=popcount):
                self.link[r] = min((d for d in range(dims) if (r >> d) & 1), key=lambda d: count[d])
                count[self.link[r]] += 1
        self.kids = {r: [k for k in range(1, blocks) if k & ~(1 << self.link[k]) == r] for r in range(blocks)}
        height = {}
        for r in sorted(range(blocks), key=popcount, reverse=True):
            height[r] = max([1 + height[k] for k in self.kids[r]], default=0)
        for r in self.kids:
            self.kids[r].sort(key=lambda k: -height[k])


class Plan:
    def __init__(self, dims):
        self.dims = dims
        self.blocks = 1 << dims
        self.turns = self.blocks // 2 + 1
        self.fwd = [Tree(dims, KEY_TREE), Tree(dims, VALUE_TREE)]
        self.bwd = [Tree(dims, DK_TREE), Tree(dims, DV_TREE)]
        self.forward()
        self.backward()

    def forward(self, unit_us=1.41, hop_us=1.9, turn_us=0.78):
        free = [0.0] * self.dims
        due = {}
        done = {(0, 0), (0, 1)}
        now = 1.0
        steps, waits, ready, order = [], [], [0], []

        def send(r, x):
            for k in self.fwd[x].kids[r]:
                d = self.fwd[x].link[k]
                free[d] = max(free[d], now) + unit_us
                due[k, x] = free[d] + hop_us

        now = 0.0
        send(0, 0)
        send(0, 1)
        now = 1.0
        while True:
            for unit in sorted((u for u in due if u not in done and due[u] <= now), key=lambda u: (due[u], u)):
                done.add(unit)
                now += 0.02
                send(*unit)
                waits.append(unit)
                if unit[1] == 0 and (unit[0] ^ 1, 0) in done:
                    ready.append(unit[0] >> 1)
            turn = len(steps)
            late = order[max(turn - 2, 0):turn - 1] if turn < self.turns else order[turn - 2:]
            lacking = [r for pair in late for r in (2 * pair, 2 * pair + 1) if (r, 1) not in done]
            if turn == 2 < self.turns:
                lacking = []
            if lacking or not (ready or turn == self.turns):
                now = max(now, min(due[u] for u in due if u not in done))
                continue
            if turn == self.turns:
                break
            order.append(ready.pop(0))
            steps.append(waits)
            waits = []
            now += turn_us if turn else 0.0
        self.fwd_waits = steps + [waits]
        self.fwd_pairs = order
        self.fwd_mate = max(i for i, pair in enumerate(order) if pair == 0)

    def backward(self, unit_us=2.9, hop_us=2.1, turn_us=1.55, add_us=0.035):
        if self.dims == 6:
            order = [int(c, 32) for c in BWD_ORDER]
        else:
            order = sorted(range(1, self.blocks // 2), key=lambda pair: -popcount(pair))
        order += [0, 0]
        free = [0.0] * self.dims
        due = {}
        waiting, sends, steps = set(), [], []
        now = 1.57

        def kids(unit):
            return [(k, unit[1]) for k in self.bwd[unit[1]].kids[unit[0]]]

        def flush():
            nonlocal now
            able = True
            while able:
                able = [u for u in waiting if all(due.get(k, 1e9) <= now for k in kids(u))]
                for unit in sorted(able, key=lambda u: (-popcount(u[0]), u)):
                    waiting.discard(unit)
                    now += add_us * len(kids(unit)) + 0.01
                    d = self.bwd[unit[1]].link[unit[0]]
                    free[d] = max(free[d], now) + unit_us
                    due[unit] = free[d] + hop_us
                    sends.append(unit)

        for i, pair in enumerate(order):
            waiting |= {(r, x) for r in (2 * pair, 2 * pair + 1) for x in range(2) if r} if i < len(order) - 1 else set()
            flush()
            steps.append(sends)
            sends = []
            if i == 0:
                now += 0.85
                flush()
                steps.append(sends)
                sends = []
            now += turn_us if i < len(order) - 1 else 0.0
        while waiting:
            now = max(now, min(max(due.get(k, 1e9) for k in kids(u)) for u in waiting))
            flush()
        self.bwd_sends = steps[:-1] + [steps[-1] + sends]
        self.bwd_pairs = order
        self.bwd_last = sorted((u for x in range(2) for u in kids((0, x))), key=lambda u: due[u])


def div(a, b):
    return lax.div(a, jnp.int32(b))


def mod(a, b):
    return lax.rem(a, jnp.int32(b))


def xor(a, b):
    return a + b - 2 * a * b


def lookup(index, table):
    level = [jnp.int32(v) for v in table]
    bit = 1
    while len(level) > 1:
        odd = mod(div(index, bit), 2) == 1
        nxt = [jnp.where(odd, level[i + 1], level[i]) for i in range(0, len(level) - 1, 2)]
        level = nxt + level[2 * len(nxt):]
        bit *= 2
    return level[0]


def branch(index, count, leaf):
    once = div(index, count) + 1

    def pick(low, high):
        if high - low == 1:
            acts = leaf(low)
            if acts:
                pl.loop(0, once)(lambda _: [act() for act in acts] and None)
            return
        mid = (low + high) // 2
        lax.cond(index < mid, lambda: pick(low, mid), lambda: pick(mid, high))

    pick(0, count)


def kernel(plan, q_ref, k_ref, v_ref, g_ref, o_ref, dq_ref, dk_ref, dv_ref,
           kv, stg, land, s_buf, t_buf, p_buf, d_buf, top, q_s, g_s, v_s, q_t, g_t, c_t, acc, mst, lst, dec,
           xacc, xm, xl, lrow, drow, lcol, dcol, dq_s, xdq, o_s, dq_o, dk_o, dv_o,
           ag_send, ag_recv, rs_send, rs_recv, x_send, x_recv, io):
    dims, turns = plan.dims, plan.turns
    pieces = 4 * plan.blocks
    f32, bf16 = jnp.float32, jnp.bfloat16
    me = lax.axis_index("ctx")
    core = mod(me, 2)
    chip = div(me, 2)
    bits = [mod(div(chip, 1 << d), 2) for d in range(dims)]
    gray = [xor(bits[d], bits[d + 1]) if d % 2 == 0 and d + 1 < dims else bits[d] for d in range(dims)]
    nbr = []
    for d in range(dims):
        other = chip + (1 - 2 * bits[d]) * (1 << d)
        if d % 2:
            other = other + (1 - 2 * bits[d - 1]) * (1 << (d - 1))
        nbr.append(2 * other + core)
    mate = me + 1 - 2 * core
    my_pair = div(chip, 2)

    barrier = pltpu.get_barrier_semaphore()
    for dev in nbr + [mate]:
        pl.semaphore_signal(barrier, inc=1, device_id={"ctx": dev}, device_id_type=MESH)

    def half(h):
        return pl.ds(h * PIECE, PIECE)

    loads = []
    for h in range(2):
        loads += [pltpu.make_async_copy(k_ref.at[half(h)], kv.at[0, 0, 0, h], io.at[h]),
                  pltpu.make_async_copy(v_ref.at[half(h)], v_s.at[h], io.at[2 + h])]
    for h in range(2):
        for j, (src, dst) in enumerate(((q_ref, q_s), (g_ref, g_s))):
            loads.append(pltpu.make_async_copy(src.at[:, half(h)], dst.at[h, pl.ds(0, HEADS)], io.at[4 + 2 * j + h]))
    for copy in loads:
        copy.start()
    mst[...] = jnp.full(mst.shape, NEG, f32)
    lst[...] = jnp.zeros(lst.shape, f32)
    acc[...] = jnp.zeros(acc.shape, f32)
    dec[...] = jnp.ones(dec.shape, f32)
    p_buf[...] = jnp.zeros(p_buf.shape, bf16)
    for copy in loads[:4]:
        copy.wait()
    for h in range(2):
        kv[0, 0, 1, h] = v_s[h].T

    pl.semaphore_wait(barrier, dims + 1)

    def ag_copy(k, x):
        d = plan.fwd[x].link[k]
        r = k ^ (1 << d)
        return pltpu.make_async_remote_copy(
            src_ref=kv.at[r >> 1, r & 1, x], dst_ref=kv.at[k >> 1, k & 1, x], send_sem=ag_send.at[k, x],
            recv_sem=ag_recv.at[k, x], device_id={"ctx": nbr[d]}, device_id_type=MESH)

    def rs_copy(r, x):
        return pltpu.make_async_remote_copy(
            src_ref=stg.at[r >> 1, r & 1, x], dst_ref=land.at[r, x], send_sem=rs_send.at[r, x], recv_sem=rs_recv.at[r, x],
            device_id={"ctx": nbr[plan.bwd[x].link[r]]}, device_id_type=MESH)

    def mate_copy(src, dst, sem):
        return pltpu.make_async_remote_copy(src_ref=src, dst_ref=dst, send_sem=x_send.at[sem], recv_sem=x_recv.at[sem],
                                            device_id={"ctx": mate}, device_id_type=MESH)

    ours, theirs = pl.ds(0, SPAN), pl.ds(SPAN, SPAN)

    for x in range(2):
        for k in plan.fwd[x].kids[0]:
            ag_copy(k, x).start()
    for copy in loads[4:]:
        copy.wait()
    x_q = [mate_copy(ref.at[h, pl.ds(0, HEADS)], ref.at[h, pl.ds(HEADS, HEADS)], 2 * j + h)
           for j, ref in enumerate((q_s, g_s)) for h in range(2)]
    for copy in x_q:
        copy.start()

    def ag_events(waits):
        return [act for r, x in waits for act in [ag_copy(r, x).wait_recv] + [ag_copy(k, x).start for k in plan.fwd[x].kids[r]]]

    coef = SCALE * LOG2E

    def transposes(h):
        def turn(i):
            cols = pl.ds(pl.multiple_of(i * 128, 128), 128)
            turned = q_s[h, i].T
            q_t[h, :, cols] = turned
            g_t[h, :, cols] = g_s[h, i].T
            scaled = turned.astype(f32) * coef
            high = scaled.astype(bf16)
            c_t[h, pl.ds(0, HD), cols] = high
            c_t[h, pl.ds(HD, HD), cols] = (scaled - high.astype(f32)).astype(bf16)

        return turn

    for h in range(2):
        pl.loop(0, HEADS)(transposes(h))
    for copy in x_q:
        copy.wait_recv()
    for h in range(2):
        pl.loop(HEADS, TILES)(transposes(h))

    def is_future(pair):
        rel = [mod(div(pair, 1 << (d - 1)), 2) for d in range(1, dims)]
        gp = [None] + [xor(gray[d], rel[d - 1]) for d in range(1, dims)]
        other = gp[1] if dims > 1 else 0
        for d in range(2, dims):
            bit = xor(gp[d], gp[d + 1]) if d % 2 == 0 and d + 1 < dims else gp[d]
            other = other + bit * (1 << (d - 1))
        return div(other - my_pair + plan.blocks, plan.blocks)

    def place(pair, a):
        mine = div(plan.blocks // 2 - pair, plan.blocks // 2)
        fut = is_future(pair)
        turn = (pair,)
        for slot in range(2):
            h = (1 - mine) * fut * slot
            turn += (mine * a, h, mine * a + 1 - mine, mine + h, mine * slot + (1 - mine) * (fut + (1 - fut) * slot))
        return turn

    def groups(turn, some):
        for slot in range(2):
            if not any(slot * HEADS <= b < slot * HEADS + HEADS for b in some):
                continue
            p0, h0, p1, h1, qg = turn[1 + 5 * slot:6 + 5 * slot]
            yield slot, ((turn[0], p0, h0), (turn[0], p1, h1)), qg

    def key_tile(where):
        return jnp.concatenate([kv[pair, par, 0, h] for pair, par, h in where], axis=0)

    def value_tile_t(where):
        return jnp.concatenate([kv[pair, par, 1, h] for pair, par, h in where], axis=1)

    def tile_of(memo, slot, kind, where):
        key = (kind, slot)
        if key not in memo:
            memo[key] = value_tile_t(where) if kind == "v" else key_tile(where) if kind == "k" else key_tile(where).T
        return memo[key]

    def tall(ref, qg, t):
        return ref[qg, pl.ds(2 * t, 2)].reshape(256, 128)

    def cols_of(t):
        return pl.ds(t * 256, 256)

    def rows(b):
        return pl.ds(b * 256, 256)

    def mask_scores(a, keys_axis):
        key_low = me + a * (2 * (1 - 2 * mod(chip, 2)))

        def two(base0, base1, axis):
            i = lax.broadcasted_iota(jnp.int32, (256, 256), axis)
            return i + jnp.where(i < PIECE, base0, base1 - PIECE)

        def query_base(c):
            h, par = div(c, TILES), mod(div(c, HEADS), 2)
            low = me + par * (mate - me)
            return (low + h * (pieces - 1 - 2 * low)) * PIECE

        @pl.loop(0, TILES)
        def _(b):
            kpos = two(key_low * PIECE, (pieces - 1 - key_low) * PIECE, keys_axis)
            qpos = two(query_base(2 * b), query_base(2 * b + 1), 1 - keys_axis)
            s = jnp.where(qpos >= kpos, s_buf[b], NEG)
            s_buf[b] = s
            if keys_axis == 0:
                top[b] = jnp.max(s.reshape(32, 8, 256), axis=0)

    def fwd_scores(turn, some, memo):
        for slot, where, qg in groups(turn, some):
            kt = tile_of(memo, slot, "k", where)
            twice = jnp.concatenate([kt, kt], axis=1)
            for t in range(HEADS):
                b, cols = slot * HEADS + t, cols_of(t)
                if b in some:
                    s = jnp.dot(twice, c_t[qg, :, cols], preferred_element_type=f32)
                    s_buf[b] = s
                    top[b] = jnp.max(s.reshape(32, 8, 256), axis=0)

    def fwd_softmax(turn, some):
        for slot, _, qg in groups(turn, some):
            for t in range(HEADS):
                b, cols = slot * HEADS + t, cols_of(t)
                if b not in some:
                    continue
                m_old = mst[qg, :, cols]
                m_new = jnp.maximum(m_old, jnp.max(top[b], axis=0, keepdims=True))
                p = jnp.exp2(s_buf[b] - m_new[0:1])
                decay = jnp.exp2(m_old - m_new)
                lst[qg, :, cols] = lst[qg, :, cols] * decay + jnp.sum(p.reshape(32, 8, 256), axis=0)
                p_buf[rows(b), :] = p.astype(bf16)
                dec[b] = decay
                mst[qg, :, cols] = m_new

    def fwd_out(turn, some, memo):
        for slot, where, qg in groups(turn, some):
            vt = tile_of(memo, slot, "v", where)
            for t in range(HEADS):
                b, cols = slot * HEADS + t, cols_of(t)
                if b in some:
                    pv = jnp.dot(vt, p_buf[rows(b), :], preferred_element_type=f32)
                    acc[qg, :, cols] = acc[qg, :, cols] * dec[b, 0:1] + pv

    def fwd_place(j):
        return place(lookup(jnp.minimum(j, turns - 1), plan.fwd_pairs), jnp.minimum(j, 1))

    every = range(TILES)
    for act in ag_events(plan.fwd_waits[0]):
        act()
    first = fwd_place(me * 0)
    fwd_scores(first, every, {})

    def fwd_turn(j, carry):
        old, cur, new = carry
        branch(j, turns, lambda i: ag_events(plan.fwd_waits[i + 1]))

        @pl.when((j == 0) | (j == plan.fwd_mate))
        def _():
            mask_scores(jnp.minimum(j, 1), 0)

        after = fwd_place(j + 2)
        memo, memo_old = {}, {}
        for b in range(TILES + 2):
            fwd_scores(new, (b - 2,), memo)
            fwd_softmax(cur, (b - 1,))
            fwd_out(old, (b,), memo_old)
        return cur, new, after

    old, cur, _ = lax.fori_loop(0, turns - 1, fwd_turn, (first, first, fwd_place(me * 0 + 1)))
    for act in ag_events(plan.fwd_waits[turns]):
        act()
    if plan.fwd_mate == turns - 1:
        mask_scores(1, 0)
    memo = {}
    for b in range(TILES + 1):
        fwd_softmax(cur, (b - 1,))
        fwd_out(old, (b,), memo)
    late = [b for b in every if b % HEADS < HEADS // 2]
    fwd_out(cur, [b for b in every if b not in late], {})

    def bwd_scores(turn, some, memo):
        for slot, where, qg in groups(turn, some):
            for t in range(HEADS):
                b, cols = slot * HEADS + t, cols_of(t)
                if b in some:
                    for buf, lhs, kind in ((s_buf, q_s, "t"), (t_buf, g_s, "v")):
                        buf[b] = jnp.dot(tall(lhs, qg, t), tile_of(memo, slot, kind, where), preferred_element_type=f32)

    def bwd_softmax(turn, some):
        for slot, _, qg in groups(turn, some):
            for t in range(HEADS):
                b, cols = slot * HEADS + t, cols_of(t)
                if b in some:
                    lse, dr = tall(lcol, qg, t), tall(dcol, qg, t)
                    p = jnp.exp2(s_buf[b] * coef - jnp.concatenate([lse, lse], axis=1))
                    p_buf[rows(b), :] = p.astype(bf16)
                    d_buf[rows(b), :] = (p * (t_buf[b] - jnp.concatenate([dr, dr], axis=1))).astype(bf16)

    def bwd_out(turn, some, memo, parts=(True, True)):
        for slot, where, qg in groups(turn, some):
            for t in range(HEADS):
                b, cols = slot * HEADS + t, cols_of(t)
                if b not in some:
                    continue
                ds = d_buf[rows(b), :]
                if parts[1]:
                    dq_s[qg, :, cols] += lax.dot_general(tile_of(memo, slot, "t", where), ds, (((1,), (1,)), ((), ())),
                                                         preferred_element_type=f32)
                for x, (ref, buf) in enumerate(((q_t, ds), (g_t, p_buf[rows(b), :])) if parts[0] else ()):
                    grad = jnp.dot(ref[qg, :, cols], buf, preferred_element_type=f32)
                    memo[x] = memo[x] + grad if t else grad
                    for j, (pair, par, h) in enumerate(where if t == HEADS - 1 else ()):
                        value = memo[x][:, j * 128:j * 128 + 128]
                        stg[pair, par, x, h] = value + stg[pair, par, x, h] if slot else value

    def bwd_place(j):
        at = jnp.minimum(j, turns - 1)
        return place(lookup(at, plan.bwd_pairs), 1 - div(at + 1, turns))

    x_m = [mate_copy(ref.at[h, :, theirs], box.at[h], 4 + 3 * h + i)
           for h in range(2) for i, (ref, box) in enumerate(((acc, xacc), (mst, xm), (lst, xl)))]
    for copy in x_m:
        copy.start()
    fwd_out(cur, late, {})
    first = bwd_place(me * 0)
    bwd_scores(first, every, {})
    for k in range(1, plan.blocks):
        for x in range(2):
            ag_copy(k, x).wait_send()
    dq_s[...] = jnp.zeros(dq_s.shape, f32)
    x_r = [mate_copy(ref.at[h, :, ours], ref.at[h, :, theirs], 10 + 2 * j + h) for j, ref in enumerate((lrow, drow)) for h in range(2)]

    for h in range(2):
        for copy in x_m[3 * h:3 * h + 3]:
            copy.wait_recv()
        for head in range(HEADS):
            cols = pl.ds(head * PIECE, PIECE)
            m1, m2 = mst[h, :, cols], xm[h, :, cols]
            m = jnp.maximum(m1, m2)
            w1, w2 = jnp.exp2(m1 - m), jnp.exp2(m2 - m)
            total = jnp.sum(lst[h, :, cols] * w1 + xl[h, :, cols] * w2, axis=0, keepdims=True)
            out = (acc[h, :, cols] * w1[0:1] + xacc[h, :, cols] * w2[0:1]) / total
            o_s[head, half(h), :] = out.T.astype(bf16)
            lrow[h, :, cols] = m + jnp.log2(total)
            rounded = out.astype(bf16).astype(f32)
            d = jnp.sum(rounded * g_t[h, :, cols].astype(f32), axis=0, keepdims=True)
            drow[h, :, cols] = jnp.broadcast_to(d, (8, 128))
        for copy in x_r[h::2]:
            copy.start()
    stores = [pltpu.make_async_copy(o_s, o_ref, io.at[8])]
    stores[0].start()

    def columns(h, i):
        cols = pl.ds(i * 128, 128)
        for row, col in ((lrow, lcol), (drow, dcol)):
            col[h, i] = jnp.broadcast_to(row[h, 0:1, cols], (128, 128)).T

    def rs_add(r, k, x):
        rs_copy(k, x).wait_recv()
        for h in range(2):
            stg[r >> 1, r & 1, x, h] += land[k, x, h]

    def rs_events(sends):
        return ([functools.partial(rs_add, r, k, x) for r, x in sends for k in plan.bwd[x].kids[r]]
                + [rs_copy(r, x).start for r, x in sends])

    def clear(pair):
        for i in range(4):
            stg[pair, i // 2, i % 2, 1] = jnp.zeros((128, 128), f32)

    for i in range(TILES):
        columns(i // HEADS, i % HEADS)
    if turns < 4:
        mask_scores(turns - 1, 1)
    second, third = bwd_place(me * 0 + 1), bwd_place(me * 0 + 2)
    memo = {}
    for b in late:
        bwd_softmax(first, (b,))
        bwd_scores(second, (b,), memo)
    for copy in x_r:
        copy.wait_recv()
    for i in range(TILES):
        columns(i // HEADS, HEADS + i % HEADS)
    memo = {}
    for b in every:
        if b not in late:
            bwd_softmax(first, (b,))
            bwd_scores(second, (b,), memo)
    clear(first[0])
    bwd_out(first, every, {}, (True, False))
    for act in rs_events(plan.bwd_sends[0]):
        act()
    bwd_out(first, every, {}, (False, True))
    if turns < 4:
        mask_scores(turns - 2, 1)
    memo = {}
    for b in range(TILES + 1):
        bwd_softmax(second, (b,))
        bwd_scores(third, (b - 1,), memo)

    def bwd_turn(j, carry):
        old, cur, new = carry
        branch(j, turns, lambda i: rs_events(plan.bwd_sends[i - 1]) if i > 1 else [])

        @pl.when(j < turns - 1)
        def _():
            clear(old[0])

        @pl.when(j >= turns - 2)
        def _():
            mask_scores(turns - 1 - j, 1)

        after = bwd_place(j + 2)
        memo, memo_old = {}, {}
        for b in range(TILES + 2):
            bwd_out(old, (b,), memo_old)
            bwd_softmax(cur, (b - 1,))
            bwd_scores(new, (b - 2,), memo)
        return cur, new, after

    last = lax.fori_loop(2, turns, bwd_turn, (second, third, bwd_place(me * 0 + 3)))[0]
    for act in rs_events(plan.bwd_sends[turns - 1]):
        act()
    bwd_out(last, every, {})

    x_d = [mate_copy(dq_s.at[h, :, theirs], xdq.at[h], 14 + h) for h in range(2)]
    for copy in x_d:
        copy.start()
    for unit in plan.bwd_sends[turns]:
        for act in rs_events([unit]):
            act()
    for h in range(2):
        x_d[h].wait_recv()
        for head in range(HEADS):
            cols = pl.ds(head * PIECE, PIECE)
            total = (dq_s[h, :, cols] + xdq[h, :, cols]) * SCALE
            dq_o[head, half(h), :] = total.T.astype(bf16)
    stores.append(pltpu.make_async_copy(dq_o, dq_ref, io.at[9]))
    stores[1].start()
    for k in range(1, plan.blocks):
        for x in range(2):
            rs_copy(k, x).wait_send()
    for copy in x_q + x_m + x_r + x_d:
        copy.wait_send()
    left = [dims, dims]
    for k, x in plan.bwd_last:
        rs_add(0, k, x)
        left[x] -= 1
        if not left[x]:
            buf, ref, factor = ((dk_o, dk_ref, SCALE), (dv_o, dv_ref, 1.0))[x]
            for h in range(2):
                buf[half(h), :] = (stg[0, 0, x, h] * factor).T.astype(bf16)
            stores.append(pltpu.make_async_copy(buf, ref, io.at[10 + x]))
            stores[-1].start()

    for copy in stores:
        copy.wait()


def relay(*refs):
    count = (len(refs) - 1) // 3
    src, dst, buf, sem = refs[:count], refs[count:2 * count], refs[2 * count:3 * count], refs[3 * count]
    into = [pltpu.make_async_copy(a, b, sem.at[i]) for i, (a, b) in enumerate(zip(src, buf))]
    out = [pltpu.make_async_copy(b, c, sem.at[count + i]) for i, (b, c) in enumerate(zip(buf, dst))]
    for copy in into:
        copy.start()
    for i in range(count):
        into[i].wait()
        out[i].start()
    for copy in out:
        copy.wait()


def solution(mesh):
    size = mesh.shape["ctx"]
    plan = Plan(int(math.log2(size)) - 1)
    spec = P("data", "ctx", None, None)
    n = plan.blocks
    f32, bf16 = jnp.float32, jnp.bfloat16
    vm, sem = pltpu.VMEM, pltpu.SemaphoreType.DMA

    def local(queries, keys, values, grad_out):
        tokens = queries.shape[1]
        q = queries[0].transpose(1, 0, 2)
        g = grad_out[0].transpose(1, 0, 2)
        tile = (128, 128)
        big = jax.ShapeDtypeStruct((HEADS, tokens, HD), bf16)
        small = jax.ShapeDtypeStruct((tokens, HD), bf16)
        anywhere = pl.BlockSpec(memory_space=pl.ANY)
        rows, wide, half_wide = (2, TILES) + tile, (2, HD, 2 * SPAN), (2, HD, SPAN)
        stat, few = (2, 8, 2 * SPAN), (2, 8, SPAN)
        results = pl.pallas_call(
            functools.partial(kernel, plan),
            out_shape=(big, big, small, small),
            in_specs=[anywhere] * 4,
            out_specs=(anywhere,) * 4,
            scratch_shapes=[
                vm((n // 2, 2, 2, 2) + tile, bf16), vm((n // 2, 2, 2, 2) + tile, f32), vm((n, 2, 2) + tile, f32),
                vm((TILES, 256, 256), f32), vm((TILES, 256, 256), f32), vm((TILES * 256, 256), bf16), vm((TILES * 256, 256), bf16),
                vm((TILES, 8, 256), f32),
                vm(rows, bf16), vm(rows, bf16), vm((2,) + tile, bf16), vm(wide, bf16), vm(wide, bf16), vm((2, 2 * HD, 2 * SPAN), bf16),
                vm(wide, f32), vm(stat, f32), vm(stat, f32), vm((TILES, 8, 256), f32),
                vm(half_wide, f32), vm(few, f32), vm(few, f32), vm(stat, f32), vm(stat, f32), vm(rows, f32), vm(rows, f32),
                vm(wide, f32), vm(half_wide, f32),
                vm(big.shape, bf16), vm(big.shape, bf16), vm(small.shape, bf16), vm(small.shape, bf16),
                sem((n, 2)), sem((n, 2)), sem((n, 2)), sem((n, 2)), sem((16,)), sem((16,)), sem((12,)),
            ],
            compiler_params=pltpu.CompilerParams(collective_id=0, has_side_effects=True, vmem_limit_bytes=67043328),
            cost_estimate=pl.CostEstimate(flops=14 * 640 * PIECE * n * 2 * HD, bytes_accessed=4 << 20, transcendentals=0),
        )(q, keys[0, :, 0], values[0, :, 0], g)
        o, dq, dk, dv = pl.pallas_call(
            relay,
            out_shape=(big, big, small, small),
            in_specs=[anywhere] * 4,
            out_specs=(anywhere,) * 4,
            scratch_shapes=[vm(x.shape, bf16) for x in (big, big, small, small)] + [sem((8,))],
            cost_estimate=pl.CostEstimate(flops=1 << 20, bytes_accessed=2 << 20, transcendentals=0),
        )(*results)
        return (o.transpose(1, 0, 2)[None], dq.transpose(1, 0, 2)[None], dk[None, :, None], dv[None, :, None])

    return jax.shard_map(local, mesh=mesh, in_specs=(spec,) * 4, out_specs=(spec,) * 4, check_vma=False)
```

```python
import functools
import math

import jax
import jax.numpy as jnp
from jax import lax
from jax.experimental import pallas as pl
from jax.experimental.pallas import tpu as pltpu
from jax.sharding import PartitionSpec as P

MESH = pl.DeviceIdType.MESH
NEG = -1e30
HD = 128
HEADS = 5
PIECE = 128
SCALE = HD ** -0.5
LOG2E = 1.4426950408889634
TILES = 2 * HEADS
SPAN = HEADS * PIECE

KEY_TREE = "011222133332330444044204331303450512252553132154554251534405024"
VALUE_TREE = "011202133303032404124114441201150505210501022525540551434312353"
DK_TREE = "011202230302020401042203040443255115012501525315014524043545435"
DV_TREE = "011221233332313444144214343331155555212333535104510402554435224"
BWD_ORDER = "vtfrsnmud7qjklp3cobe9ai6h45g128"


def popcount(value):
    return bin(value).count("1")


class Tree:
    def __init__(self, dims, links):
        blocks = 1 << dims
        if dims == 6:
            self.link = [None] + [int(d) for d in links]
        else:
            self.link = [None] * blocks
            count = [0] * dims
            for r in sorted(range(1, blocks), key=popcount):
                self.link[r] = min((d for d in range(dims) if (r >> d) & 1), key=lambda d: count[d])
                count[self.link[r]] += 1
        self.kids = {r: [k for k in range(1, blocks) if k & ~(1 << self.link[k]) == r] for r in range(blocks)}
        height = {}
        for r in sorted(range(blocks), key=popcount, reverse=True):
            height[r] = max([1 + height[k] for k in self.kids[r]], default=0)
        for r in self.kids:
            self.kids[r].sort(key=lambda k: -height[k])


class Plan:
    def __init__(self, dims):
        self.dims = dims
        self.blocks = 1 << dims
        self.turns = self.blocks // 2 + 1
        self.fwd = [Tree(dims, KEY_TREE), Tree(dims, VALUE_TREE)]
        self.bwd = [Tree(dims, DK_TREE), Tree(dims, DV_TREE)]
        self.forward()
        self.backward()

    def forward(self, unit_us=1.41, hop_us=1.9, turn_us=0.78):
        free = [0.0] * self.dims
        due = {}
        done = {(0, 0), (0, 1)}
        now = 1.0
        steps, waits, ready, order = [], [], [0], []

        def send(r, x):
            for k in self.fwd[x].kids[r]:
                d = self.fwd[x].link[k]
                free[d] = max(free[d], now) + unit_us
                due[k, x] = free[d] + hop_us

        now = 0.0
        send(0, 0)
        send(0, 1)
        now = 1.0
        while True:
            for unit in sorted((u for u in due if u not in done and due[u] <= now), key=lambda u: (due[u], u)):
                done.add(unit)
                now += 0.02
                send(*unit)
                waits.append(unit)
                if unit[1] == 0 and (unit[0] ^ 1, 0) in done:
                    ready.append(unit[0] >> 1)
            turn = len(steps)
            late = order[max(turn - 2, 0):turn - 1] if turn < self.turns else order[turn - 2:]
            lacking = [r for pair in late for r in (2 * pair, 2 * pair + 1) if (r, 1) not in done]
            if turn == 2 < self.turns:
                lacking = []
            if lacking or not (ready or turn == self.turns):
                now = max(now, min(due[u] for u in due if u not in done))
                continue
            if turn == self.turns:
                break
            order.append(ready.pop(0))
            steps.append(waits)
            waits = []
            now += turn_us if turn else 0.0
        self.fwd_waits = steps + [waits]
        self.fwd_pairs = order
        self.fwd_mate = max(i for i, pair in enumerate(order) if pair == 0)

    def backward(self, unit_us=2.9, hop_us=2.1, turn_us=1.6, add_us=0.025):
        if self.dims == 6:
            order = [int(c, 32) for c in BWD_ORDER]
        else:
            order = sorted(range(1, self.blocks // 2), key=lambda pair: -popcount(pair))
        order += [0, 0]
        free = [0.0] * self.dims
        due = {}
        waiting, sends, steps = set(), [], []
        now = 1.65

        def kids(unit):
            return [(k, unit[1]) for k in self.bwd[unit[1]].kids[unit[0]]]

        def flush():
            nonlocal now
            able = True
            while able:
                able = [u for u in waiting if all(due.get(k, 1e9) <= now for k in kids(u))]
                for unit in sorted(able, key=lambda u: (-popcount(u[0]), u)):
                    waiting.discard(unit)
                    now += add_us * len(kids(unit)) + 0.01
                    d = self.bwd[unit[1]].link[unit[0]]
                    free[d] = max(free[d], now) + unit_us
                    due[unit] = free[d] + hop_us
                    sends.append(unit)

        for i, pair in enumerate(order):
            if i:
                now += 0.12
                flush()
                steps.append(sends)
                sends = []
                now += turn_us
            waiting |= {(r, x) for r in (2 * pair, 2 * pair + 1) for x in range(2) if r} if i < len(order) - 1 else set()
            if not i:
                flush()
                steps.append(sends)
                sends = []
                now += 0.9
        flush()
        while waiting:
            now = max(now, min(max(due.get(k, 1e9) for k in kids(u)) for u in waiting))
            flush()
        self.bwd_sends = steps + [sends]
        self.bwd_pairs = order
        self.bwd_last = sorted((u for x in range(2) for u in kids((0, x))), key=lambda u: due[u])


def div(a, b):
    return lax.div(a, jnp.int32(b))


def mod(a, b):
    return lax.rem(a, jnp.int32(b))


def xor(a, b):
    return a + b - 2 * a * b


def lookup(index, table):
    level = [jnp.int32(v) for v in table]
    bit = 1
    while len(level) > 1:
        odd = mod(div(index, bit), 2) == 1
        nxt = [jnp.where(odd, level[i + 1], level[i]) for i in range(0, len(level) - 1, 2)]
        level = nxt + level[2 * len(nxt):]
        bit *= 2
    return level[0]


def branch(index, count, leaf):
    once = div(index, count) + 1

    def pick(low, high):
        if high - low == 1:
            acts = leaf(low)
            if acts:
                pl.loop(0, once)(lambda _: [act() for act in acts] and None)
            return
        mid = (low + high) // 2
        lax.cond(index < mid, lambda: pick(low, mid), lambda: pick(mid, high))

    pick(0, count)


def kernel(plan, q_ref, k_ref, v_ref, g_ref, o_ref, dq_ref, dk_ref, dv_ref,
           kv, kt_s, stg, land, s_buf, t_buf, p_buf, d_buf, top, q_s, g_s, v_s, q_t, g_t, c_t, acc, mst, lst, dec,
           xacc, xm, xl, lrow, drow, lcol, dcol, o_s, dq_o, dk_o, dv_o,
           ag_send, ag_recv, rs_send, rs_recv, x_send, x_recv, io):
    dims, turns = plan.dims, plan.turns
    pieces = 4 * plan.blocks
    f32, bf16 = jnp.float32, jnp.bfloat16
    me = lax.axis_index("ctx")
    core = mod(me, 2)
    chip = div(me, 2)
    bits = [mod(div(chip, 1 << d), 2) for d in range(dims)]
    gray = [xor(bits[d], bits[d + 1]) if d % 2 == 0 and d + 1 < dims else bits[d] for d in range(dims)]
    nbr = []
    for d in range(dims):
        other = chip + (1 - 2 * bits[d]) * (1 << d)
        if d % 2:
            other = other + (1 - 2 * bits[d - 1]) * (1 << (d - 1))
        nbr.append(2 * other + core)
    mate = me + 1 - 2 * core
    my_pair = div(chip, 2)

    barrier = pltpu.get_barrier_semaphore()
    for dev in nbr + [mate]:
        pl.semaphore_signal(barrier, inc=1, device_id={"ctx": dev}, device_id_type=MESH)

    def half(h):
        return pl.ds(h * PIECE, PIECE)

    loads = []
    for h in range(2):
        loads += [pltpu.make_async_copy(k_ref.at[half(h)], kv.at[0, 0, 0, h], io.at[h]),
                  pltpu.make_async_copy(v_ref.at[half(h)], v_s.at[h], io.at[2 + h])]
    for h in range(2):
        for j, (src, dst) in enumerate(((q_ref, q_s), (g_ref, g_s))):
            loads.append(pltpu.make_async_copy(src.at[:, half(h)], dst.at[h, pl.ds(0, HEADS)], io.at[4 + 2 * j + h]))
    for copy in loads:
        copy.start()
    mst[...] = jnp.full(mst.shape, NEG, f32)
    lst[...] = jnp.zeros(lst.shape, f32)
    acc[...] = jnp.zeros(acc.shape, f32)
    dec[...] = jnp.ones(dec.shape, f32)
    p_buf[...] = jnp.zeros(p_buf.shape, bf16)
    for copy in loads[:4]:
        copy.wait()
    for h in range(2):
        kv[0, 0, 1, h] = v_s[h].T

    pl.semaphore_wait(barrier, dims + 1)

    def ag_copy(k, x):
        d = plan.fwd[x].link[k]
        r = k ^ (1 << d)
        return pltpu.make_async_remote_copy(
            src_ref=kv.at[r >> 1, r & 1, x], dst_ref=kv.at[k >> 1, k & 1, x], send_sem=ag_send.at[k, x],
            recv_sem=ag_recv.at[k, x], device_id={"ctx": nbr[d]}, device_id_type=MESH)

    def rs_copy(r, x):
        return pltpu.make_async_remote_copy(
            src_ref=stg.at[r >> 1, r & 1, x], dst_ref=land.at[r - 1, x], send_sem=rs_send.at[r, x], recv_sem=rs_recv.at[r, x],
            device_id={"ctx": nbr[plan.bwd[x].link[r]]}, device_id_type=MESH)

    def mate_copy(src, dst, sem):
        return pltpu.make_async_remote_copy(src_ref=src, dst_ref=dst, send_sem=x_send.at[sem], recv_sem=x_recv.at[sem],
                                            device_id={"ctx": mate}, device_id_type=MESH)

    ours, theirs = pl.ds(0, SPAN), pl.ds(SPAN, SPAN)

    for x in range(2):
        for k in plan.fwd[x].kids[0]:
            ag_copy(k, x).start()
    for copy in loads[4:]:
        copy.wait()
    x_q = [mate_copy(ref.at[h, pl.ds(0, HEADS)], ref.at[h, pl.ds(HEADS, HEADS)], 2 * j + h)
           for j, ref in enumerate((q_s, g_s)) for h in range(2)]
    for copy in x_q:
        copy.start()

    def ag_events(waits):
        return [act for r, x in waits for act in [ag_copy(r, x).wait_recv] + [ag_copy(k, x).start for k in plan.fwd[x].kids[r]]]

    coef = SCALE * LOG2E

    def transposes(h):
        def turn(i):
            cols = pl.ds(pl.multiple_of(i * 128, 128), 128)
            turned = q_s[h, i].T
            q_t[h, :, cols] = turned
            g_t[h, :, cols] = g_s[h, i].T
            scaled = turned.astype(f32) * coef
            high = scaled.astype(bf16)
            c_t[h, pl.ds(0, HD), cols] = high
            c_t[h, pl.ds(HD, HD), cols] = (scaled - high.astype(f32)).astype(bf16)

        return turn

    for h in range(2):
        pl.loop(0, HEADS)(transposes(h))
    for copy in x_q:
        copy.wait_recv()
    for h in range(2):
        pl.loop(HEADS, TILES)(transposes(h))

    def is_future(pair):
        rel = [mod(div(pair, 1 << (d - 1)), 2) for d in range(1, dims)]
        gp = [None] + [xor(gray[d], rel[d - 1]) for d in range(1, dims)]
        other = gp[1] if dims > 1 else 0
        for d in range(2, dims):
            bit = xor(gp[d], gp[d + 1]) if d % 2 == 0 and d + 1 < dims else gp[d]
            other = other + bit * (1 << (d - 1))
        return div(other - my_pair + plan.blocks, plan.blocks)

    def place(pair, a):
        mine = div(plan.blocks // 2 - pair, plan.blocks // 2)
        fut = is_future(pair)
        turn = (pair,)
        for slot in range(2):
            h = (1 - mine) * fut * slot
            turn += (mine * a, h, mine * a + 1 - mine, mine + h, mine * slot + (1 - mine) * (fut + (1 - fut) * slot))
        return turn

    def groups(turn, some):
        for slot in range(2):
            if not any(slot * HEADS <= b < slot * HEADS + HEADS for b in some):
                continue
            p0, h0, p1, h1, qg = turn[1 + 5 * slot:6 + 5 * slot]
            yield slot, ((turn[0], p0, h0), (turn[0], p1, h1)), qg

    def key_tile(where):
        return jnp.concatenate([kv[pair, par, 0, h] for pair, par, h in where], axis=0)

    def value_tile_t(where):
        return jnp.concatenate([kv[pair, par, 1, h] for pair, par, h in where], axis=1)

    def key_tile_t(where):
        return jnp.concatenate([kt_s[pair, par, h] for pair, par, h in where], axis=1)

    def tile_of(memo, slot, kind, where):
        key = (kind, slot)
        if key not in memo:
            memo[key] = value_tile_t(where) if kind == "v" else key_tile(where) if kind == "k" else key_tile_t(where)
        return memo[key]

    def tall(ref, qg, t):
        return ref[qg, pl.ds(2 * t, 2)].reshape(256, 128)

    def cols_of(t):
        return pl.ds(t * 256, 256)

    def rows(b):
        return pl.ds(b * 256, 256)

    def mask_scores(a, keys_axis):
        key_low = me + a * (2 * (1 - 2 * mod(chip, 2)))

        def two(base0, base1, axis):
            i = lax.broadcasted_iota(jnp.int32, (256, 256), axis)
            return i + jnp.where(i < PIECE, base0, base1 - PIECE)

        def query_base(c):
            h, par = div(c, TILES), mod(div(c, HEADS), 2)
            low = me + par * (mate - me)
            return (low + h * (pieces - 1 - 2 * low)) * PIECE

        @pl.loop(0, TILES)
        def _(b):
            kpos = two(key_low * PIECE, (pieces - 1 - key_low) * PIECE, keys_axis)
            qpos = two(query_base(2 * b), query_base(2 * b + 1), 1 - keys_axis)
            s = jnp.where(qpos >= kpos, s_buf[b], NEG)
            s_buf[b] = s
            if keys_axis == 0:
                top[b] = jnp.max(s.reshape(32, 8, 256), axis=0)

    def fwd_scores(turn, some, memo):
        for slot, where, qg in groups(turn, some):
            kt = tile_of(memo, slot, "k", where)
            twice = jnp.concatenate([kt, kt], axis=1)
            for t in range(HEADS):
                b, cols = slot * HEADS + t, cols_of(t)
                if b in some:
                    if t == 0:
                        for pair, par, h in where:
                            kt_s[pair, par, h] = kv[pair, par, 0, h].T
                    s = jnp.dot(twice, c_t[qg, :, cols], preferred_element_type=f32)
                    s_buf[b] = s
                    top[b] = jnp.max(s.reshape(32, 8, 256), axis=0)

    def fwd_softmax(turn, some):
        for slot, _, qg in groups(turn, some):
            for t in range(HEADS):
                b, cols = slot * HEADS + t, cols_of(t)
                if b not in some:
                    continue
                m_old = mst[qg, :, cols]
                m_new = jnp.maximum(m_old, jnp.max(top[b], axis=0, keepdims=True))
                p = jnp.exp2(s_buf[b] - m_new[0:1])
                decay = jnp.exp2(m_old - m_new)
                lst[qg, :, cols] = lst[qg, :, cols] * decay + jnp.sum(p.reshape(32, 8, 256), axis=0)
                p_buf[rows(b), :] = p.astype(bf16)
                dec[b] = decay
                mst[qg, :, cols] = m_new

    def fwd_out(turn, some, memo):
        for slot, where, qg in groups(turn, some):
            vt = tile_of(memo, slot, "v", where)
            for t in range(HEADS):
                b, cols = slot * HEADS + t, cols_of(t)
                if b in some:
                    pv = jnp.dot(vt, p_buf[rows(b), :], preferred_element_type=f32)
                    acc[qg, :, cols] = acc[qg, :, cols] * dec[b, 0:1] + pv

    def fwd_place(j):
        return place(lookup(jnp.minimum(j, turns - 1), plan.fwd_pairs), jnp.minimum(j, 1))

    every = range(TILES)
    for act in ag_events(plan.fwd_waits[0]):
        act()
    first = fwd_place(me * 0)
    fwd_scores(first, every, {})

    def fwd_turn(j, carry):
        old, cur, new = carry
        branch(j, turns, lambda i: ag_events(plan.fwd_waits[i + 1]))

        @pl.when((j == 0) | (j == plan.fwd_mate))
        def _():
            mask_scores(jnp.minimum(j, 1), 0)

        after = fwd_place(j + 2)
        memo, memo_old = {}, {}
        for b in range(TILES + 2):
            fwd_scores(new, (b - 2,), memo)
            fwd_softmax(cur, (b - 1,))
            fwd_out(old, (b,), memo_old)
        return cur, new, after

    old, cur, _ = lax.fori_loop(0, turns - 1, fwd_turn, (first, first, fwd_place(me * 0 + 1)))
    for act in ag_events(plan.fwd_waits[turns]):
        act()
    if plan.fwd_mate == turns - 1:
        mask_scores(1, 0)
    memo = {}
    for b in range(TILES + 1):
        fwd_softmax(cur, (b - 1,))
        fwd_out(old, (b,), memo)
    late = [b for b in every if b % HEADS < HEADS // 2]
    fwd_out(cur, [b for b in every if b not in late], {})

    def bwd_scores(turn, some, memo):
        for slot, where, qg in groups(turn, some):
            for t in range(HEADS):
                b, cols = slot * HEADS + t, cols_of(t)
                if b in some:
                    for buf, lhs, kind in ((s_buf, q_s, "t"), (t_buf, g_s, "v")):
                        buf[b] = jnp.dot(tall(lhs, qg, t), tile_of(memo, slot, kind, where), preferred_element_type=f32)

    def bwd_softmax(turn, some):
        for slot, _, qg in groups(turn, some):
            for t in range(HEADS):
                b, cols = slot * HEADS + t, cols_of(t)
                if b in some:
                    lse, dr = tall(lcol, qg, t), tall(dcol, qg, t)
                    p = jnp.exp2(s_buf[b] * coef - jnp.concatenate([lse, lse], axis=1))
                    p_buf[rows(b), :] = p.astype(bf16)
                    d_buf[rows(b), :] = (p * (t_buf[b] - jnp.concatenate([dr, dr], axis=1))).astype(bf16)

    def bwd_out(turn, some, memo, parts=(True, True)):
        for slot, where, qg in groups(turn, some):
            for t in range(HEADS):
                b, cols = slot * HEADS + t, cols_of(t)
                if b not in some:
                    continue
                ds = d_buf[rows(b), :]
                if parts[1]:
                    acc[qg, :, cols] += lax.dot_general(tile_of(memo, slot, "t", where), ds, (((1,), (1,)), ((), ())),
                                                         preferred_element_type=f32)
                for x, (ref, buf) in enumerate(((q_t, ds), (g_t, p_buf[rows(b), :])) if parts[0] else ()):
                    grad = jnp.dot(ref[qg, :, cols], buf, preferred_element_type=f32)
                    memo[x] = memo[x] + grad if t else grad
                    if t < HEADS - 1:
                        continue
                    for pair, par, _ in () if slot else where:
                        stg[pair, par, x, 1] = jnp.zeros((128, 128), f32)
                    for j, (pair, par, h) in enumerate(where):
                        value = memo[x][:, j * 128:j * 128 + 128]
                        stg[pair, par, x, h] = value + stg[pair, par, x, h] if slot else value

    def bwd_place(j):
        at = jnp.minimum(j, turns - 1)
        return place(lookup(at, plan.bwd_pairs), 1 - div(at + 1, turns))

    x_m = [mate_copy(ref.at[h, :, theirs], box.at[h], 4 + 3 * h + i)
           for h in range(2) for i, (ref, box) in enumerate(((acc, xacc), (mst, xm), (lst, xl)))]
    for copy in x_m:
        copy.start()
    fwd_out(cur, late, {})
    first = bwd_place(me * 0)
    bwd_scores(first, every, {})
    for k in range(1, plan.blocks):
        for x in range(2):
            ag_copy(k, x).wait_send()
    x_r = [mate_copy(ref.at[h, :, ours], ref.at[h, :, theirs], 10 + 2 * j + h) for j, ref in enumerate((lrow, drow)) for h in range(2)]

    for h in range(2):
        for copy in x_m[3 * h:3 * h + 3]:
            copy.wait_recv()
        for head in range(HEADS):
            cols = pl.ds(head * PIECE, PIECE)
            m1, m2 = mst[h, :, cols], xm[h, :, cols]
            m = jnp.maximum(m1, m2)
            w1, w2 = jnp.exp2(m1 - m), jnp.exp2(m2 - m)
            total = jnp.sum(lst[h, :, cols] * w1 + xl[h, :, cols] * w2, axis=0, keepdims=True)
            out = (acc[h, :, cols] * w1[0:1] + xacc[h, :, cols] * w2[0:1]) / total
            o_s[head, half(h), :] = out.T.astype(bf16)
            lrow[h, :, cols] = m + jnp.log2(total)
            rounded = out.astype(bf16).astype(f32)
            d = jnp.sum(rounded * g_t[h, :, cols].astype(f32), axis=0, keepdims=True)
            drow[h, :, cols] = jnp.broadcast_to(d, (8, 128))
        for copy in x_r[h::2]:
            copy.start()
    for copy in x_m:
        copy.wait_send()
    acc[...] = jnp.zeros(acc.shape, f32)
    stores = [pltpu.make_async_copy(o_s, o_ref, io.at[8])]
    stores[0].start()

    def columns(h, i):
        cols = pl.ds(i * 128, 128)
        for row, col in ((lrow, lcol), (drow, dcol)):
            col[h, i] = jnp.broadcast_to(row[h, 0:1, cols], (128, 128)).T

    def rs_sum(r, x, kids):
        for k in kids:
            rs_copy(k, x).wait_recv()
        for h in range(2):
            total = stg[r >> 1, r & 1, x, h]
            for k in kids:
                total = total + land[k - 1, x, h]
            stg[r >> 1, r & 1, x, h] = total

    def rs_events(sends):
        return ([functools.partial(rs_sum, r, x, plan.bwd[x].kids[r]) for r, x in sends if plan.bwd[x].kids[r]]
                + [rs_copy(r, x).start for r, x in sends])

    for i in range(TILES):
        columns(i // HEADS, i % HEADS)
    if turns < 4:
        mask_scores(turns - 1, 1)
    second, third = bwd_place(me * 0 + 1), bwd_place(me * 0 + 2)
    memo = {}
    for b in late:
        bwd_softmax(first, (b,))
        bwd_scores(second, (b,), memo)
    for copy in x_r:
        copy.wait_recv()
    for i in range(TILES):
        columns(i // HEADS, HEADS + i % HEADS)
    memo = {}
    for b in every:
        if b not in late:
            bwd_softmax(first, (b,))
            bwd_scores(second, (b,), memo)
    bwd_out(first, every, {}, (True, False))
    for act in rs_events(plan.bwd_sends[0]):
        act()
    bwd_out(first, every, {}, (False, True))
    if turns < 4:
        mask_scores(turns - 2, 1)
    memo = {}
    for b in range(TILES + 1):
        bwd_softmax(second, (b,))
        bwd_scores(third, (b - 1,), memo)

    def bwd_turn(j, carry):
        old, cur, new = carry
        branch(j, turns, lambda i: rs_events(plan.bwd_sends[i - 1]) if i > 1 else [])

        @pl.when(j >= turns - 2)
        def _():
            mask_scores(turns - 1 - j, 1)

        after = bwd_place(j + 2)
        memo, memo_old = {}, {}
        for b in range(TILES + 2):
            bwd_scores(new, (b - 2,), memo)
            bwd_out(old, (b - 1,), memo_old, (False, True))
            bwd_out(old, (b,), memo_old, (True, False))
            bwd_softmax(cur, (b - 1,))
        return cur, new, after

    last = lax.fori_loop(2, turns, bwd_turn, (second, third, bwd_place(me * 0 + 3)))[0]
    for act in rs_events(plan.bwd_sends[turns - 1]):
        act()
    bwd_out(last, every, {})

    x_d = [mate_copy(acc.at[h, :, theirs], xacc.at[h], 14 + h) for h in range(2)]
    for copy in x_d:
        copy.start()
    for unit in plan.bwd_sends[turns]:
        for act in rs_events([unit]):
            act()
    for h in range(2):
        x_d[h].wait_recv()
        for head in range(HEADS):
            cols = pl.ds(head * PIECE, PIECE)
            total = (acc[h, :, cols] + xacc[h, :, cols]) * SCALE
            dq_o[head, half(h), :] = total.T.astype(bf16)
    stores.append(pltpu.make_async_copy(dq_o, dq_ref, io.at[9]))
    stores[1].start()
    for k in range(1, plan.blocks):
        for x in range(2):
            rs_copy(k, x).wait_send()
    for copy in x_q + x_r + x_d:
        copy.wait_send()
    left = [dims, dims]
    for k, x in plan.bwd_last:
        rs_sum(0, x, [k])
        left[x] -= 1
        if not left[x]:
            buf, ref, factor = ((dk_o, dk_ref, SCALE), (dv_o, dv_ref, 1.0))[x]
            for h in range(2):
                buf[half(h), :] = (stg[0, 0, x, h] * factor).T.astype(bf16)
            stores.append(pltpu.make_async_copy(buf, ref, io.at[10 + x]))
            stores[-1].start()

    for copy in stores:
        copy.wait()


def relay(*refs):
    count = (len(refs) - 1) // 3
    src, dst, buf, sem = refs[:count], refs[count:2 * count], refs[2 * count:3 * count], refs[3 * count]
    into = [pltpu.make_async_copy(a, b, sem.at[i]) for i, (a, b) in enumerate(zip(src, buf))]
    out = [pltpu.make_async_copy(b, c, sem.at[count + i]) for i, (b, c) in enumerate(zip(buf, dst))]
    for copy in into:
        copy.start()
    for i in range(count):
        into[i].wait()
        out[i].start()
    for copy in out:
        copy.wait()


def solution(mesh):
    size = mesh.shape["ctx"]
    plan = Plan(int(math.log2(size)) - 1)
    spec = P("data", "ctx", None, None)
    n = plan.blocks
    f32, bf16 = jnp.float32, jnp.bfloat16
    vm, sem = pltpu.VMEM, pltpu.SemaphoreType.DMA

    def local(queries, keys, values, grad_out):
        tokens = queries.shape[1]
        q = queries[0].transpose(1, 0, 2)
        g = grad_out[0].transpose(1, 0, 2)
        tile = (128, 128)
        big = jax.ShapeDtypeStruct((HEADS, tokens, HD), bf16)
        small = jax.ShapeDtypeStruct((tokens, HD), bf16)
        anywhere = pl.BlockSpec(memory_space=pl.ANY)
        rows, wide, half_wide = (2, TILES) + tile, (2, HD, 2 * SPAN), (2, HD, SPAN)
        stat, few = (2, 8, 2 * SPAN), (2, 8, SPAN)
        results = pl.pallas_call(
            functools.partial(kernel, plan),
            out_shape=(big, big, small, small),
            in_specs=[anywhere] * 4,
            out_specs=(anywhere,) * 4,
            scratch_shapes=[
                vm((n // 2, 2, 2, 2) + tile, bf16), vm((n // 2, 2, 2) + tile, bf16), vm((n // 2, 2, 2, 2) + tile, f32), vm((n - 1, 2, 2) + tile, f32),
                vm((TILES, 256, 256), f32), vm((TILES, 256, 256), f32), vm((TILES * 256, 256), bf16), vm((TILES * 256, 256), bf16),
                vm((TILES, 8, 256), f32),
                vm(rows, bf16), vm(rows, bf16), vm((2,) + tile, bf16), vm(wide, bf16), vm(wide, bf16), vm((2, 2 * HD, 2 * SPAN), bf16),
                vm(wide, f32), vm(stat, f32), vm(stat, f32), vm((TILES, 8, 256), f32),
                vm(half_wide, f32), vm(few, f32), vm(few, f32), vm(stat, f32), vm(stat, f32), vm(rows, f32), vm(rows, f32),
                vm(big.shape, bf16), vm(big.shape, bf16), vm(small.shape, bf16), vm(small.shape, bf16),
                sem((n, 2)), sem((n, 2)), sem((n, 2)), sem((n, 2)), sem((16,)), sem((16,)), sem((12,)),
            ],
            compiler_params=pltpu.CompilerParams(collective_id=0, has_side_effects=True, vmem_limit_bytes=67043328),
            cost_estimate=pl.CostEstimate(flops=14 * 640 * PIECE * n * 2 * HD, bytes_accessed=4 << 20, transcendentals=0),
        )(q, keys[0, :, 0], values[0, :, 0], g)
        o, dq, dk, dv = pl.pallas_call(
            relay,
            out_shape=(big, big, small, small),
            in_specs=[anywhere] * 4,
            out_specs=(anywhere,) * 4,
            scratch_shapes=[vm(x.shape, bf16) for x in (big, big, small, small)] + [sem((8,))],
            cost_estimate=pl.CostEstimate(flops=1 << 20, bytes_accessed=2 << 20, transcendentals=0),
        )(*results)
        return (o.transpose(1, 0, 2)[None], dq.transpose(1, 0, 2)[None], dk[None, :, None], dv[None, :, None])

    return jax.shard_map(local, mesh=mesh, in_specs=(spec,) * 4, out_specs=(spec,) * 4, check_vma=False)
```

```python
import functools
import math

import jax
import jax.numpy as jnp
from jax import lax
from jax.experimental import pallas as pl
from jax.experimental.pallas import tpu as pltpu
from jax.sharding import PartitionSpec as P

MESH = pl.DeviceIdType.MESH
NEG = -1e30
HD = 128
HEADS = 5
PIECE = 128
SCALE = HD ** -0.5
LOG2E = 1.4426950408889634
TILES = 2 * HEADS
SPAN = HEADS * PIECE

KEY_TREE = "011222133332330444044204331303450512252553132154554251534405024"
VALUE_TREE = "011202133303032404124114441201150505210501022525540551434312353"
DK_TREE = "011202230302020401042203040443255115012501525315014524043545435"
DV_TREE = "011221233332313444144214343331155555212333535104510402554435224"
BWD_ORDER = "vtfrsnmud7qjklp3cobe9ai6h45g128"


def popcount(value):
    return bin(value).count("1")


class Tree:
    def __init__(self, dims, links):
        blocks = 1 << dims
        if dims == 6:
            self.link = [None] + [int(d) for d in links]
        else:
            self.link = [None] * blocks
            count = [0] * dims
            for r in sorted(range(1, blocks), key=popcount):
                self.link[r] = min((d for d in range(dims) if (r >> d) & 1), key=lambda d: count[d])
                count[self.link[r]] += 1
        self.kids = {r: [k for k in range(1, blocks) if k & ~(1 << self.link[k]) == r] for r in range(blocks)}
        height = {}
        for r in sorted(range(blocks), key=popcount, reverse=True):
            height[r] = max([1 + height[k] for k in self.kids[r]], default=0)
        for r in self.kids:
            self.kids[r].sort(key=lambda k: -height[k])


class Plan:
    def __init__(self, dims):
        self.dims = dims
        self.blocks = 1 << dims
        self.turns = self.blocks // 2 + 1
        self.fwd = [Tree(dims, KEY_TREE), Tree(dims, VALUE_TREE)]
        self.bwd = [Tree(dims, DK_TREE), Tree(dims, DV_TREE)]
        self.forward()
        self.backward()

    def forward(self, unit_us=1.45, hop_us=2.0, single_us=0.92, double_us=0.83):
        bodies = self.turns - 1
        self.singles = bodies if bodies < 4 else 2 + bodies % 2
        self.doubles = (bodies - self.singles) // 2
        free = [0.0] * self.dims
        due = {}
        done = {(0, 0), (0, 1)}
        steps, waits, ready, order = [], [], [0], []
        now = 0.0

        def send(r, x):
            for k in self.fwd[x].kids[r]:
                d = self.fwd[x].link[k]
                free[d] = max(free[d], now) + unit_us
                due[k, x] = free[d] + hop_us

        send(0, 0)
        send(0, 1)
        now = 1.0
        for group in [1] * (1 + self.singles) + [2] * self.doubles + [0]:
            while True:
                for unit in sorted((u for u in due if u not in done and due[u] <= now), key=lambda u: (due[u], u)):
                    done.add(unit)
                    now += 0.02
                    send(*unit)
                    waits.append(unit)
                    if unit[1] == 0 and (unit[0] ^ 1, 0) in done:
                        ready.append(unit[0] >> 1)
                i = len(order)
                outs = order[max(i - 2, 0):i - 2 + group] if group else order[i - 2:]
                skip = i == 2 < self.turns
                lacking = [r for pair in (() if skip else outs) for r in (2 * pair, 2 * pair + 1) if (r, 1) not in done]
                if not lacking and len(ready) >= group:
                    break
                now = max(now, min(due[u] for u in due if u not in done))
            steps.append(waits)
            waits = []
            for _ in range(group):
                order.append(ready.pop(0))
                now += 0.0 if len(order) == 1 else double_us if group > 1 else single_us
        self.fwd_waits = steps
        self.fwd_pairs = order
        self.fwd_mate = max(i for i, pair in enumerate(order) if pair == 0)

    def backward(self, unit_us=2.9, hop_us=2.1, turn_us=1.6, add_us=0.025):
        if self.dims == 6:
            order = [int(c, 32) for c in BWD_ORDER]
        else:
            order = sorted(range(1, self.blocks // 2), key=lambda pair: -popcount(pair))
        order += [0, 0]
        free = [0.0] * self.dims
        due = {}
        waiting, sends, steps = set(), [], []
        now = 1.65

        def kids(unit):
            return [(k, unit[1]) for k in self.bwd[unit[1]].kids[unit[0]]]

        def flush():
            nonlocal now
            able = True
            while able:
                able = [u for u in waiting if all(due.get(k, 1e9) <= now for k in kids(u))]
                for unit in sorted(able, key=lambda u: (-popcount(u[0]), u)):
                    waiting.discard(unit)
                    now += add_us * len(kids(unit)) + 0.01
                    d = self.bwd[unit[1]].link[unit[0]]
                    free[d] = max(free[d], now) + unit_us
                    due[unit] = free[d] + hop_us
                    sends.append(unit)

        for i, pair in enumerate(order):
            if i:
                now += 0.12
                flush()
                steps.append(sends)
                sends = []
                now += turn_us
            waiting |= {(r, x) for r in (2 * pair, 2 * pair + 1) for x in range(2) if r} if i < len(order) - 1 else set()
            if not i:
                flush()
                steps.append(sends)
                sends = []
                now += 0.9
        flush()
        while waiting:
            now = max(now, min(max(due.get(k, 1e9) for k in kids(u)) for u in waiting))
            flush()
        self.bwd_sends = steps + [sends]
        self.bwd_pairs = order
        self.bwd_last = sorted((u for x in range(2) for u in kids((0, x))), key=lambda u: due[u])


def div(a, b):
    return lax.div(a, jnp.int32(b))


def mod(a, b):
    return lax.rem(a, jnp.int32(b))


def xor(a, b):
    return a + b - 2 * a * b


def lookup(index, table):
    level = [jnp.int32(v) for v in table]
    bit = 1
    while len(level) > 1:
        odd = mod(div(index, bit), 2) == 1
        nxt = [jnp.where(odd, level[i + 1], level[i]) for i in range(0, len(level) - 1, 2)]
        level = nxt + level[2 * len(nxt):]
        bit *= 2
    return level[0]


def branch(index, count, leaf):
    once = div(index, count) + 1

    def pick(low, high):
        if high - low == 1:
            acts = leaf(low)
            if acts:
                pl.loop(0, once)(lambda _: [act() for act in acts] and None)
            return
        mid = (low + high) // 2
        lax.cond(index < mid, lambda: pick(low, mid), lambda: pick(mid, high))

    pick(0, count)


def kernel(plan, q_ref, k_ref, v_ref, g_ref, o_ref, dq_ref, dk_ref, dv_ref,
           kv, kt_s, stg, land, s_buf, t_buf, p_buf, d_buf, top, q_s, g_s, v_s, q_t, g_t, c_t, acc, mst, lst, dec,
           xacc, xm, xl, lrow, drow, lcol, dcol, o_s, dq_o, dk_o, dv_o,
           ag_send, ag_recv, rs_send, rs_recv, x_send, x_recv, io):
    dims, turns = plan.dims, plan.turns
    pieces = 4 * plan.blocks
    f32, bf16 = jnp.float32, jnp.bfloat16
    me = lax.axis_index("ctx")
    core = mod(me, 2)
    chip = div(me, 2)
    bits = [mod(div(chip, 1 << d), 2) for d in range(dims)]
    gray = [xor(bits[d], bits[d + 1]) if d % 2 == 0 and d + 1 < dims else bits[d] for d in range(dims)]
    nbr = []
    for d in range(dims):
        other = chip + (1 - 2 * bits[d]) * (1 << d)
        if d % 2:
            other = other + (1 - 2 * bits[d - 1]) * (1 << (d - 1))
        nbr.append(2 * other + core)
    mate = me + 1 - 2 * core
    my_pair = div(chip, 2)

    barrier = pltpu.get_barrier_semaphore()
    for dev in nbr + [mate]:
        pl.semaphore_signal(barrier, inc=1, device_id={"ctx": dev}, device_id_type=MESH)

    def half(h):
        return pl.ds(h * PIECE, PIECE)

    loads = []
    for h in range(2):
        loads += [pltpu.make_async_copy(k_ref.at[half(h)], kv.at[0, 0, 0, h], io.at[h]),
                  pltpu.make_async_copy(v_ref.at[half(h)], v_s.at[h], io.at[2 + h])]
    for h in range(2):
        for j, (src, dst) in enumerate(((q_ref, q_s), (g_ref, g_s))):
            loads.append(pltpu.make_async_copy(src.at[:, half(h)], dst.at[h, pl.ds(0, HEADS)], io.at[4 + 2 * j + h]))
    for copy in loads:
        copy.start()
    mst[...] = jnp.full(mst.shape, NEG, f32)
    lst[...] = jnp.zeros(lst.shape, f32)
    acc[...] = jnp.zeros(acc.shape, f32)
    dec[...] = jnp.ones(dec.shape, f32)
    p_buf[...] = jnp.zeros(p_buf.shape, bf16)
    for copy in loads[:4]:
        copy.wait()
    for h in range(2):
        kv[0, 0, 1, h] = v_s[h].T

    pl.semaphore_wait(barrier, dims + 1)

    def ag_copy(k, x):
        d = plan.fwd[x].link[k]
        r = k ^ (1 << d)
        return pltpu.make_async_remote_copy(
            src_ref=kv.at[r >> 1, r & 1, x], dst_ref=kv.at[k >> 1, k & 1, x], send_sem=ag_send.at[k, x],
            recv_sem=ag_recv.at[k, x], device_id={"ctx": nbr[d]}, device_id_type=MESH)

    def rs_copy(r, x):
        return pltpu.make_async_remote_copy(
            src_ref=stg.at[r >> 1, r & 1, x], dst_ref=land.at[r - 1, x], send_sem=rs_send.at[r, x], recv_sem=rs_recv.at[r, x],
            device_id={"ctx": nbr[plan.bwd[x].link[r]]}, device_id_type=MESH)

    def mate_copy(src, dst, sem):
        return pltpu.make_async_remote_copy(src_ref=src, dst_ref=dst, send_sem=x_send.at[sem], recv_sem=x_recv.at[sem],
                                            device_id={"ctx": mate}, device_id_type=MESH)

    ours, theirs = pl.ds(0, SPAN), pl.ds(SPAN, SPAN)

    for x in range(2):
        for k in plan.fwd[x].kids[0]:
            ag_copy(k, x).start()
    for copy in loads[4:]:
        copy.wait()
    x_q = [mate_copy(ref.at[h, pl.ds(0, HEADS)], ref.at[h, pl.ds(HEADS, HEADS)], 2 * j + h)
           for j, ref in enumerate((q_s, g_s)) for h in range(2)]
    for copy in x_q:
        copy.start()

    def ag_events(waits):
        return [act for r, x in waits for act in [ag_copy(r, x).wait_recv] + [ag_copy(k, x).start for k in plan.fwd[x].kids[r]]]

    coef = SCALE * LOG2E

    def transposes(h):
        def turn(i):
            cols = pl.ds(pl.multiple_of(i * 128, 128), 128)
            turned = q_s[h, i].T
            q_t[h, :, cols] = turned
            g_t[h, :, cols] = g_s[h, i].T
            scaled = turned.astype(f32) * coef
            high = scaled.astype(bf16)
            c_t[h, pl.ds(0, HD), cols] = high
            c_t[h, pl.ds(HD, HD), cols] = (scaled - high.astype(f32)).astype(bf16)

        return turn

    for h in range(2):
        pl.loop(0, HEADS)(transposes(h))
    for copy in x_q:
        copy.wait_recv()
    for h in range(2):
        pl.loop(HEADS, TILES)(transposes(h))

    def is_future(pair):
        rel = [mod(div(pair, 1 << (d - 1)), 2) for d in range(1, dims)]
        gp = [None] + [xor(gray[d], rel[d - 1]) for d in range(1, dims)]
        other = gp[1] if dims > 1 else 0
        for d in range(2, dims):
            bit = xor(gp[d], gp[d + 1]) if d % 2 == 0 and d + 1 < dims else gp[d]
            other = other + bit * (1 << (d - 1))
        return div(other - my_pair + plan.blocks, plan.blocks)

    def place(pair, a):
        mine = div(plan.blocks // 2 - pair, plan.blocks // 2)
        fut = is_future(pair)
        turn = (pair,)
        for slot in range(2):
            h = (1 - mine) * fut * slot
            turn += (mine * a, h, mine * a + 1 - mine, mine + h, mine * slot + (1 - mine) * (fut + (1 - fut) * slot))
        return turn

    def groups(turn, some):
        for slot in range(2):
            if not any(slot * HEADS <= b < slot * HEADS + HEADS for b in some):
                continue
            p0, h0, p1, h1, qg = turn[1 + 5 * slot:6 + 5 * slot]
            yield slot, ((turn[0], p0, h0), (turn[0], p1, h1)), qg

    def key_tile(where):
        return jnp.concatenate([kv[pair, par, 0, h] for pair, par, h in where], axis=0)

    def value_tile_t(where):
        return jnp.concatenate([kv[pair, par, 1, h] for pair, par, h in where], axis=1)

    def key_tile_t(where):
        return jnp.concatenate([kt_s[pair, par, h] for pair, par, h in where], axis=1)

    def tile_of(memo, slot, kind, where):
        key = (kind, slot)
        if key not in memo:
            memo[key] = value_tile_t(where) if kind == "v" else key_tile(where) if kind == "k" else key_tile_t(where)
        return memo[key]

    def tall(ref, qg, t):
        return ref[qg, pl.ds(2 * t, 2)].reshape(256, 128)

    def cols_of(t):
        return pl.ds(t * 256, 256)

    def rows(b):
        return pl.ds(b * 256, 256)

    def mask_scores(a, keys_axis):
        key_low = me + a * (2 * (1 - 2 * mod(chip, 2)))

        def two(base0, base1, axis):
            i = lax.broadcasted_iota(jnp.int32, (256, 256), axis)
            return i + jnp.where(i < PIECE, base0, base1 - PIECE)

        def query_base(c):
            h, par = div(c, TILES), mod(div(c, HEADS), 2)
            low = me + par * (mate - me)
            return (low + h * (pieces - 1 - 2 * low)) * PIECE

        @pl.loop(0, TILES)
        def _(b):
            kpos = two(key_low * PIECE, (pieces - 1 - key_low) * PIECE, keys_axis)
            qpos = two(query_base(2 * b), query_base(2 * b + 1), 1 - keys_axis)
            s = jnp.where(qpos >= kpos, s_buf[b], NEG)
            s_buf[b] = s
            if keys_axis == 0:
                top[b] = jnp.max(s.reshape(32, 8, 256), axis=0)

    def fwd_scores(turn, some, memo):
        for slot, where, qg in groups(turn, some):
            kt = tile_of(memo, slot, "k", where)
            twice = jnp.concatenate([kt, kt], axis=1)
            for t in range(HEADS):
                b, cols = slot * HEADS + t, cols_of(t)
                if b in some:
                    if t == 0:
                        for pair, par, h in where:
                            kt_s[pair, par, h] = kv[pair, par, 0, h].T
                    s = jnp.dot(twice, c_t[qg, :, cols], preferred_element_type=f32)
                    s_buf[b] = s
                    top[b] = jnp.max(s.reshape(32, 8, 256), axis=0)

    def fwd_softmax(turn, some):
        for slot, _, qg in groups(turn, some):
            for t in range(HEADS):
                b, cols = slot * HEADS + t, cols_of(t)
                if b not in some:
                    continue
                m_old = mst[qg, :, cols]
                m_new = jnp.maximum(m_old, jnp.max(top[b], axis=0, keepdims=True))
                p = jnp.exp2(s_buf[b] - m_new[0:1])
                decay = jnp.exp2(m_old - m_new)
                lst[qg, :, cols] = lst[qg, :, cols] * decay + jnp.sum(p.reshape(32, 8, 256), axis=0)
                p_buf[rows(b), :] = p.astype(bf16)
                dec[b] = decay
                mst[qg, :, cols] = m_new

    def fwd_out(turn, some, memo):
        for slot, where, qg in groups(turn, some):
            vt = tile_of(memo, slot, "v", where)
            for t in range(HEADS):
                b, cols = slot * HEADS + t, cols_of(t)
                if b in some:
                    pv = jnp.dot(vt, p_buf[rows(b), :], preferred_element_type=f32)
                    acc[qg, :, cols] = acc[qg, :, cols] * dec[b, 0:1] + pv

    def fwd_place(j):
        return place(lookup(jnp.minimum(j, turns - 1), plan.fwd_pairs), jnp.minimum(j, 1))

    every = range(TILES)
    for act in ag_events(plan.fwd_waits[0]):
        act()
    first = fwd_place(me * 0)
    fwd_scores(first, every, {})
    singles, doubles = plan.singles, plan.doubles

    def fwd_body(line):
        count = len(line) - 2
        memos = [{} for _ in line], [{} for _ in line]
        for b in range(count * TILES + 2):
            for lag, stage in ((2, 2), (1, 1), (0, 0)):
                i, tile = (b - lag) // TILES, (b - lag) % TILES
                if not 0 <= i < count:
                    continue
                if stage == 2:
                    fwd_scores(line[i + 2], (tile,), memos[0][i])
                elif stage == 1:
                    fwd_softmax(line[i + 1], (tile,))
                else:
                    fwd_out(line[i], (tile,), memos[1][i])

    def fwd_turn(j, carry):
        old, cur, new = carry
        branch(j, singles, lambda i: ag_events(plan.fwd_waits[i + 1]))

        @pl.when((j == 0) | (j == plan.fwd_mate))
        def _():
            mask_scores(jnp.minimum(j, 1), 0)

        after = fwd_place(j + 2)
        fwd_body((old, cur, new))
        return cur, new, after

    def fwd_double(i, carry):
        old, cur, new, then = carry
        branch(i, doubles, lambda i: ag_events(plan.fwd_waits[singles + 1 + i]))
        after = fwd_place(singles + 2 * i + 3), fwd_place(singles + 2 * i + 4)
        fwd_body((old, cur, new, then))
        return (new, then) + after

    old, cur, new = lax.fori_loop(0, singles, fwd_turn, (first, first, fwd_place(me * 0 + 1)))
    if doubles:
        old, cur, _, _ = lax.fori_loop(0, doubles, fwd_double, (old, cur, new, fwd_place(me * 0 + singles + 2)))
    for act in ag_events(plan.fwd_waits[singles + doubles + 1]):
        act()
    if plan.fwd_mate == turns - 1:
        mask_scores(1, 0)
    memo = {}
    for b in range(TILES + 1):
        fwd_softmax(cur, (b - 1,))
        fwd_out(old, (b,), memo)
    late = [b for b in every if b % HEADS < HEADS // 2]
    fwd_out(cur, [b for b in every if b not in late], {})

    def bwd_scores(turn, some, memo):
        for slot, where, qg in groups(turn, some):
            for t in range(HEADS):
                b, cols = slot * HEADS + t, cols_of(t)
                if b in some:
                    for buf, lhs, kind in ((s_buf, q_s, "t"), (t_buf, g_s, "v")):
                        buf[b] = jnp.dot(tall(lhs, qg, t), tile_of(memo, slot, kind, where), preferred_element_type=f32)

    def bwd_softmax(turn, some):
        for slot, _, qg in groups(turn, some):
            for t in range(HEADS):
                b, cols = slot * HEADS + t, cols_of(t)
                if b in some:
                    lse, dr = tall(lcol, qg, t), tall(dcol, qg, t)
                    p = jnp.exp2(s_buf[b] * coef - jnp.concatenate([lse, lse], axis=1))
                    p_buf[rows(b), :] = p.astype(bf16)
                    d_buf[rows(b), :] = (p * (t_buf[b] - jnp.concatenate([dr, dr], axis=1))).astype(bf16)

    def bwd_out(turn, some, memo, parts=(True, True)):
        for slot, where, qg in groups(turn, some):
            for t in range(HEADS):
                b, cols = slot * HEADS + t, cols_of(t)
                if b not in some:
                    continue
                ds = d_buf[rows(b), :]
                if parts[1]:
                    acc[qg, :, cols] += lax.dot_general(tile_of(memo, slot, "t", where), ds, (((1,), (1,)), ((), ())),
                                                         preferred_element_type=f32)
                for x, (ref, buf) in enumerate(((q_t, ds), (g_t, p_buf[rows(b), :])) if parts[0] else ()):
                    grad = jnp.dot(ref[qg, :, cols], buf, preferred_element_type=f32)
                    memo[x] = memo[x] + grad if t else grad
                    if t < HEADS - 1:
                        continue
                    for pair, par, _ in () if slot else where:
                        stg[pair, par, x, 1] = jnp.zeros((128, 128), f32)
                    for j, (pair, par, h) in enumerate(where):
                        value = memo[x][:, j * 128:j * 128 + 128]
                        stg[pair, par, x, h] = value + stg[pair, par, x, h] if slot else value

    def bwd_place(j):
        at = jnp.minimum(j, turns - 1)
        return place(lookup(at, plan.bwd_pairs), 1 - div(at + 1, turns))

    x_m = [mate_copy(ref.at[h, :, theirs], box.at[h], 4 + 3 * h + i)
           for h in range(2) for i, (ref, box) in enumerate(((acc, xacc), (mst, xm), (lst, xl)))]
    for copy in x_m:
        copy.start()
    fwd_out(cur, late, {})
    first = bwd_place(me * 0)
    bwd_scores(first, every, {})
    for k in range(1, plan.blocks):
        for x in range(2):
            ag_copy(k, x).wait_send()
    x_r = [mate_copy(ref.at[h, :, ours], ref.at[h, :, theirs], 10 + 2 * j + h) for j, ref in enumerate((lrow, drow)) for h in range(2)]

    for h in range(2):
        for copy in x_m[3 * h:3 * h + 3]:
            copy.wait_recv()
        for head in range(HEADS):
            cols = pl.ds(head * PIECE, PIECE)
            m1, m2 = mst[h, :, cols], xm[h, :, cols]
            m = jnp.maximum(m1, m2)
            w1, w2 = jnp.exp2(m1 - m), jnp.exp2(m2 - m)
            total = jnp.sum(lst[h, :, cols] * w1 + xl[h, :, cols] * w2, axis=0, keepdims=True)
            out = (acc[h, :, cols] * w1[0:1] + xacc[h, :, cols] * w2[0:1]) / total
            o_s[head, half(h), :] = out.T.astype(bf16)
            lrow[h, :, cols] = m + jnp.log2(total)
            rounded = out.astype(bf16).astype(f32)
            d = jnp.sum(rounded * g_t[h, :, cols].astype(f32), axis=0, keepdims=True)
            drow[h, :, cols] = jnp.broadcast_to(d, (8, 128))
        for copy in x_r[h::2]:
            copy.start()
    for copy in x_m:
        copy.wait_send()
    acc[...] = jnp.zeros(acc.shape, f32)
    stores = [pltpu.make_async_copy(o_s, o_ref, io.at[8])]
    stores[0].start()

    def columns(h, i):
        cols = pl.ds(i * 128, 128)
        for row, col in ((lrow, lcol), (drow, dcol)):
            col[h, i] = jnp.broadcast_to(row[h, 0:1, cols], (128, 128)).T

    def rs_sum(r, x, kids):
        for k in kids:
            rs_copy(k, x).wait_recv()
        for h in range(2):
            total = stg[r >> 1, r & 1, x, h]
            for k in kids:
                total = total + land[k - 1, x, h]
            stg[r >> 1, r & 1, x, h] = total

    def rs_events(sends):
        return ([functools.partial(rs_sum, r, x, plan.bwd[x].kids[r]) for r, x in sends if plan.bwd[x].kids[r]]
                + [rs_copy(r, x).start for r, x in sends])

    for i in range(TILES):
        columns(i // HEADS, i % HEADS)
    if turns < 4:
        mask_scores(turns - 1, 1)
    second, third = bwd_place(me * 0 + 1), bwd_place(me * 0 + 2)
    memo = {}
    for b in late:
        bwd_softmax(first, (b,))
        bwd_scores(second, (b,), memo)
    for copy in x_r:
        copy.wait_recv()
    for i in range(TILES):
        columns(i // HEADS, HEADS + i % HEADS)
    memo = {}
    for b in every:
        if b not in late:
            bwd_softmax(first, (b,))
            bwd_scores(second, (b,), memo)
    bwd_out(first, every, {}, (True, False))
    for act in rs_events(plan.bwd_sends[0]):
        act()
    bwd_out(first, every, {}, (False, True))
    if turns < 4:
        mask_scores(turns - 2, 1)
    memo = {}
    for b in range(TILES + 1):
        bwd_softmax(second, (b,))
        bwd_scores(third, (b - 1,), memo)

    def bwd_turn(j, carry):
        old, cur, new = carry
        branch(j, turns, lambda i: rs_events(plan.bwd_sends[i - 1]) if i > 1 else [])

        @pl.when(j >= turns - 2)
        def _():
            mask_scores(turns - 1 - j, 1)

        after = bwd_place(j + 2)
        memo, memo_old = {}, {}
        for b in range(TILES + 2):
            bwd_scores(new, (b - 2,), memo)
            bwd_out(old, (b - 1,), memo_old, (False, True))
            bwd_out(old, (b,), memo_old, (True, False))
            bwd_softmax(cur, (b - 1,))
        return cur, new, after

    last = lax.fori_loop(2, turns, bwd_turn, (second, third, bwd_place(me * 0 + 3)))[0]
    for act in rs_events(plan.bwd_sends[turns - 1]):
        act()
    bwd_out(last, every, {})

    x_d = [mate_copy(acc.at[h, :, theirs], xacc.at[h], 14 + h) for h in range(2)]
    for copy in x_d:
        copy.start()
    for unit in plan.bwd_sends[turns]:
        for act in rs_events([unit]):
            act()
    for h in range(2):
        x_d[h].wait_recv()
        for head in range(HEADS):
            cols = pl.ds(head * PIECE, PIECE)
            total = (acc[h, :, cols] + xacc[h, :, cols]) * SCALE
            dq_o[head, half(h), :] = total.T.astype(bf16)
    stores.append(pltpu.make_async_copy(dq_o, dq_ref, io.at[9]))
    stores[1].start()
    for k in range(1, plan.blocks):
        for x in range(2):
            rs_copy(k, x).wait_send()
    for copy in x_q + x_r + x_d:
        copy.wait_send()
    left = [dims, dims]
    for k, x in plan.bwd_last:
        rs_sum(0, x, [k])
        left[x] -= 1
        if not left[x]:
            buf, ref, factor = ((dk_o, dk_ref, SCALE), (dv_o, dv_ref, 1.0))[x]
            for h in range(2):
                buf[half(h), :] = (stg[0, 0, x, h] * factor).T.astype(bf16)
            stores.append(pltpu.make_async_copy(buf, ref, io.at[10 + x]))
            stores[-1].start()

    for copy in stores:
        copy.wait()


def relay(*refs):
    count = (len(refs) - 1) // 3
    src, dst, buf, sem = refs[:count], refs[count:2 * count], refs[2 * count:3 * count], refs[3 * count]
    into = [pltpu.make_async_copy(a, b, sem.at[i]) for i, (a, b) in enumerate(zip(src, buf))]
    out = [pltpu.make_async_copy(b, c, sem.at[count + i]) for i, (b, c) in enumerate(zip(buf, dst))]
    for copy in into:
        copy.start()
    for i in range(count):
        into[i].wait()
        out[i].start()
    for copy in out:
        copy.wait()


def solution(mesh):
    size = mesh.shape["ctx"]
    plan = Plan(int(math.log2(size)) - 1)
    spec = P("data", "ctx", None, None)
    n = plan.blocks
    f32, bf16 = jnp.float32, jnp.bfloat16
    vm, sem = pltpu.VMEM, pltpu.SemaphoreType.DMA

    def local(queries, keys, values, grad_out):
        tokens = queries.shape[1]
        q = queries[0].transpose(1, 0, 2)
        g = grad_out[0].transpose(1, 0, 2)
        tile = (128, 128)
        big = jax.ShapeDtypeStruct((HEADS, tokens, HD), bf16)
        small = jax.ShapeDtypeStruct((tokens, HD), bf16)
        anywhere = pl.BlockSpec(memory_space=pl.ANY)
        rows, wide, half_wide = (2, TILES) + tile, (2, HD, 2 * SPAN), (2, HD, SPAN)
        stat, few = (2, 8, 2 * SPAN), (2, 8, SPAN)
        results = pl.pallas_call(
            functools.partial(kernel, plan),
            out_shape=(big, big, small, small),
            in_specs=[anywhere] * 4,
            out_specs=(anywhere,) * 4,
            scratch_shapes=[
                vm((n // 2, 2, 2, 2) + tile, bf16), vm((n // 2, 2, 2) + tile, bf16), vm((n // 2, 2, 2, 2) + tile, f32), vm((n - 1, 2, 2) + tile, f32),
                vm((TILES, 256, 256), f32), vm((TILES, 256, 256), f32), vm((TILES * 256, 256), bf16), vm((TILES * 256, 256), bf16),
                vm((TILES, 8, 256), f32),
                vm(rows, bf16), vm(rows, bf16), vm((2,) + tile, bf16), vm(wide, bf16), vm(wide, bf16), vm((2, 2 * HD, 2 * SPAN), bf16),
                vm(wide, f32), vm(stat, f32), vm(stat, f32), vm((TILES, 8, 256), f32),
                vm(half_wide, f32), vm(few, f32), vm(few, f32), vm(stat, f32), vm(stat, f32), vm(rows, f32), vm(rows, f32),
                vm(big.shape, bf16), vm(big.shape, bf16), vm(small.shape, bf16), vm(small.shape, bf16),
                sem((n, 2)), sem((n, 2)), sem((n, 2)), sem((n, 2)), sem((16,)), sem((16,)), sem((12,)),
            ],
            compiler_params=pltpu.CompilerParams(collective_id=0, has_side_effects=True, vmem_limit_bytes=67043328),
            cost_estimate=pl.CostEstimate(flops=14 * 640 * PIECE * n * 2 * HD, bytes_accessed=4 << 20, transcendentals=0),
        )(q, keys[0, :, 0], values[0, :, 0], g)
        o, dq, dk, dv = pl.pallas_call(
            relay,
            out_shape=(big, big, small, small),
            in_specs=[anywhere] * 4,
            out_specs=(anywhere,) * 4,
            scratch_shapes=[vm(x.shape, bf16) for x in (big, big, small, small)] + [sem((8,))],
            cost_estimate=pl.CostEstimate(flops=1 << 20, bytes_accessed=2 << 20, transcendentals=0),
        )(*results)
        return (o.transpose(1, 0, 2)[None], dq.transpose(1, 0, 2)[None], dk[None, :, None], dv[None, :, None])

    return jax.shard_map(local, mesh=mesh, in_specs=(spec,) * 4, out_specs=(spec,) * 4, check_vma=False)
```

```python
import functools
import math

import jax
import jax.numpy as jnp
from jax import lax
from jax.experimental import pallas as pl
from jax.experimental.pallas import tpu as pltpu
from jax.sharding import PartitionSpec as P

MESH = pl.DeviceIdType.MESH
NEG = -1e30
HD = 128
HEADS = 5
PIECE = 128
SCALE = HD ** -0.5
LOG2E = 1.4426950408889634
TILES = 2 * HEADS
SPAN = HEADS * PIECE

KEY_TREE = "011222133332330444044204331303450512252553132154554251534405024"
VALUE_TREE = "011202133303032404124114441201150505210501022525540551434312353"
DK_TREE = "011202030312311404440413410322055502551351320125544451033135454"
DV_TREE = "011222133313020444022124310233455512520331055524450502154433451"
BWD_ORDER = "vtrujnfsd7meockplbq36i95ha8g124"


def popcount(value):
    return bin(value).count("1")


class Tree:
    def __init__(self, dims, links):
        blocks = 1 << dims
        if dims == 6:
            self.link = [None] + [int(d) for d in links]
        else:
            self.link = [None] * blocks
            count = [0] * dims
            for r in sorted(range(1, blocks), key=popcount):
                self.link[r] = min((d for d in range(dims) if (r >> d) & 1), key=lambda d: count[d])
                count[self.link[r]] += 1
        self.kids = {r: [k for k in range(1, blocks) if k & ~(1 << self.link[k]) == r] for r in range(blocks)}
        height = {}
        for r in sorted(range(blocks), key=popcount, reverse=True):
            height[r] = max([1 + height[k] for k in self.kids[r]], default=0)
        for r in self.kids:
            self.kids[r].sort(key=lambda k: -height[k])


class Plan:
    def __init__(self, dims):
        self.dims = dims
        self.blocks = 1 << dims
        self.turns = self.blocks // 2 + 1
        self.fwd = [Tree(dims, KEY_TREE), Tree(dims, VALUE_TREE)]
        self.bwd = [Tree(dims, DK_TREE), Tree(dims, DV_TREE)]
        self.forward()
        self.backward()

    def forward(self, unit_us=1.41, hop_us=1.9, turn_us=0.78):
        free = [0.0] * self.dims
        due = {}
        done = {(0, 0), (0, 1)}
        now = 1.0
        steps, waits, ready, order = [], [], [0], []

        def send(r, x):
            for k in self.fwd[x].kids[r]:
                d = self.fwd[x].link[k]
                free[d] = max(free[d], now) + unit_us
                due[k, x] = free[d] + hop_us

        now = 0.0
        send(0, 0)
        send(0, 1)
        now = 1.0
        while True:
            for unit in sorted((u for u in due if u not in done and due[u] <= now), key=lambda u: (due[u], u)):
                done.add(unit)
                now += 0.02
                send(*unit)
                waits.append(unit)
                if unit[1] == 0 and (unit[0] ^ 1, 0) in done:
                    ready.append(unit[0] >> 1)
            turn = len(steps)
            late = order[max(turn - 2, 0):turn - 1] if turn < self.turns else order[turn - 2:]
            lacking = [r for pair in late for r in (2 * pair, 2 * pair + 1) if (r, 1) not in done]
            if turn == 2 < self.turns:
                lacking = []
            if lacking or not (ready or turn == self.turns):
                now = max(now, min(due[u] for u in due if u not in done))
                continue
            if turn == self.turns:
                break
            order.append(ready.pop(0))
            steps.append(waits)
            waits = []
            now += turn_us if turn else 0.0
        self.fwd_waits = steps + [waits]
        self.fwd_pairs = order
        self.fwd_mate = max(i for i, pair in enumerate(order) if pair == 0)

    def backward(self, unit_us=2.84, hop_us=2.75, turn_us=1.62, add_us=0.025):
        if self.dims == 6:
            order = [int(c, 32) for c in BWD_ORDER]
        else:
            order = sorted(range(1, self.blocks // 2), key=lambda pair: -popcount(pair))
        order += [0, 0]
        free = [0.0] * self.dims
        due = {}
        waiting, sends, steps = set(), [], []
        now = 1.65

        def kids(unit):
            return [(k, unit[1]) for k in self.bwd[unit[1]].kids[unit[0]]]

        def flush():
            nonlocal now
            able = True
            while able:
                able = [u for u in waiting if all(due.get(k, 1e9) <= now for k in kids(u))]
                for unit in sorted(able, key=lambda u: (-popcount(u[0]), u)):
                    waiting.discard(unit)
                    now += add_us * len(kids(unit)) + 0.01
                    d = self.bwd[unit[1]].link[unit[0]]
                    free[d] = max(free[d], now) + unit_us
                    due[unit] = free[d] + hop_us
                    sends.append(unit)

        for i, pair in enumerate(order):
            if i:
                now += 0.12
                flush()
                steps.append(sends)
                sends = []
                now += turn_us
            waiting |= {(r, x) for r in (2 * pair, 2 * pair + 1) for x in range(2) if r} if i < len(order) - 1 else set()
            if not i:
                flush()
                steps.append(sends)
                sends = []
                now += 0.9
        flush()
        while waiting:
            now = max(now, min(max(due.get(k, 1e9) for k in kids(u)) for u in waiting))
            flush()
        self.bwd_sends = steps + [sends]
        self.bwd_pairs = order
        self.bwd_last = sorted((u for x in range(2) for u in kids((0, x))), key=lambda u: due[u])


def div(a, b):
    return lax.div(a, jnp.int32(b))


def mod(a, b):
    return lax.rem(a, jnp.int32(b))


def xor(a, b):
    return a + b - 2 * a * b


def lookup(index, table):
    level = [jnp.int32(v) for v in table]
    bit = 1
    while len(level) > 1:
        odd = mod(div(index, bit), 2) == 1
        nxt = [jnp.where(odd, level[i + 1], level[i]) for i in range(0, len(level) - 1, 2)]
        level = nxt + level[2 * len(nxt):]
        bit *= 2
    return level[0]


def branch(index, count, leaf):
    once = div(index, count) + 1

    def pick(low, high):
        if high - low == 1:
            acts = leaf(low)
            if acts:
                pl.loop(0, once)(lambda _: [act() for act in acts] and None)
            return
        mid = (low + high) // 2
        lax.cond(index < mid, lambda: pick(low, mid), lambda: pick(mid, high))

    pick(0, count)


def kernel(plan, q_ref, k_ref, v_ref, g_ref, o_ref, dq_ref, dk_ref, dv_ref,
           kv, kt_s, stg, land, s_buf, t_buf, p_buf, d_buf, top, q_s, g_s, v_s, q_t, g_t, c_t, acc, mst, lst, dec,
           xacc, xm, xl, lrow, drow, lcol, dcol, o_s, dq_o, dk_o, dv_o,
           ag_send, ag_recv, rs_send, rs_recv, x_send, x_recv, io):
    dims, turns = plan.dims, plan.turns
    pieces = 4 * plan.blocks
    f32, bf16 = jnp.float32, jnp.bfloat16
    me = lax.axis_index("ctx")
    core = mod(me, 2)
    chip = div(me, 2)
    bits = [mod(div(chip, 1 << d), 2) for d in range(dims)]
    gray = [xor(bits[d], bits[d + 1]) if d % 2 == 0 and d + 1 < dims else bits[d] for d in range(dims)]
    nbr = []
    for d in range(dims):
        other = chip + (1 - 2 * bits[d]) * (1 << d)
        if d % 2:
            other = other + (1 - 2 * bits[d - 1]) * (1 << (d - 1))
        nbr.append(2 * other + core)
    mate = me + 1 - 2 * core
    my_pair = div(chip, 2)

    barrier = pltpu.get_barrier_semaphore()
    for dev in nbr + [mate]:
        pl.semaphore_signal(barrier, inc=1, device_id={"ctx": dev}, device_id_type=MESH)

    def half(h):
        return pl.ds(h * PIECE, PIECE)

    loads = []
    for h in range(2):
        loads += [pltpu.make_async_copy(k_ref.at[half(h)], kv.at[0, 0, 0, h], io.at[h]),
                  pltpu.make_async_copy(v_ref.at[half(h)], v_s.at[h], io.at[2 + h])]
    for h in range(2):
        for j, (src, dst) in enumerate(((q_ref, q_s), (g_ref, g_s))):
            loads.append(pltpu.make_async_copy(src.at[:, half(h)], dst.at[h, pl.ds(0, HEADS)], io.at[4 + 2 * j + h]))
    for copy in loads:
        copy.start()
    mst[...] = jnp.full(mst.shape, NEG, f32)
    lst[...] = jnp.zeros(lst.shape, f32)
    acc[...] = jnp.zeros(acc.shape, f32)
    dec[...] = jnp.ones(dec.shape, f32)
    p_buf[...] = jnp.zeros(p_buf.shape, bf16)
    for copy in loads[:4]:
        copy.wait()
    for h in range(2):
        kv[0, 0, 1, h] = v_s[h].T

    pl.semaphore_wait(barrier, dims + 1)

    def ag_copy(k, x):
        d = plan.fwd[x].link[k]
        r = k ^ (1 << d)
        return pltpu.make_async_remote_copy(
            src_ref=kv.at[r >> 1, r & 1, x], dst_ref=kv.at[k >> 1, k & 1, x], send_sem=ag_send.at[k, x],
            recv_sem=ag_recv.at[k, x], device_id={"ctx": nbr[d]}, device_id_type=MESH)

    def rs_copy(r, x):
        return pltpu.make_async_remote_copy(
            src_ref=stg.at[r >> 1, r & 1, x], dst_ref=land.at[r - 1, x], send_sem=rs_send.at[r, x], recv_sem=rs_recv.at[r, x],
            device_id={"ctx": nbr[plan.bwd[x].link[r]]}, device_id_type=MESH)

    def mate_copy(src, dst, sem):
        return pltpu.make_async_remote_copy(src_ref=src, dst_ref=dst, send_sem=x_send.at[sem], recv_sem=x_recv.at[sem],
                                            device_id={"ctx": mate}, device_id_type=MESH)

    ours, theirs = pl.ds(0, SPAN), pl.ds(SPAN, SPAN)

    for x in range(2):
        for k in plan.fwd[x].kids[0]:
            ag_copy(k, x).start()
    for copy in loads[4:]:
        copy.wait()
    x_q = [mate_copy(ref.at[h, pl.ds(0, HEADS)], ref.at[h, pl.ds(HEADS, HEADS)], 2 * j + h)
           for j, ref in enumerate((q_s, g_s)) for h in range(2)]
    for copy in x_q:
        copy.start()

    def ag_events(waits):
        return [act for r, x in waits for act in [ag_copy(r, x).wait_recv] + [ag_copy(k, x).start for k in plan.fwd[x].kids[r]]]

    coef = SCALE * LOG2E

    def transposes(h):
        def turn(i):
            cols = pl.ds(pl.multiple_of(i * 128, 128), 128)
            turned = q_s[h, i].T
            q_t[h, :, cols] = turned
            g_t[h, :, cols] = g_s[h, i].T
            scaled = turned.astype(f32) * coef
            high = scaled.astype(bf16)
            c_t[h, pl.ds(0, HD), cols] = high
            c_t[h, pl.ds(HD, HD), cols] = (scaled - high.astype(f32)).astype(bf16)

        return turn

    for h in range(2):
        pl.loop(0, HEADS)(transposes(h))
    for copy in x_q:
        copy.wait_recv()
    for h in range(2):
        pl.loop(HEADS, TILES)(transposes(h))

    def is_future(pair):
        rel = [mod(div(pair, 1 << (d - 1)), 2) for d in range(1, dims)]
        gp = [None] + [xor(gray[d], rel[d - 1]) for d in range(1, dims)]
        other = gp[1] if dims > 1 else 0
        for d in range(2, dims):
            bit = xor(gp[d], gp[d + 1]) if d % 2 == 0 and d + 1 < dims else gp[d]
            other = other + bit * (1 << (d - 1))
        return div(other - my_pair + plan.blocks, plan.blocks)

    def place(pair, a):
        mine = div(plan.blocks // 2 - pair, plan.blocks // 2)
        fut = is_future(pair)
        turn = (pair,)
        for slot in range(2):
            h = (1 - mine) * fut * slot
            turn += (mine * a, h, mine * a + 1 - mine, mine + h, mine * slot + (1 - mine) * (fut + (1 - fut) * slot))
        return turn

    def groups(turn, some):
        for slot in range(2):
            if not any(slot * HEADS <= b < slot * HEADS + HEADS for b in some):
                continue
            p0, h0, p1, h1, qg = turn[1 + 5 * slot:6 + 5 * slot]
            yield slot, ((turn[0], p0, h0), (turn[0], p1, h1)), qg

    def key_tile(where):
        return jnp.concatenate([kv[pair, par, 0, h] for pair, par, h in where], axis=0)

    def value_tile_t(where):
        return jnp.concatenate([kv[pair, par, 1, h] for pair, par, h in where], axis=1)

    def key_tile_t(where):
        return jnp.concatenate([kt_s[pair, par, h] for pair, par, h in where], axis=1)

    def tile_of(memo, slot, kind, where):
        key = (kind, slot)
        if key not in memo:
            memo[key] = value_tile_t(where) if kind == "v" else key_tile(where) if kind == "k" else key_tile_t(where)
        return memo[key]

    def tall(ref, qg, t):
        return ref[qg, pl.ds(2 * t, 2)].reshape(256, 128)

    def cols_of(t):
        return pl.ds(t * 256, 256)

    def rows(b):
        return pl.ds(b * 256, 256)

    def mask_scores(a, keys_axis):
        key_low = me + a * (2 * (1 - 2 * mod(chip, 2)))

        def two(base0, base1, axis):
            i = lax.broadcasted_iota(jnp.int32, (256, 256), axis)
            return i + jnp.where(i < PIECE, base0, base1 - PIECE)

        def query_base(c):
            h, par = div(c, TILES), mod(div(c, HEADS), 2)
            low = me + par * (mate - me)
            return (low + h * (pieces - 1 - 2 * low)) * PIECE

        @pl.loop(0, TILES)
        def _(b):
            kpos = two(key_low * PIECE, (pieces - 1 - key_low) * PIECE, keys_axis)
            qpos = two(query_base(2 * b), query_base(2 * b + 1), 1 - keys_axis)
            s = jnp.where(qpos >= kpos, s_buf[b], NEG)
            s_buf[b] = s
            if keys_axis == 0:
                top[b] = jnp.max(s.reshape(32, 8, 256), axis=0)

    def fwd_scores(turn, some, memo):
        for slot, where, qg in groups(turn, some):
            kt = tile_of(memo, slot, "k", where)
            twice = jnp.concatenate([kt, kt], axis=1)
            for t in range(HEADS):
                b, cols = slot * HEADS + t, cols_of(t)
                if b in some:
                    if t == 0:
                        for pair, par, h in where:
                            kt_s[pair, par, h] = kv[pair, par, 0, h].T
                    s = jnp.dot(twice, c_t[qg, :, cols], preferred_element_type=f32)
                    s_buf[b] = s
                    top[b] = jnp.max(s.reshape(32, 8, 256), axis=0)

    def fwd_softmax(turn, some):
        for slot, _, qg in groups(turn, some):
            for t in range(HEADS):
                b, cols = slot * HEADS + t, cols_of(t)
                if b not in some:
                    continue
                m_old = mst[qg, :, cols]
                m_new = jnp.maximum(m_old, jnp.max(top[b], axis=0, keepdims=True))
                p = jnp.exp2(s_buf[b] - m_new[0:1])
                decay = jnp.exp2(m_old - m_new)
                lst[qg, :, cols] = lst[qg, :, cols] * decay + jnp.sum(p.reshape(32, 8, 256), axis=0)
                p_buf[rows(b), :] = p.astype(bf16)
                dec[b] = decay
                mst[qg, :, cols] = m_new

    def fwd_out(turn, some, memo):
        for slot, where, qg in groups(turn, some):
            vt = tile_of(memo, slot, "v", where)
            for t in range(HEADS):
                b, cols = slot * HEADS + t, cols_of(t)
                if b in some:
                    pv = jnp.dot(vt, p_buf[rows(b), :], preferred_element_type=f32)
                    acc[qg, :, cols] = acc[qg, :, cols] * dec[b, 0:1] + pv

    def fwd_place(j):
        return place(lookup(jnp.minimum(j, turns - 1), plan.fwd_pairs), jnp.minimum(j, 1))

    every = range(TILES)
    for act in ag_events(plan.fwd_waits[0]):
        act()
    first = fwd_place(me * 0)
    fwd_scores(first, every, {})

    def fwd_turn(j, carry):
        old, cur, new = carry
        branch(j, turns, lambda i: ag_events(plan.fwd_waits[i + 1]))

        @pl.when((j == 0) | (j == plan.fwd_mate))
        def _():
            mask_scores(jnp.minimum(j, 1), 0)

        after = fwd_place(j + 2)
        memo, memo_old = {}, {}
        for b in range(TILES + 2):
            fwd_scores(new, (b - 2,), memo)
            fwd_softmax(cur, (b - 1,))
            fwd_out(old, (b,), memo_old)
        return cur, new, after

    old, cur, _ = lax.fori_loop(0, turns - 1, fwd_turn, (first, first, fwd_place(me * 0 + 1)))
    for act in ag_events(plan.fwd_waits[turns]):
        act()
    if plan.fwd_mate == turns - 1:
        mask_scores(1, 0)
    memo = {}
    for b in range(TILES + 1):
        fwd_softmax(cur, (b - 1,))
        fwd_out(old, (b,), memo)
    late = [b for b in every if b % HEADS < HEADS // 2]
    fwd_out(cur, [b for b in every if b not in late], {})

    def bwd_scores(turn, some, memo):
        for slot, where, qg in groups(turn, some):
            for t in range(HEADS):
                b, cols = slot * HEADS + t, cols_of(t)
                if b in some:
                    for buf, lhs, kind in ((s_buf, q_s, "t"), (t_buf, g_s, "v")):
                        buf[b] = jnp.dot(tall(lhs, qg, t), tile_of(memo, slot, kind, where), preferred_element_type=f32)

    def bwd_softmax(turn, some):
        for slot, _, qg in groups(turn, some):
            for t in range(HEADS):
                b, cols = slot * HEADS + t, cols_of(t)
                if b in some:
                    lse, dr = tall(lcol, qg, t), tall(dcol, qg, t)
                    p = jnp.exp2(s_buf[b] * coef - jnp.concatenate([lse, lse], axis=1))
                    p_buf[rows(b), :] = p.astype(bf16)
                    d_buf[rows(b), :] = (p * (t_buf[b] - jnp.concatenate([dr, dr], axis=1))).astype(bf16)

    def bwd_out(turn, some, memo, parts=(True, True)):
        for slot, where, qg in groups(turn, some):
            for t in range(HEADS):
                b, cols = slot * HEADS + t, cols_of(t)
                if b not in some:
                    continue
                ds = d_buf[rows(b), :]
                if parts[1]:
                    acc[qg, :, cols] += lax.dot_general(tile_of(memo, slot, "t", where), ds, (((1,), (1,)), ((), ())),
                                                         preferred_element_type=f32)
                for x, (ref, buf) in enumerate(((q_t, ds), (g_t, p_buf[rows(b), :])) if parts[0] else ()):
                    grad = jnp.dot(ref[qg, :, cols], buf, preferred_element_type=f32)
                    memo[x] = memo[x] + grad if t else grad
                    if t < HEADS - 1:
                        continue
                    for pair, par, _ in () if slot else where:
                        stg[pair, par, x, 1] = jnp.zeros((128, 128), f32)
                    for j, (pair, par, h) in enumerate(where):
                        value = memo[x][:, j * 128:j * 128 + 128]
                        stg[pair, par, x, h] = value + stg[pair, par, x, h] if slot else value

    def bwd_place(j):
        at = jnp.minimum(j, turns - 1)
        return place(lookup(at, plan.bwd_pairs), 1 - div(at + 1, turns))

    x_m = [mate_copy(ref.at[h, :, theirs], box.at[h], 4 + 3 * h + i)
           for h in range(2) for i, (ref, box) in enumerate(((acc, xacc), (mst, xm), (lst, xl)))]
    for copy in x_m:
        copy.start()
    fwd_out(cur, late, {})
    first = bwd_place(me * 0)
    bwd_scores(first, every, {})
    for k in range(1, plan.blocks):
        for x in range(2):
            ag_copy(k, x).wait_send()
    x_r = [mate_copy(ref.at[h, :, ours], ref.at[h, :, theirs], 10 + 2 * j + h) for j, ref in enumerate((lrow, drow)) for h in range(2)]

    for h in range(2):
        for copy in x_m[3 * h:3 * h + 3]:
            copy.wait_recv()
        for head in range(HEADS):
            cols = pl.ds(head * PIECE, PIECE)
            m1, m2 = mst[h, :, cols], xm[h, :, cols]
            m = jnp.maximum(m1, m2)
            w1, w2 = jnp.exp2(m1 - m), jnp.exp2(m2 - m)
            total = jnp.sum(lst[h, :, cols] * w1 + xl[h, :, cols] * w2, axis=0, keepdims=True)
            out = (acc[h, :, cols] * w1[0:1] + xacc[h, :, cols] * w2[0:1]) / total
            o_s[head, half(h), :] = out.T.astype(bf16)
            lrow[h, :, cols] = m + jnp.log2(total)
            rounded = out.astype(bf16).astype(f32)
            d = jnp.sum(rounded * g_t[h, :, cols].astype(f32), axis=0, keepdims=True)
            drow[h, :, cols] = jnp.broadcast_to(d, (8, 128))
        for copy in x_r[h::2]:
            copy.start()
    for copy in x_m:
        copy.wait_send()
    acc[...] = jnp.zeros(acc.shape, f32)
    stores = [pltpu.make_async_copy(o_s, o_ref, io.at[8])]
    stores[0].start()

    def columns(h, i):
        cols = pl.ds(i * 128, 128)
        for row, col in ((lrow, lcol), (drow, dcol)):
            col[h, i] = jnp.broadcast_to(row[h, 0:1, cols], (128, 128)).T

    def rs_sum(r, x, kids):
        for k in kids:
            rs_copy(k, x).wait_recv()
        for h in range(2):
            total = stg[r >> 1, r & 1, x, h]
            for k in kids:
                total = total + land[k - 1, x, h]
            stg[r >> 1, r & 1, x, h] = total

    def rs_events(sends):
        return ([functools.partial(rs_sum, r, x, plan.bwd[x].kids[r]) for r, x in sends if plan.bwd[x].kids[r]]
                + [rs_copy(r, x).start for r, x in sends])

    for i in range(TILES):
        columns(i // HEADS, i % HEADS)
    if turns < 4:
        mask_scores(turns - 1, 1)
    second, third = bwd_place(me * 0 + 1), bwd_place(me * 0 + 2)
    memo = {}
    for b in late:
        bwd_softmax(first, (b,))
        bwd_scores(second, (b,), memo)
    for copy in x_r:
        copy.wait_recv()
    for i in range(TILES):
        columns(i // HEADS, HEADS + i % HEADS)
    memo = {}
    for b in every:
        if b not in late:
            bwd_softmax(first, (b,))
            bwd_scores(second, (b,), memo)
    bwd_out(first, every, {}, (True, False))
    for act in rs_events(plan.bwd_sends[0]):
        act()
    bwd_out(first, every, {}, (False, True))
    if turns < 4:
        mask_scores(turns - 2, 1)
    memo = {}
    for b in range(TILES + 1):
        bwd_softmax(second, (b,))
        bwd_scores(third, (b - 1,), memo)

    def bwd_turn(j, carry):
        old, cur, new = carry
        branch(j, turns, lambda i: rs_events(plan.bwd_sends[i - 1]) if i > 1 else [])

        @pl.when(j >= turns - 2)
        def _():
            mask_scores(turns - 1 - j, 1)

        after = bwd_place(j + 2)
        memo, memo_old = {}, {}
        for b in range(TILES + 2):
            bwd_scores(new, (b - 2,), memo)
            bwd_out(old, (b - 1,), memo_old, (False, True))
            bwd_out(old, (b,), memo_old, (True, False))
            bwd_softmax(cur, (b - 1,))
        return cur, new, after

    last = lax.fori_loop(2, turns, bwd_turn, (second, third, bwd_place(me * 0 + 3)))[0]
    for act in rs_events(plan.bwd_sends[turns - 1]):
        act()
    bwd_out(last, every, {})

    x_d = [mate_copy(acc.at[h, :, theirs], xacc.at[h], 14 + h) for h in range(2)]
    for copy in x_d:
        copy.start()
    for unit in plan.bwd_sends[turns]:
        for act in rs_events([unit]):
            act()
    for h in range(2):
        x_d[h].wait_recv()
        for head in range(HEADS):
            cols = pl.ds(head * PIECE, PIECE)
            total = (acc[h, :, cols] + xacc[h, :, cols]) * SCALE
            dq_o[head, half(h), :] = total.T.astype(bf16)
    stores.append(pltpu.make_async_copy(dq_o, dq_ref, io.at[9]))
    stores[1].start()
    for k in range(1, plan.blocks):
        for x in range(2):
            rs_copy(k, x).wait_send()
    for copy in x_q + x_r + x_d:
        copy.wait_send()
    left = [dims, dims]
    for k, x in plan.bwd_last:
        rs_sum(0, x, [k])
        left[x] -= 1
        if not left[x]:
            buf, ref, factor = ((dk_o, dk_ref, SCALE), (dv_o, dv_ref, 1.0))[x]
            for h in range(2):
                buf[half(h), :] = (stg[0, 0, x, h] * factor).T.astype(bf16)
            stores.append(pltpu.make_async_copy(buf, ref, io.at[10 + x]))
            stores[-1].start()

    for copy in stores:
        copy.wait()


def relay(*refs):
    count = (len(refs) - 1) // 3
    src, dst, buf, sem = refs[:count], refs[count:2 * count], refs[2 * count:3 * count], refs[3 * count]
    into = [pltpu.make_async_copy(a, b, sem.at[i]) for i, (a, b) in enumerate(zip(src, buf))]
    out = [pltpu.make_async_copy(b, c, sem.at[count + i]) for i, (b, c) in enumerate(zip(buf, dst))]
    for copy in into:
        copy.start()
    for i in range(count):
        into[i].wait()
        out[i].start()
    for copy in out:
        copy.wait()


def solution(mesh):
    size = mesh.shape["ctx"]
    plan = Plan(int(math.log2(size)) - 1)
    spec = P("data", "ctx", None, None)
    n = plan.blocks
    f32, bf16 = jnp.float32, jnp.bfloat16
    vm, sem = pltpu.VMEM, pltpu.SemaphoreType.DMA

    def local(queries, keys, values, grad_out):
        tokens = queries.shape[1]
        q = queries[0].transpose(1, 0, 2)
        g = grad_out[0].transpose(1, 0, 2)
        tile = (128, 128)
        big = jax.ShapeDtypeStruct((HEADS, tokens, HD), bf16)
        small = jax.ShapeDtypeStruct((tokens, HD), bf16)
        anywhere = pl.BlockSpec(memory_space=pl.ANY)
        rows, wide, half_wide = (2, TILES) + tile, (2, HD, 2 * SPAN), (2, HD, SPAN)
        stat, few = (2, 8, 2 * SPAN), (2, 8, SPAN)
        results = pl.pallas_call(
            functools.partial(kernel, plan),
            out_shape=(big, big, small, small),
            in_specs=[anywhere] * 4,
            out_specs=(anywhere,) * 4,
            scratch_shapes=[
                vm((n // 2, 2, 2, 2) + tile, bf16), vm((n // 2, 2, 2) + tile, bf16), vm((n // 2, 2, 2, 2) + tile, f32), vm((n - 1, 2, 2) + tile, f32),
                vm((TILES, 256, 256), f32), vm((TILES, 256, 256), f32), vm((TILES * 256, 256), bf16), vm((TILES * 256, 256), bf16),
                vm((TILES, 8, 256), f32),
                vm(rows, bf16), vm(rows, bf16), vm((2,) + tile, bf16), vm(wide, bf16), vm(wide, bf16), vm((2, 2 * HD, 2 * SPAN), bf16),
                vm(wide, f32), vm(stat, f32), vm(stat, f32), vm((TILES, 8, 256), f32),
                vm(half_wide, f32), vm(few, f32), vm(few, f32), vm(stat, f32), vm(stat, f32), vm(rows, f32), vm(rows, f32),
                vm(big.shape, bf16), vm(big.shape, bf16), vm(small.shape, bf16), vm(small.shape, bf16),
                sem((n, 2)), sem((n, 2)), sem((n, 2)), sem((n, 2)), sem((16,)), sem((16,)), sem((12,)),
            ],
            compiler_params=pltpu.CompilerParams(collective_id=0, has_side_effects=True, vmem_limit_bytes=67043328),
            cost_estimate=pl.CostEstimate(flops=14 * 640 * PIECE * n * 2 * HD, bytes_accessed=4 << 20, transcendentals=0),
        )(q, keys[0, :, 0], values[0, :, 0], g)
        o, dq, dk, dv = pl.pallas_call(
            relay,
            out_shape=(big, big, small, small),
            in_specs=[anywhere] * 4,
            out_specs=(anywhere,) * 4,
            scratch_shapes=[vm(x.shape, bf16) for x in (big, big, small, small)] + [sem((8,))],
            cost_estimate=pl.CostEstimate(flops=1 << 20, bytes_accessed=2 << 20, transcendentals=0),
        )(*results)
        return (o.transpose(1, 0, 2)[None], dq.transpose(1, 0, 2)[None], dk[None, :, None], dv[None, :, None])

    return jax.shard_map(local, mesh=mesh, in_specs=(spec,) * 4, out_specs=(spec,) * 4, check_vma=False)
```

```python
import functools
import math

import jax
import jax.numpy as jnp
from jax import lax
from jax.experimental import pallas as pl
from jax.experimental.pallas import tpu as pltpu
from jax.sharding import PartitionSpec as P

MESH = pl.DeviceIdType.MESH
NEG = -1e30
HD = 128
HEADS = 5
PIECE = 128
SCALE = HD ** -0.5
LOG2E = 1.4426950408889634
TILES = 2 * HEADS
SPAN = HEADS * PIECE

KEY_TREE = "011222133332330444044204331303450512252553132154554251534405024"
VALUE_TREE = "011202133303032404124114441201150505210501022525540551434312353"
DK_TREE = "010221133103211404040144031203455152212301535105514225055432452"
DV_TREE = "011221033332230444442413330244055105022533550214551404233315450"
BWD_ORDER = "vtnudrlfjemp5kbq9s7ioah63c482g1"


def popcount(value):
    return bin(value).count("1")


class Tree:
    def __init__(self, dims, links):
        blocks = 1 << dims
        if dims == 6:
            self.link = [None] + [int(d) for d in links]
        else:
            self.link = [None] * blocks
            count = [0] * dims
            for r in sorted(range(1, blocks), key=popcount):
                self.link[r] = min((d for d in range(dims) if (r >> d) & 1), key=lambda d: count[d])
                count[self.link[r]] += 1
        self.kids = {r: [k for k in range(1, blocks) if k & ~(1 << self.link[k]) == r] for r in range(blocks)}
        height = {}
        for r in sorted(range(blocks), key=popcount, reverse=True):
            height[r] = max([1 + height[k] for k in self.kids[r]], default=0)
        for r in self.kids:
            self.kids[r].sort(key=lambda k: -height[k])


class Plan:
    def __init__(self, dims):
        self.dims = dims
        self.blocks = 1 << dims
        self.turns = self.blocks // 2 + 1
        self.fwd = [Tree(dims, KEY_TREE), Tree(dims, VALUE_TREE)]
        self.bwd = [Tree(dims, DK_TREE), Tree(dims, DV_TREE)]
        self.forward()
        self.backward()

    def forward(self, unit_us=1.41, hop_us=1.9, turn_us=0.78):
        free = [0.0] * self.dims
        due = {}
        done = {(0, 0), (0, 1)}
        now = 1.0
        steps, waits, ready, order = [], [], [0], []

        def send(r, x):
            for k in self.fwd[x].kids[r]:
                d = self.fwd[x].link[k]
                free[d] = max(free[d], now) + unit_us
                due[k, x] = free[d] + hop_us

        now = 0.0
        send(0, 0)
        send(0, 1)
        now = 1.0
        while True:
            for unit in sorted((u for u in due if u not in done and due[u] <= now), key=lambda u: (due[u], u)):
                done.add(unit)
                now += 0.02
                send(*unit)
                waits.append(unit)
                if unit[1] == 0 and (unit[0] ^ 1, 0) in done:
                    ready.append(unit[0] >> 1)
            turn = len(steps)
            late = order[max(turn - 2, 0):turn - 1] if turn < self.turns else order[turn - 2:]
            lacking = [r for pair in late for r in (2 * pair, 2 * pair + 1) if (r, 1) not in done]
            if turn == 2 < self.turns:
                lacking = []
            if lacking or not (ready or turn == self.turns):
                now = max(now, min(due[u] for u in due if u not in done))
                continue
            if turn == self.turns:
                break
            order.append(ready.pop(0))
            steps.append(waits)
            waits = []
            now += turn_us if turn else 0.0
        self.fwd_waits = steps + [waits]
        self.fwd_pairs = order
        self.fwd_mate = max(i for i, pair in enumerate(order) if pair == 0)

    def backward(self, unit_us=2.95, hop_us=2.5, turn_us=1.58, add_us=0.025):
        if self.dims == 6:
            order = [int(c, 32) for c in BWD_ORDER]
        else:
            order = sorted(range(1, self.blocks // 2), key=lambda pair: -popcount(pair))
        order += [0, 0]
        free = [0.0] * self.dims
        due = {}
        waiting, sends, steps = set(), [], []
        now = 1.65

        def kids(unit):
            return [(k, unit[1]) for k in self.bwd[unit[1]].kids[unit[0]]]

        def flush():
            nonlocal now
            able = True
            while able:
                able = [u for u in waiting if all(due.get(k, 1e9) <= now for k in kids(u))]
                for unit in sorted(able, key=lambda u: (-popcount(u[0]), u)):
                    waiting.discard(unit)
                    now += add_us * len(kids(unit)) + 0.01
                    d = self.bwd[unit[1]].link[unit[0]]
                    free[d] = max(free[d], now) + unit_us
                    due[unit] = free[d] + hop_us
                    sends.append(unit)

        for i, pair in enumerate(order):
            if i:
                now += 0.12
                flush()
                steps.append(sends)
                sends = []
                now += turn_us
            waiting |= {(r, x) for r in (2 * pair, 2 * pair + 1) for x in range(2) if r} if i < len(order) - 1 else set()
            if not i:
                flush()
                steps.append(sends)
                sends = []
                now += 0.9
        flush()
        while waiting:
            now = max(now, min(max(due.get(k, 1e9) for k in kids(u)) for u in waiting))
            flush()
        self.bwd_sends = steps + [sends]
        self.bwd_pairs = order
        self.bwd_last = sorted((u for x in range(2) for u in kids((0, x))), key=lambda u: due[u])


def div(a, b):
    return lax.div(a, jnp.int32(b))


def mod(a, b):
    return lax.rem(a, jnp.int32(b))


def xor(a, b):
    return a + b - 2 * a * b


def lookup(index, table):
    level = [jnp.int32(v) for v in table]
    bit = 1
    while len(level) > 1:
        odd = mod(div(index, bit), 2) == 1
        nxt = [jnp.where(odd, level[i + 1], level[i]) for i in range(0, len(level) - 1, 2)]
        level = nxt + level[2 * len(nxt):]
        bit *= 2
    return level[0]


def branch(index, count, leaf):
    once = div(index, count) + 1

    def pick(low, high):
        if high - low == 1:
            acts = leaf(low)
            if acts:
                pl.loop(0, once)(lambda _: [act() for act in acts] and None)
            return
        mid = (low + high) // 2
        lax.cond(index < mid, lambda: pick(low, mid), lambda: pick(mid, high))

    pick(0, count)


def kernel(plan, q_ref, k_ref, v_ref, g_ref, o_ref, dq_ref, dk_ref, dv_ref,
           kv, kt_s, stg, land, s_buf, t_buf, p_buf, d_buf, top, q_s, g_s, v_s, q_t, g_t, c_t, acc, mst, lst, dec,
           xacc, xm, xl, lrow, drow, lcol, dcol, o_s, dq_o, dk_o, dv_o,
           ag_send, ag_recv, rs_send, rs_recv, x_send, x_recv, io):
    dims, turns = plan.dims, plan.turns
    pieces = 4 * plan.blocks
    f32, bf16 = jnp.float32, jnp.bfloat16
    me = lax.axis_index("ctx")
    core = mod(me, 2)
    chip = div(me, 2)
    bits = [mod(div(chip, 1 << d), 2) for d in range(dims)]
    gray = [xor(bits[d], bits[d + 1]) if d % 2 == 0 and d + 1 < dims else bits[d] for d in range(dims)]
    nbr = []
    for d in range(dims):
        other = chip + (1 - 2 * bits[d]) * (1 << d)
        if d % 2:
            other = other + (1 - 2 * bits[d - 1]) * (1 << (d - 1))
        nbr.append(2 * other + core)
    mate = me + 1 - 2 * core
    my_pair = div(chip, 2)

    barrier = pltpu.get_barrier_semaphore()
    for dev in nbr + [mate]:
        pl.semaphore_signal(barrier, inc=1, device_id={"ctx": dev}, device_id_type=MESH)

    def half(h):
        return pl.ds(h * PIECE, PIECE)

    loads = []
    for h in range(2):
        loads += [pltpu.make_async_copy(k_ref.at[half(h)], kv.at[0, 0, 0, h], io.at[h]),
                  pltpu.make_async_copy(v_ref.at[half(h)], v_s.at[h], io.at[2 + h])]
    for h in range(2):
        for j, (src, dst) in enumerate(((q_ref, q_s), (g_ref, g_s))):
            loads.append(pltpu.make_async_copy(src.at[:, half(h)], dst.at[h, pl.ds(0, HEADS)], io.at[4 + 2 * j + h]))
    for copy in loads:
        copy.start()
    mst[...] = jnp.full(mst.shape, NEG, f32)
    lst[...] = jnp.zeros(lst.shape, f32)
    acc[...] = jnp.zeros(acc.shape, f32)
    dec[...] = jnp.ones(dec.shape, f32)
    p_buf[...] = jnp.zeros(p_buf.shape, bf16)
    for copy in loads[:4]:
        copy.wait()
    for h in range(2):
        kv[0, 0, 1, h] = v_s[h].T

    pl.semaphore_wait(barrier, dims + 1)

    def ag_copy(k, x):
        d = plan.fwd[x].link[k]
        r = k ^ (1 << d)
        return pltpu.make_async_remote_copy(
            src_ref=kv.at[r >> 1, r & 1, x], dst_ref=kv.at[k >> 1, k & 1, x], send_sem=ag_send.at[k, x],
            recv_sem=ag_recv.at[k, x], device_id={"ctx": nbr[d]}, device_id_type=MESH)

    def rs_copy(r, x):
        return pltpu.make_async_remote_copy(
            src_ref=stg.at[r >> 1, r & 1, x], dst_ref=land.at[r - 1, x], send_sem=rs_send.at[r, x], recv_sem=rs_recv.at[r, x],
            device_id={"ctx": nbr[plan.bwd[x].link[r]]}, device_id_type=MESH)

    def mate_copy(src, dst, sem):
        return pltpu.make_async_remote_copy(src_ref=src, dst_ref=dst, send_sem=x_send.at[sem], recv_sem=x_recv.at[sem],
                                            device_id={"ctx": mate}, device_id_type=MESH)

    ours, theirs = pl.ds(0, SPAN), pl.ds(SPAN, SPAN)

    for x in range(2):
        for k in plan.fwd[x].kids[0]:
            ag_copy(k, x).start()
    for copy in loads[4:]:
        copy.wait()
    x_q = [mate_copy(ref.at[h, pl.ds(0, HEADS)], ref.at[h, pl.ds(HEADS, HEADS)], 2 * j + h)
           for j, ref in enumerate((q_s, g_s)) for h in range(2)]
    for copy in x_q:
        copy.start()

    def ag_events(waits):
        return [act for r, x in waits for act in [ag_copy(r, x).wait_recv] + [ag_copy(k, x).start for k in plan.fwd[x].kids[r]]]

    coef = SCALE * LOG2E

    def transposes(h):
        def turn(i):
            cols = pl.ds(pl.multiple_of(i * 128, 128), 128)
            turned = q_s[h, i].T
            q_t[h, :, cols] = turned
            g_t[h, :, cols] = g_s[h, i].T
            scaled = turned.astype(f32) * coef
            high = scaled.astype(bf16)
            c_t[h, pl.ds(0, HD), cols] = high
            c_t[h, pl.ds(HD, HD), cols] = (scaled - high.astype(f32)).astype(bf16)

        return turn

    for h in range(2):
        pl.loop(0, HEADS)(transposes(h))
    for copy in x_q:
        copy.wait_recv()
    for h in range(2):
        pl.loop(HEADS, TILES)(transposes(h))

    def is_future(pair):
        rel = [mod(div(pair, 1 << (d - 1)), 2) for d in range(1, dims)]
        gp = [None] + [xor(gray[d], rel[d - 1]) for d in range(1, dims)]
        other = gp[1] if dims > 1 else 0
        for d in range(2, dims):
            bit = xor(gp[d], gp[d + 1]) if d % 2 == 0 and d + 1 < dims else gp[d]
            other = other + bit * (1 << (d - 1))
        return div(other - my_pair + plan.blocks, plan.blocks)

    def place(pair, a):
        mine = div(plan.blocks // 2 - pair, plan.blocks // 2)
        fut = is_future(pair)
        turn = (pair,)
        for slot in range(2):
            h = (1 - mine) * fut * slot
            turn += (mine * a, h, mine * a + 1 - mine, mine + h, mine * slot + (1 - mine) * (fut + (1 - fut) * slot))
        return turn

    def groups(turn, some):
        for slot in range(2):
            if not any(slot * HEADS <= b < slot * HEADS + HEADS for b in some):
                continue
            p0, h0, p1, h1, qg = turn[1 + 5 * slot:6 + 5 * slot]
            yield slot, ((turn[0], p0, h0), (turn[0], p1, h1)), qg

    def key_tile(where):
        return jnp.concatenate([kv[pair, par, 0, h] for pair, par, h in where], axis=0)

    def value_tile_t(where):
        return jnp.concatenate([kv[pair, par, 1, h] for pair, par, h in where], axis=1)

    def key_tile_t(where):
        return jnp.concatenate([kt_s[pair, par, h] for pair, par, h in where], axis=1)

    def tile_of(memo, slot, kind, where):
        key = (kind, slot)
        if key not in memo:
            memo[key] = value_tile_t(where) if kind == "v" else key_tile(where) if kind == "k" else key_tile_t(where)
        return memo[key]

    def tall(ref, qg, t):
        return ref[qg, pl.ds(2 * t, 2)].reshape(256, 128)

    def cols_of(t):
        return pl.ds(t * 256, 256)

    def rows(b):
        return pl.ds(b * 256, 256)

    def mask_scores(a, keys_axis):
        key_low = me + a * (2 * (1 - 2 * mod(chip, 2)))

        def two(base0, base1, axis):
            i = lax.broadcasted_iota(jnp.int32, (256, 256), axis)
            return i + jnp.where(i < PIECE, base0, base1 - PIECE)

        def query_base(c):
            h, par = div(c, TILES), mod(div(c, HEADS), 2)
            low = me + par * (mate - me)
            return (low + h * (pieces - 1 - 2 * low)) * PIECE

        @pl.loop(0, TILES)
        def _(b):
            kpos = two(key_low * PIECE, (pieces - 1 - key_low) * PIECE, keys_axis)
            qpos = two(query_base(2 * b), query_base(2 * b + 1), 1 - keys_axis)
            s = jnp.where(qpos >= kpos, s_buf[b], NEG)
            s_buf[b] = s
            if keys_axis == 0:
                top[b] = jnp.max(s.reshape(32, 8, 256), axis=0)

    def fwd_scores(turn, some, memo):
        for slot, where, qg in groups(turn, some):
            kt = tile_of(memo, slot, "k", where)
            twice = jnp.concatenate([kt, kt], axis=1)
            for t in range(HEADS):
                b, cols = slot * HEADS + t, cols_of(t)
                if b in some:
                    if t == 0:
                        for pair, par, h in where:
                            kt_s[pair, par, h] = kv[pair, par, 0, h].T
                    s = jnp.dot(twice, c_t[qg, :, cols], preferred_element_type=f32)
                    s_buf[b] = s
                    top[b] = jnp.max(s.reshape(32, 8, 256), axis=0)

    def fwd_softmax(turn, some):
        for slot, _, qg in groups(turn, some):
            for t in range(HEADS):
                b, cols = slot * HEADS + t, cols_of(t)
                if b not in some:
                    continue
                m_old = mst[qg, :, cols]
                m_new = jnp.maximum(m_old, jnp.max(top[b], axis=0, keepdims=True))
                p = jnp.exp2(s_buf[b] - m_new[0:1])
                decay = jnp.exp2(m_old - m_new)
                lst[qg, :, cols] = lst[qg, :, cols] * decay + jnp.sum(p.reshape(32, 8, 256), axis=0)
                p_buf[rows(b), :] = p.astype(bf16)
                dec[b] = decay
                mst[qg, :, cols] = m_new

    def fwd_out(turn, some, memo):
        for slot, where, qg in groups(turn, some):
            vt = tile_of(memo, slot, "v", where)
            for t in range(HEADS):
                b, cols = slot * HEADS + t, cols_of(t)
                if b in some:
                    pv = jnp.dot(vt, p_buf[rows(b), :], preferred_element_type=f32)
                    acc[qg, :, cols] = acc[qg, :, cols] * dec[b, 0:1] + pv

    def fwd_place(j):
        return place(lookup(jnp.minimum(j, turns - 1), plan.fwd_pairs), jnp.minimum(j, 1))

    every = range(TILES)
    for act in ag_events(plan.fwd_waits[0]):
        act()
    first = fwd_place(me * 0)
    fwd_scores(first, every, {})

    def fwd_turn(j, carry):
        old, cur, new = carry
        branch(j, turns, lambda i: ag_events(plan.fwd_waits[i + 1]))

        @pl.when((j == 0) | (j == plan.fwd_mate))
        def _():
            mask_scores(jnp.minimum(j, 1), 0)

        after = fwd_place(j + 2)
        memo, memo_old = {}, {}
        for b in range(TILES + 2):
            fwd_scores(new, (b - 2,), memo)
            fwd_softmax(cur, (b - 1,))
            fwd_out(old, (b,), memo_old)
        return cur, new, after

    old, cur, _ = lax.fori_loop(0, turns - 1, fwd_turn, (first, first, fwd_place(me * 0 + 1)))
    for act in ag_events(plan.fwd_waits[turns]):
        act()
    if plan.fwd_mate == turns - 1:
        mask_scores(1, 0)
    memo = {}
    for b in range(TILES + 1):
        fwd_softmax(cur, (b - 1,))
        fwd_out(old, (b,), memo)
    late = [b for b in every if b % HEADS < HEADS // 2]
    fwd_out(cur, [b for b in every if b not in late], {})

    def bwd_scores(turn, some, memo):
        for slot, where, qg in groups(turn, some):
            for t in range(HEADS):
                b, cols = slot * HEADS + t, cols_of(t)
                if b in some:
                    for buf, lhs, kind in ((s_buf, q_s, "t"), (t_buf, g_s, "v")):
                        buf[b] = jnp.dot(tall(lhs, qg, t), tile_of(memo, slot, kind, where), preferred_element_type=f32)

    def bwd_softmax(turn, some):
        for slot, _, qg in groups(turn, some):
            for t in range(HEADS):
                b, cols = slot * HEADS + t, cols_of(t)
                if b in some:
                    lse, dr = tall(lcol, qg, t), tall(dcol, qg, t)
                    p = jnp.exp2(s_buf[b] * coef - jnp.concatenate([lse, lse], axis=1))
                    p_buf[rows(b), :] = p.astype(bf16)
                    d_buf[rows(b), :] = (p * (t_buf[b] - jnp.concatenate([dr, dr], axis=1))).astype(bf16)

    def bwd_out(turn, some, memo, parts=(True, True)):
        for slot, where, qg in groups(turn, some):
            for t in range(HEADS):
                b, cols = slot * HEADS + t, cols_of(t)
                if b not in some:
                    continue
                ds = d_buf[rows(b), :]
                if parts[1]:
                    acc[qg, :, cols] += lax.dot_general(tile_of(memo, slot, "t", where), ds, (((1,), (1,)), ((), ())),
                                                         preferred_element_type=f32)
                for x, (ref, buf) in enumerate(((q_t, ds), (g_t, p_buf[rows(b), :])) if parts[0] else ()):
                    grad = jnp.dot(ref[qg, :, cols], buf, preferred_element_type=f32)
                    memo[x] = memo[x] + grad if t else grad
                    if t < HEADS - 1:
                        continue
                    for pair, par, _ in () if slot else where:
                        stg[pair, par, x, 1] = jnp.zeros((128, 128), f32)
                    for j, (pair, par, h) in enumerate(where):
                        value = memo[x][:, j * 128:j * 128 + 128]
                        stg[pair, par, x, h] = value + stg[pair, par, x, h] if slot else value

    def bwd_place(j):
        at = jnp.minimum(j, turns - 1)
        return place(lookup(at, plan.bwd_pairs), 1 - div(at + 1, turns))

    x_m = [mate_copy(ref.at[h, :, theirs], box.at[h], 4 + 3 * h + i)
           for h in range(2) for i, (ref, box) in enumerate(((acc, xacc), (mst, xm), (lst, xl)))]
    for copy in x_m:
        copy.start()
    fwd_out(cur, late, {})
    first = bwd_place(me * 0)
    bwd_scores(first, every, {})
    for k in range(1, plan.blocks):
        for x in range(2):
            ag_copy(k, x).wait_send()
    x_r = [mate_copy(ref.at[h, :, ours], ref.at[h, :, theirs], 10 + 2 * j + h) for j, ref in enumerate((lrow, drow)) for h in range(2)]

    for h in range(2):
        for copy in x_m[3 * h:3 * h + 3]:
            copy.wait_recv()
        for head in range(HEADS):
            cols = pl.ds(head * PIECE, PIECE)
            m1, m2 = mst[h, :, cols], xm[h, :, cols]
            m = jnp.maximum(m1, m2)
            w1, w2 = jnp.exp2(m1 - m), jnp.exp2(m2 - m)
            total = jnp.sum(lst[h, :, cols] * w1 + xl[h, :, cols] * w2, axis=0, keepdims=True)
            out = (acc[h, :, cols] * w1[0:1] + xacc[h, :, cols] * w2[0:1]) / total
            o_s[head, half(h), :] = out.T.astype(bf16)
            lrow[h, :, cols] = m + jnp.log2(total)
            rounded = out.astype(bf16).astype(f32)
            d = jnp.sum(rounded * g_t[h, :, cols].astype(f32), axis=0, keepdims=True)
            drow[h, :, cols] = jnp.broadcast_to(d, (8, 128))
        for copy in x_r[h::2]:
            copy.start()
    for copy in x_m:
        copy.wait_send()
    acc[...] = jnp.zeros(acc.shape, f32)
    stores = [pltpu.make_async_copy(o_s, o_ref, io.at[8])]
    stores[0].start()

    def columns(h, i):
        cols = pl.ds(i * 128, 128)
        for row, col in ((lrow, lcol), (drow, dcol)):
            col[h, i] = jnp.broadcast_to(row[h, 0:1, cols], (128, 128)).T

    def rs_sum(r, x, kids):
        for k in kids:
            rs_copy(k, x).wait_recv()
        for h in range(2):
            total = stg[r >> 1, r & 1, x, h]
            for k in kids:
                total = total + land[k - 1, x, h]
            stg[r >> 1, r & 1, x, h] = total

    def rs_events(sends):
        return ([functools.partial(rs_sum, r, x, plan.bwd[x].kids[r]) for r, x in sends if plan.bwd[x].kids[r]]
                + [rs_copy(r, x).start for r, x in sends])

    for i in range(TILES):
        columns(i // HEADS, i % HEADS)
    if turns < 4:
        mask_scores(turns - 1, 1)
    second, third = bwd_place(me * 0 + 1), bwd_place(me * 0 + 2)
    memo = {}
    for b in late:
        bwd_softmax(first, (b,))
        bwd_scores(second, (b,), memo)
    for copy in x_r:
        copy.wait_recv()
    for i in range(TILES):
        columns(i // HEADS, HEADS + i % HEADS)
    memo = {}
    for b in every:
        if b not in late:
            bwd_softmax(first, (b,))
            bwd_scores(second, (b,), memo)
    bwd_out(first, every, {}, (True, False))
    for act in rs_events(plan.bwd_sends[0]):
        act()
    bwd_out(first, every, {}, (False, True))
    if turns < 4:
        mask_scores(turns - 2, 1)
    memo = {}
    for b in range(TILES + 1):
        bwd_softmax(second, (b,))
        bwd_scores(third, (b - 1,), memo)

    def bwd_turn(j, carry):
        old, cur, new = carry
        branch(j, turns, lambda i: rs_events(plan.bwd_sends[i - 1]) if i > 1 else [])

        @pl.when(j >= turns - 2)
        def _():
            mask_scores(turns - 1 - j, 1)

        after = bwd_place(j + 2)
        memo, memo_old = {}, {}
        for b in range(TILES + 2):
            bwd_scores(new, (b - 2,), memo)
            bwd_out(old, (b - 1,), memo_old, (False, True))
            bwd_out(old, (b,), memo_old, (True, False))
            bwd_softmax(cur, (b - 1,))
        return cur, new, after

    last = lax.fori_loop(2, turns, bwd_turn, (second, third, bwd_place(me * 0 + 3)))[0]
    for act in rs_events(plan.bwd_sends[turns - 1]):
        act()
    bwd_out(last, every, {})

    x_d = [mate_copy(acc.at[h, :, theirs], xacc.at[h], 14 + h) for h in range(2)]
    for copy in x_d:
        copy.start()
    for unit in plan.bwd_sends[turns]:
        for act in rs_events([unit]):
            act()
    for h in range(2):
        x_d[h].wait_recv()
        for head in range(HEADS):
            cols = pl.ds(head * PIECE, PIECE)
            total = (acc[h, :, cols] + xacc[h, :, cols]) * SCALE
            dq_o[head, half(h), :] = total.T.astype(bf16)
    stores.append(pltpu.make_async_copy(dq_o, dq_ref, io.at[9]))
    stores[1].start()
    for k in range(1, plan.blocks):
        for x in range(2):
            rs_copy(k, x).wait_send()
    for copy in x_q + x_r + x_d:
        copy.wait_send()
    left = [dims, dims]
    for k, x in plan.bwd_last:
        rs_sum(0, x, [k])
        left[x] -= 1
        if not left[x]:
            buf, ref, factor = ((dk_o, dk_ref, SCALE), (dv_o, dv_ref, 1.0))[x]
            for h in range(2):
                buf[half(h), :] = (stg[0, 0, x, h] * factor).T.astype(bf16)
            stores.append(pltpu.make_async_copy(buf, ref, io.at[10 + x]))
            stores[-1].start()

    for copy in stores:
        copy.wait()


def relay(*refs):
    count = (len(refs) - 1) // 3
    src, dst, buf, sem = refs[:count], refs[count:2 * count], refs[2 * count:3 * count], refs[3 * count]
    into = [pltpu.make_async_copy(a, b, sem.at[i]) for i, (a, b) in enumerate(zip(src, buf))]
    out = [pltpu.make_async_copy(b, c, sem.at[count + i]) for i, (b, c) in enumerate(zip(buf, dst))]
    for copy in into:
        copy.start()
    for i in range(count):
        into[i].wait()
        out[i].start()
    for copy in out:
        copy.wait()


def solution(mesh):
    size = mesh.shape["ctx"]
    plan = Plan(int(math.log2(size)) - 1)
    spec = P("data", "ctx", None, None)
    n = plan.blocks
    f32, bf16 = jnp.float32, jnp.bfloat16
    vm, sem = pltpu.VMEM, pltpu.SemaphoreType.DMA

    def local(queries, keys, values, grad_out):
        tokens = queries.shape[1]
        q = queries[0].transpose(1, 0, 2)
        g = grad_out[0].transpose(1, 0, 2)
        tile = (128, 128)
        big = jax.ShapeDtypeStruct((HEADS, tokens, HD), bf16)
        small = jax.ShapeDtypeStruct((tokens, HD), bf16)
        anywhere = pl.BlockSpec(memory_space=pl.ANY)
        rows, wide, half_wide = (2, TILES) + tile, (2, HD, 2 * SPAN), (2, HD, SPAN)
        stat, few = (2, 8, 2 * SPAN), (2, 8, SPAN)
        results = pl.pallas_call(
            functools.partial(kernel, plan),
            out_shape=(big, big, small, small),
            in_specs=[anywhere] * 4,
            out_specs=(anywhere,) * 4,
            scratch_shapes=[
                vm((n // 2, 2, 2, 2) + tile, bf16), vm((n // 2, 2, 2) + tile, bf16), vm((n // 2, 2, 2, 2) + tile, f32), vm((n - 1, 2, 2) + tile, f32),
                vm((TILES, 256, 256), f32), vm((TILES, 256, 256), f32), vm((TILES * 256, 256), bf16), vm((TILES * 256, 256), bf16),
                vm((TILES, 8, 256), f32),
                vm(rows, bf16), vm(rows, bf16), vm((2,) + tile, bf16), vm(wide, bf16), vm(wide, bf16), vm((2, 2 * HD, 2 * SPAN), bf16),
                vm(wide, f32), vm(stat, f32), vm(stat, f32), vm((TILES, 8, 256), f32),
                vm(half_wide, f32), vm(few, f32), vm(few, f32), vm(stat, f32), vm(stat, f32), vm(rows, f32), vm(rows, f32),
                vm(big.shape, bf16), vm(big.shape, bf16), vm(small.shape, bf16), vm(small.shape, bf16),
                sem((n, 2)), sem((n, 2)), sem((n, 2)), sem((n, 2)), sem((16,)), sem((16,)), sem((12,)),
            ],
            compiler_params=pltpu.CompilerParams(collective_id=0, has_side_effects=True, vmem_limit_bytes=67043328),
            cost_estimate=pl.CostEstimate(flops=14 * 640 * PIECE * n * 2 * HD, bytes_accessed=4 << 20, transcendentals=0),
        )(q, keys[0, :, 0], values[0, :, 0], g)
        o, dq, dk, dv = pl.pallas_call(
            relay,
            out_shape=(big, big, small, small),
            in_specs=[anywhere] * 4,
            out_specs=(anywhere,) * 4,
            scratch_shapes=[vm(x.shape, bf16) for x in (big, big, small, small)] + [sem((8,))],
            cost_estimate=pl.CostEstimate(flops=1 << 20, bytes_accessed=2 << 20, transcendentals=0),
        )(*results)
        return (o.transpose(1, 0, 2)[None], dq.transpose(1, 0, 2)[None], dk[None, :, None], dv[None, :, None])

    return jax.shard_map(local, mesh=mesh, in_specs=(spec,) * 4, out_specs=(spec,) * 4, check_vma=False)
```

```python
import functools
import math

import jax
import jax.numpy as jnp
from jax import lax
from jax.experimental import pallas as pl
from jax.experimental.pallas import tpu as pltpu
from jax.sharding import PartitionSpec as P

MESH = pl.DeviceIdType.MESH
NEG = -1e30
HD = 128
HEADS = 5
PIECE = 128
SCALE = HD ** -0.5
LOG2E = 1.4426950408889634
TILES = 2 * HEADS
SPAN = HEADS * PIECE

KEY_TREE = "011222133332330444044204331303450512252553132154554251534405024"
VALUE_TREE = "011202133303032404124114441201150505210501022525540551434312353"
DK_TREE = "011202230302020401042203040443255115012501525315014524043545435"
DV_TREE = "011221233332313444144214343331155555212333535104510402554435224"
BWD_ORDER = "vtfrsnmud7qjklp3cobe9ai6h45g128"


def popcount(value):
    return bin(value).count("1")


class Tree:
    def __init__(self, dims, links):
        blocks = 1 << dims
        if dims == 6:
            self.link = [None] + [int(d) for d in links]
        else:
            self.link = [None] * blocks
            count = [0] * dims
            for r in sorted(range(1, blocks), key=popcount):
                self.link[r] = min((d for d in range(dims) if (r >> d) & 1), key=lambda d: count[d])
                count[self.link[r]] += 1
        self.kids = {r: [k for k in range(1, blocks) if k & ~(1 << self.link[k]) == r] for r in range(blocks)}
        height = {}
        for r in sorted(range(blocks), key=popcount, reverse=True):
            height[r] = max([1 + height[k] for k in self.kids[r]], default=0)
        for r in self.kids:
            self.kids[r].sort(key=lambda k: -height[k])


class Plan:
    def __init__(self, dims):
        self.dims = dims
        self.blocks = 1 << dims
        self.turns = self.blocks // 2 + 1
        self.fwd = [Tree(dims, KEY_TREE), Tree(dims, VALUE_TREE)]
        self.bwd = [Tree(dims, DK_TREE), Tree(dims, DV_TREE)]
        self.forward()
        self.backward()

    def forward(self, unit_us=1.41, hop_us=1.9, turn_us=0.78):
        free = [0.0] * self.dims
        due = {}
        done = {(0, 0), (0, 1)}
        now = 1.0
        steps, waits, ready, order = [], [], [0], []

        def send(r, x):
            for k in self.fwd[x].kids[r]:
                d = self.fwd[x].link[k]
                free[d] = max(free[d], now) + unit_us
                due[k, x] = free[d] + hop_us

        now = 0.0
        send(0, 0)
        send(0, 1)
        now = 1.0
        while True:
            for unit in sorted((u for u in due if u not in done and due[u] <= now), key=lambda u: (due[u], u)):
                done.add(unit)
                now += 0.02
                send(*unit)
                waits.append(unit)
                if unit[1] == 0 and (unit[0] ^ 1, 0) in done:
                    ready.append(unit[0] >> 1)
            turn = len(steps)
            late = order[max(turn - 2, 0):turn - 1] if turn < self.turns else order[turn - 2:]
            lacking = [r for pair in late for r in (2 * pair, 2 * pair + 1) if (r, 1) not in done]
            if turn == 2 < self.turns:
                lacking = []
            if lacking or not (ready or turn == self.turns):
                now = max(now, min(due[u] for u in due if u not in done))
                continue
            if turn == self.turns:
                break
            order.append(ready.pop(0))
            steps.append(waits)
            waits = []
            now += turn_us if turn else 0.0
        self.fwd_waits = steps + [waits]
        self.fwd_pairs = order
        self.fwd_mate = max(i for i, pair in enumerate(order) if pair == 0)

    def backward(self, unit_us=2.9, hop_us=2.1, turn_us=1.6, add_us=0.025):
        if self.dims == 6:
            order = [int(c, 32) for c in BWD_ORDER]
        else:
            order = sorted(range(1, self.blocks // 2), key=lambda pair: -popcount(pair))
        order += [0, 0]
        free = [0.0] * self.dims
        due = {}
        waiting, sends, steps = set(), [], []
        now = 1.65

        def kids(unit):
            return [(k, unit[1]) for k in self.bwd[unit[1]].kids[unit[0]]]

        def flush():
            nonlocal now
            able = True
            while able:
                able = [u for u in waiting if all(due.get(k, 1e9) <= now for k in kids(u))]
                for unit in sorted(able, key=lambda u: (-popcount(u[0]), u)):
                    waiting.discard(unit)
                    now += add_us * len(kids(unit)) + 0.01
                    d = self.bwd[unit[1]].link[unit[0]]
                    free[d] = max(free[d], now) + unit_us
                    due[unit] = free[d] + hop_us
                    sends.append(unit)

        for i, pair in enumerate(order):
            if i:
                now += 0.12
                flush()
                steps.append(sends)
                sends = []
                now += turn_us
            waiting |= {(r, x) for r in (2 * pair, 2 * pair + 1) for x in range(2) if r} if i < len(order) - 1 else set()
            if not i:
                flush()
                steps.append(sends)
                sends = []
                now += 0.9
        flush()
        while waiting:
            now = max(now, min(max(due.get(k, 1e9) for k in kids(u)) for u in waiting))
            flush()
        self.bwd_sends = steps + [sends]
        self.bwd_pairs = order
        self.bwd_last = sorted((u for x in range(2) for u in kids((0, x))), key=lambda u: due[u])


def div(a, b):
    return lax.div(a, jnp.int32(b))


def mod(a, b):
    return lax.rem(a, jnp.int32(b))


def xor(a, b):
    return a + b - 2 * a * b


def lookup(index, table):
    level = [jnp.int32(v) for v in table]
    bit = 1
    while len(level) > 1:
        odd = mod(div(index, bit), 2) == 1
        nxt = [jnp.where(odd, level[i + 1], level[i]) for i in range(0, len(level) - 1, 2)]
        level = nxt + level[2 * len(nxt):]
        bit *= 2
    return level[0]


def branch(index, count, leaf):
    once = div(index, count) + 1

    def pick(low, high):
        if high - low == 1:
            acts = leaf(low)
            if acts:
                pl.loop(0, once)(lambda _: [act() for act in acts] and None)
            return
        mid = (low + high) // 2
        lax.cond(index < mid, lambda: pick(low, mid), lambda: pick(mid, high))

    pick(0, count)


def kernel(plan, q_ref, k_ref, v_ref, g_ref, o_ref, dq_ref, dk_ref, dv_ref,
           kv, kt_s, stg, land, s_buf, t_buf, p_buf, d_buf, top, q_s, g_s, v_s, q_t, g_t, c_t, acc, mst, lst, dec,
           xacc, xm, xl, lrow, drow, lcol, dcol, o_s, dq_o, dk_o, dv_o,
           ag_send, ag_recv, rs_send, rs_recv, x_send, x_recv, io):
    dims, turns = plan.dims, plan.turns
    pieces = 4 * plan.blocks
    f32, bf16 = jnp.float32, jnp.bfloat16
    me = lax.axis_index("ctx")
    core = mod(me, 2)
    chip = div(me, 2)
    bits = [mod(div(chip, 1 << d), 2) for d in range(dims)]
    gray = [xor(bits[d], bits[d + 1]) if d % 2 == 0 and d + 1 < dims else bits[d] for d in range(dims)]
    nbr = []
    for d in range(dims):
        other = chip + (1 - 2 * bits[d]) * (1 << d)
        if d % 2:
            other = other + (1 - 2 * bits[d - 1]) * (1 << (d - 1))
        nbr.append(2 * other + core)
    mate = me + 1 - 2 * core
    my_pair = div(chip, 2)

    barrier = pltpu.get_barrier_semaphore()
    for dev in nbr + [mate]:
        pl.semaphore_signal(barrier, inc=1, device_id={"ctx": dev}, device_id_type=MESH)

    def half(h):
        return pl.ds(h * PIECE, PIECE)

    loads = []
    for h in range(2):
        loads += [pltpu.make_async_copy(k_ref.at[half(h)], kv.at[0, 0, 0, h], io.at[h]),
                  pltpu.make_async_copy(v_ref.at[half(h)], v_s.at[h], io.at[2 + h])]
    for h in range(2):
        for j, (src, dst) in enumerate(((q_ref, q_s), (g_ref, g_s))):
            loads.append(pltpu.make_async_copy(src.at[:, half(h)], dst.at[h, pl.ds(0, HEADS)], io.at[4 + 2 * j + h]))
    for copy in loads:
        copy.start()
    mst[...] = jnp.full(mst.shape, NEG, f32)
    lst[...] = jnp.zeros(lst.shape, f32)
    acc[...] = jnp.zeros(acc.shape, f32)
    dec[...] = jnp.ones(dec.shape, f32)
    p_buf[...] = jnp.zeros(p_buf.shape, bf16)
    for copy in loads[:4]:
        copy.wait()
    for h in range(2):
        kv[0, 0, 1, h] = v_s[h].T

    pl.semaphore_wait(barrier, dims + 1)

    def ag_copy(k, x):
        d = plan.fwd[x].link[k]
        r = k ^ (1 << d)
        return pltpu.make_async_remote_copy(
            src_ref=kv.at[r >> 1, r & 1, x], dst_ref=kv.at[k >> 1, k & 1, x], send_sem=ag_send.at[k, x],
            recv_sem=ag_recv.at[k, x], device_id={"ctx": nbr[d]}, device_id_type=MESH)

    def rs_copy(r, x):
        return pltpu.make_async_remote_copy(
            src_ref=stg.at[r >> 1, r & 1, x], dst_ref=land.at[r - 1, x], send_sem=rs_send.at[r, x], recv_sem=rs_recv.at[r, x],
            device_id={"ctx": nbr[plan.bwd[x].link[r]]}, device_id_type=MESH)

    def mate_copy(src, dst, sem):
        return pltpu.make_async_remote_copy(src_ref=src, dst_ref=dst, send_sem=x_send.at[sem], recv_sem=x_recv.at[sem],
                                            device_id={"ctx": mate}, device_id_type=MESH)

    ours, theirs = pl.ds(0, SPAN), pl.ds(SPAN, SPAN)

    for x in range(2):
        for k in plan.fwd[x].kids[0]:
            ag_copy(k, x).start()
    for copy in loads[4:]:
        copy.wait()
    x_q = [mate_copy(ref.at[h, pl.ds(0, HEADS)], ref.at[h, pl.ds(HEADS, HEADS)], 2 * j + h)
           for j, ref in enumerate((q_s, g_s)) for h in range(2)]
    for copy in x_q:
        copy.start()

    def ag_events(waits):
        return [act for r, x in waits for act in [ag_copy(r, x).wait_recv] + [ag_copy(k, x).start for k in plan.fwd[x].kids[r]]]

    coef = SCALE * LOG2E

    def transposes(h):
        def turn(i):
            cols = pl.ds(pl.multiple_of(i * 128, 128), 128)
            turned = q_s[h, i].T
            q_t[h, :, cols] = turned
            g_t[h, :, cols] = g_s[h, i].T
            scaled = turned.astype(f32) * coef
            high = scaled.astype(bf16)
            c_t[h, pl.ds(0, HD), cols] = high
            c_t[h, pl.ds(HD, HD), cols] = (scaled - high.astype(f32)).astype(bf16)

        return turn

    for h in range(2):
        pl.loop(0, HEADS)(transposes(h))
    for copy in x_q:
        copy.wait_recv()
    for h in range(2):
        pl.loop(HEADS, TILES)(transposes(h))

    def is_future(pair):
        rel = [mod(div(pair, 1 << (d - 1)), 2) for d in range(1, dims)]
        gp = [None] + [xor(gray[d], rel[d - 1]) for d in range(1, dims)]
        other = gp[1] if dims > 1 else 0
        for d in range(2, dims):
            bit = xor(gp[d], gp[d + 1]) if d % 2 == 0 and d + 1 < dims else gp[d]
            other = other + bit * (1 << (d - 1))
        return div(other - my_pair + plan.blocks, plan.blocks)

    def place(pair, a):
        mine = div(plan.blocks // 2 - pair, plan.blocks // 2)
        fut = is_future(pair)
        turn = (pair,)
        for slot in range(2):
            h = (1 - mine) * fut * slot
            turn += (mine * a, h, mine * a + 1 - mine, mine + h, mine * slot + (1 - mine) * (fut + (1 - fut) * slot))
        return turn

    def groups(turn, some):
        for slot in range(2):
            if not any(slot * HEADS <= b < slot * HEADS + HEADS for b in some):
                continue
            p0, h0, p1, h1, qg = turn[1 + 5 * slot:6 + 5 * slot]
            yield slot, ((turn[0], p0, h0), (turn[0], p1, h1)), qg

    def key_tile(where):
        return jnp.concatenate([kv[pair, par, 0, h] for pair, par, h in where], axis=0)

    def value_tile_t(where):
        return jnp.concatenate([kv[pair, par, 1, h] for pair, par, h in where], axis=1)

    def key_tile_t(where):
        return jnp.concatenate([kt_s[pair, par, h] for pair, par, h in where], axis=1)

    def tile_of(memo, slot, kind, where):
        key = (kind, slot)
        if key not in memo:
            memo[key] = value_tile_t(where) if kind == "v" else key_tile(where) if kind == "k" else key_tile_t(where)
        return memo[key]

    def tall(ref, qg, t):
        return ref[qg, pl.ds(2 * t, 2)].reshape(256, 128)

    def cols_of(t):
        return pl.ds(t * 256, 256)

    def rows(b):
        return pl.ds(b * 256, 256)

    def mask_scores(a, keys_axis):
        key_low = me + a * (2 * (1 - 2 * mod(chip, 2)))

        def two(base0, base1, axis):
            i = lax.broadcasted_iota(jnp.int32, (256, 256), axis)
            return i + jnp.where(i < PIECE, base0, base1 - PIECE)

        def query_base(c):
            h, par = div(c, TILES), mod(div(c, HEADS), 2)
            low = me + par * (mate - me)
            return (low + h * (pieces - 1 - 2 * low)) * PIECE

        @pl.loop(0, TILES)
        def _(b):
            kpos = two(key_low * PIECE, (pieces - 1 - key_low) * PIECE, keys_axis)
            qpos = two(query_base(2 * b), query_base(2 * b + 1), 1 - keys_axis)
            s = jnp.where(qpos >= kpos, s_buf[b], NEG)
            s_buf[b] = s
            if keys_axis == 0:
                top[b] = jnp.max(s.reshape(32, 8, 256), axis=0)

    def fwd_scores(turn, some, memo):
        for slot, where, qg in groups(turn, some):
            kt = tile_of(memo, slot, "k", where)
            twice = jnp.concatenate([kt, kt], axis=1)
            for t in range(HEADS):
                b, cols = slot * HEADS + t, cols_of(t)
                if b in some:
                    if t == 0:
                        for pair, par, h in where:
                            kt_s[pair, par, h] = kv[pair, par, 0, h].T
                    s = jnp.dot(twice, c_t[qg, :, cols], preferred_element_type=f32)
                    s_buf[b] = s
                    top[b] = jnp.max(s.reshape(32, 8, 256), axis=0)

    def fwd_softmax(turn, some):
        for slot, _, qg in groups(turn, some):
            for t in range(HEADS):
                b, cols = slot * HEADS + t, cols_of(t)
                if b not in some:
                    continue
                m_old = mst[qg, :, cols]
                m_new = jnp.maximum(m_old, jnp.max(top[b], axis=0, keepdims=True))
                p = jnp.exp2(s_buf[b] - m_new[0:1])
                decay = jnp.exp2(m_old - m_new)
                lst[qg, :, cols] = lst[qg, :, cols] * decay + jnp.sum(p.reshape(32, 8, 256), axis=0)
                p_buf[rows(b), :] = p.astype(bf16)
                dec[b] = decay
                mst[qg, :, cols] = m_new

    def fwd_out(turn, some, memo):
        for slot, where, qg in groups(turn, some):
            vt = tile_of(memo, slot, "v", where)
            for t in range(HEADS):
                b, cols = slot * HEADS + t, cols_of(t)
                if b in some:
                    pv = jnp.dot(vt, p_buf[rows(b), :], preferred_element_type=f32)
                    acc[qg, :, cols] = acc[qg, :, cols] * dec[b, 0:1] + pv

    def fwd_place(j):
        return place(lookup(jnp.minimum(j, turns - 1), plan.fwd_pairs), jnp.minimum(j, 1))

    every = range(TILES)
    for act in ag_events(plan.fwd_waits[0]):
        act()
    first = fwd_place(me * 0)
    fwd_scores(first, every, {})

    def fwd_turn(j, carry):
        old, cur, new = carry
        branch(j, turns, lambda i: ag_events(plan.fwd_waits[i + 1]))

        @pl.when((j == 0) | (j == plan.fwd_mate))
        def _():
            mask_scores(jnp.minimum(j, 1), 0)

        after = fwd_place(j + 2)
        memo, memo_old = {}, {}
        for b in range(TILES + 2):
            fwd_scores(new, (b - 2,), memo)
            fwd_softmax(cur, (b - 1,))
            fwd_out(old, (b,), memo_old)
        return cur, new, after

    old, cur, _ = lax.fori_loop(0, turns - 1, fwd_turn, (first, first, fwd_place(me * 0 + 1)))
    for act in ag_events(plan.fwd_waits[turns]):
        act()
    if plan.fwd_mate == turns - 1:
        mask_scores(1, 0)
    memo = {}
    for b in range(TILES + 1):
        fwd_softmax(cur, (b - 1,))
        fwd_out(old, (b,), memo)
    late = [b for b in every if b % HEADS < HEADS // 2]
    fwd_out(cur, [b for b in every if b not in late], {})

    def bwd_scores(turn, some, memo):
        for slot, where, qg in groups(turn, some):
            for t in range(HEADS):
                b, cols = slot * HEADS + t, cols_of(t)
                if b in some:
                    for buf, lhs, kind in ((s_buf, q_s, "t"), (t_buf, g_s, "v")):
                        buf[b] = jnp.dot(tall(lhs, qg, t), tile_of(memo, slot, kind, where), preferred_element_type=f32)

    def bwd_softmax(turn, some):
        for slot, _, qg in groups(turn, some):
            for t in range(HEADS):
                b, cols = slot * HEADS + t, cols_of(t)
                if b in some:
                    lse, dr = tall(lcol, qg, t), tall(dcol, qg, t)
                    p = jnp.exp2(s_buf[b] * coef - jnp.concatenate([lse, lse], axis=1))
                    p_buf[rows(b), :] = p.astype(bf16)
                    d_buf[rows(b), :] = (p * (t_buf[b] - jnp.concatenate([dr, dr], axis=1))).astype(bf16)

    def bwd_out(turn, some, memo, parts=(True, True)):
        for slot, where, qg in groups(turn, some):
            for t in range(HEADS):
                b, cols = slot * HEADS + t, cols_of(t)
                if b not in some:
                    continue
                ds = d_buf[rows(b), :]
                if parts[1]:
                    acc[qg, :, cols] += lax.dot_general(tile_of(memo, slot, "t", where), ds, (((1,), (1,)), ((), ())),
                                                         preferred_element_type=f32)
                for x, (ref, buf) in enumerate(((q_t, ds), (g_t, p_buf[rows(b), :])) if parts[0] else ()):
                    grad = jnp.dot(ref[qg, :, cols], buf, preferred_element_type=f32)
                    memo[x] = memo[x] + grad if t else grad
                    if t < HEADS - 1:
                        continue
                    for pair, par, _ in () if slot else where:
                        stg[pair, par, x, 1] = jnp.zeros((128, 128), f32)
                    for j, (pair, par, h) in enumerate(where):
                        value = memo[x][:, j * 128:j * 128 + 128]
                        stg[pair, par, x, h] = value + stg[pair, par, x, h] if slot else value

    def bwd_place(j):
        at = jnp.minimum(j, turns - 1)
        return place(lookup(at, plan.bwd_pairs), 1 - div(at + 1, turns))

    x_m = [mate_copy(ref.at[h, :, theirs], box.at[h], 4 + 3 * h + i)
           for h in range(2) for i, (ref, box) in enumerate(((acc, xacc), (mst, xm), (lst, xl)))]
    for copy in x_m:
        copy.start()
    fwd_out(cur, late, {})
    first = bwd_place(me * 0)
    bwd_scores(first, every, {})
    for k in range(1, plan.blocks):
        for x in range(2):
            ag_copy(k, x).wait_send()
    x_r = [mate_copy(ref.at[h, :, ours], ref.at[h, :, theirs], 10 + 2 * j + h) for j, ref in enumerate((lrow, drow)) for h in range(2)]

    for h in range(2):
        for copy in x_m[3 * h:3 * h + 3]:
            copy.wait_recv()
        for head in range(HEADS):
            cols = pl.ds(head * PIECE, PIECE)
            m1, m2 = mst[h, :, cols], xm[h, :, cols]
            m = jnp.maximum(m1, m2)
            w1, w2 = jnp.exp2(m1 - m), jnp.exp2(m2 - m)
            total = jnp.sum(lst[h, :, cols] * w1 + xl[h, :, cols] * w2, axis=0, keepdims=True)
            out = (acc[h, :, cols] * w1[0:1] + xacc[h, :, cols] * w2[0:1]) / total
            o_s[head, half(h), :] = out.T.astype(bf16)
            lrow[h, :, cols] = m + jnp.log2(total)
            rounded = out.astype(bf16).astype(f32)
            d = jnp.sum(rounded * g_t[h, :, cols].astype(f32), axis=0, keepdims=True)
            drow[h, :, cols] = jnp.broadcast_to(d, (8, 128))
        for copy in x_r[h::2]:
            copy.start()
    for copy in x_m:
        copy.wait_send()
    acc[...] = jnp.zeros(acc.shape, f32)
    stores = [pltpu.make_async_copy(o_s, o_ref, io.at[8])]
    stores[0].start()

    def columns(h, i):
        cols = pl.ds(i * 128, 128)
        for row, col in ((lrow, lcol), (drow, dcol)):
            col[h, i] = jnp.broadcast_to(row[h, 0:1, cols], (128, 128)).T

    def rs_sum(r, x, kids):
        for k in kids:
            rs_copy(k, x).wait_recv()
        for h in range(2):
            total = stg[r >> 1, r & 1, x, h]
            for k in kids:
                total = total + land[k - 1, x, h]
            stg[r >> 1, r & 1, x, h] = total

    def rs_events(sends):
        return ([functools.partial(rs_sum, r, x, plan.bwd[x].kids[r]) for r, x in sends if plan.bwd[x].kids[r]]
                + [rs_copy(r, x).start for r, x in sends])

    for i in range(TILES):
        columns(i // HEADS, i % HEADS)
    if turns < 4:
        mask_scores(turns - 1, 1)
    second, third = bwd_place(me * 0 + 1), bwd_place(me * 0 + 2)
    memo = {}
    for b in late:
        bwd_softmax(first, (b,))
        bwd_scores(second, (b,), memo)
    for copy in x_r:
        copy.wait_recv()
    for i in range(TILES):
        columns(i // HEADS, HEADS + i % HEADS)
    memo = {}
    for b in every:
        if b not in late:
            bwd_softmax(first, (b,))
            bwd_scores(second, (b,), memo)
    bwd_out(first, every, {}, (True, False))
    for act in rs_events(plan.bwd_sends[0]):
        act()
    bwd_out(first, every, {}, (False, True))
    if turns < 4:
        mask_scores(turns - 2, 1)
    memo = {}
    for b in range(TILES + 1):
        bwd_softmax(second, (b,))
        bwd_scores(third, (b - 1,), memo)

    def bwd_turn(j, carry):
        old, cur, new = carry
        branch(j, turns, lambda i: rs_events(plan.bwd_sends[i - 1]) if i > 1 else [])

        @pl.when(j >= turns - 2)
        def _():
            mask_scores(turns - 1 - j, 1)

        after = bwd_place(j + 2)
        memo, memo_old = {}, {}
        for b in range(TILES + 2):
            bwd_scores(new, (b - 2,), memo)
            bwd_out(old, (b - 1,), memo_old, (False, True))
            bwd_out(old, (b,), memo_old, (True, False))
            bwd_softmax(cur, (b - 1,))
        return cur, new, after

    last = lax.fori_loop(2, turns, bwd_turn, (second, third, bwd_place(me * 0 + 3)))[0]
    for act in rs_events(plan.bwd_sends[turns - 1]):
        act()
    bwd_out(last, every, {})

    x_d = [mate_copy(acc.at[h, :, theirs], xacc.at[h], 14 + h) for h in range(2)]
    for copy in x_d:
        copy.start()
    for unit in plan.bwd_sends[turns]:
        for act in rs_events([unit]):
            act()
    for h in range(2):
        x_d[h].wait_recv()
        for head in range(HEADS):
            cols = pl.ds(head * PIECE, PIECE)
            total = (acc[h, :, cols] + xacc[h, :, cols]) * SCALE
            dq_o[head, half(h), :] = total.T.astype(bf16)
    stores.append(pltpu.make_async_copy(dq_o, dq_ref, io.at[9]))
    stores[1].start()
    for k in range(1, plan.blocks):
        for x in range(2):
            rs_copy(k, x).wait_send()
    for copy in x_q + x_r + x_d:
        copy.wait_send()
    left = [dims, dims]
    for k, x in plan.bwd_last:
        rs_sum(0, x, [k])
        left[x] -= 1
        if not left[x]:
            buf, ref, factor = ((dk_o, dk_ref, SCALE), (dv_o, dv_ref, 1.0))[x]
            for h in range(2):
                buf[half(h), :] = (stg[0, 0, x, h] * factor).T.astype(bf16)
            stores.append(pltpu.make_async_copy(buf, ref, io.at[10 + x]))
            stores[-1].start()

    for copy in stores:
        copy.wait()


def relay(*refs):
    count = (len(refs) - 1) // 2
    pairs = []
    for src, dst in zip(refs[:count], refs[count:2 * count]):
        pairs += [(src.at[h], dst.at[h]) for h in range(HEADS)] if len(src.shape) > 2 else [(src, dst)]
    copies = [pltpu.make_async_copy(src, dst, refs[-1].at[i]) for i, (src, dst) in enumerate(pairs)]
    for copy in copies:
        copy.start()
    for copy in copies:
        copy.wait()


def solution(mesh):
    size = mesh.shape["ctx"]
    plan = Plan(int(math.log2(size)) - 1)
    spec = P("data", "ctx", None, None)
    n = plan.blocks
    f32, bf16 = jnp.float32, jnp.bfloat16
    vm, sem = pltpu.VMEM, pltpu.SemaphoreType.DMA

    def local(queries, keys, values, grad_out):
        tokens = queries.shape[1]
        q = queries[0].transpose(1, 0, 2)
        g = grad_out[0].transpose(1, 0, 2)
        tile = (128, 128)
        big = jax.ShapeDtypeStruct((HEADS, tokens, HD), bf16)
        small = jax.ShapeDtypeStruct((tokens, HD), bf16)
        anywhere = pl.BlockSpec(memory_space=pl.ANY)
        rows, wide, half_wide = (2, TILES) + tile, (2, HD, 2 * SPAN), (2, HD, SPAN)
        stat, few = (2, 8, 2 * SPAN), (2, 8, SPAN)
        results = pl.pallas_call(
            functools.partial(kernel, plan),
            out_shape=(big, big, small, small),
            in_specs=[anywhere] * 4,
            out_specs=(anywhere,) * 4,
            scratch_shapes=[
                vm((n // 2, 2, 2, 2) + tile, bf16), vm((n // 2, 2, 2) + tile, bf16), vm((n // 2, 2, 2, 2) + tile, f32), vm((n - 1, 2, 2) + tile, f32),
                vm((TILES, 256, 256), f32), vm((TILES, 256, 256), f32), vm((TILES * 256, 256), bf16), vm((TILES * 256, 256), bf16),
                vm((TILES, 8, 256), f32),
                vm(rows, bf16), vm(rows, bf16), vm((2,) + tile, bf16), vm(wide, bf16), vm(wide, bf16), vm((2, 2 * HD, 2 * SPAN), bf16),
                vm(wide, f32), vm(stat, f32), vm(stat, f32), vm((TILES, 8, 256), f32),
                vm(half_wide, f32), vm(few, f32), vm(few, f32), vm(stat, f32), vm(stat, f32), vm(rows, f32), vm(rows, f32),
                vm(big.shape, bf16), vm(big.shape, bf16), vm(small.shape, bf16), vm(small.shape, bf16),
                sem((n, 2)), sem((n, 2)), sem((n, 2)), sem((n, 2)), sem((16,)), sem((16,)), sem((12,)),
            ],
            compiler_params=pltpu.CompilerParams(collective_id=0, has_side_effects=True, vmem_limit_bytes=67043328),
            cost_estimate=pl.CostEstimate(flops=14 * 640 * PIECE * n * 2 * HD, bytes_accessed=4 << 20, transcendentals=0),
        )(q, keys[0, :, 0], values[0, :, 0], g)
        o, dq, dk, dv = pl.pallas_call(
            relay,
            out_shape=(big, big, small, small),
            in_specs=[anywhere] * 4,
            out_specs=(anywhere,) * 4,
            scratch_shapes=[sem((2 * HEADS + 2,))],
            cost_estimate=pl.CostEstimate(flops=1 << 20, bytes_accessed=2 << 20, transcendentals=0),
        )(*results)
        return (o.transpose(1, 0, 2)[None], dq.transpose(1, 0, 2)[None], dk[None, :, None], dv[None, :, None])

    return jax.shard_map(local, mesh=mesh, in_specs=(spec,) * 4, out_specs=(spec,) * 4, check_vma=False)
```
